128 devices in a mesh: heads: 1, cpo: 16 (over z, y), cp: 8 (over x, core).
Axes of the slice: x: 4, y: 4, z: 4, core: 2. Of those that a mesh axis runs over, the one named last changes fastest.
Arguments:
- queries: bfloat16 [2, 1024, 24, 128], P(None, ('cpo', 'cp'), 'heads')
- attn_out: bfloat16 [2, 1024, 24, 128], P(None, ('cpo', 'cp'), 'heads')
- grad_out: bfloat16 [2, 1024, 24, 128], P(None, ('cpo', 'cp'), 'heads')
- log_sum_exp: float32 [2, 1024, 24], P(None, ('cpo', 'cp'), 'heads')
- key_cache: bfloat16 [4096, 8, 128], P(('cpo', 'cp'), 'heads')
- value_cache: bfloat16 [4096, 8, 128], P(('cpo', 'cp'), 'heads')
Outputs:
- output 1: bfloat16 [2, 1024, 24, 128], P(None, ('cpo', 'cp'), 'heads')
- output 2: float32 [4096, 8, 128], P(('cpo', 'cp'), 'heads')
- output 3: float32 [4096, 8, 128], P(('cpo', 'cp'), 'heads')
All inputs are finite; a program needn't handle non-finite values.
Results may differ from the reference program's by a relative error of at most 0.001.
Values are sent between devices in bfloat16 or wider.
A program may use at most 1 GiB of HBM per device.

```python
import jax
import jax.numpy as jnp
from jax import lax

N_SLICES = 2
SLICE_LEN = 1024
PREFIX_BASE = 2048
Q_HEADS = 24
KV_HEADS = 8
HEAD_DIM = 128
ROW_BLOCK = 8


def slice_lse(queries_f, keys_f, slice_idx):
    group_size = Q_HEADS // KV_HEADS
    softmax_scale = HEAD_DIM ** -0.5
    limit_len = PREFIX_BASE + (slice_idx + 1) * SLICE_LEN
    key_part = keys_f[:limit_len]
    key_pos = jnp.arange(limit_len)
    n_blocks = SLICE_LEN // ROW_BLOCK
    q_blocks = queries_f.reshape(n_blocks, ROW_BLOCK, KV_HEADS, group_size, HEAD_DIM)
    row_starts = PREFIX_BASE + slice_idx * SLICE_LEN + ROW_BLOCK * jnp.arange(n_blocks)

    def one_block(operand):
        q_blk, row_start = operand
        scores = jnp.einsum('rhgd,khd->rhgk', q_blk, key_part) * softmax_scale
        q_pos = row_start + jnp.arange(ROW_BLOCK)
        visible = (key_pos[None, :] <= q_pos[:, None])[:, None, None, :]
        scores = jnp.where(visible, scores, -jnp.inf)
        return jax.nn.logsumexp(scores, axis=-1).reshape(ROW_BLOCK, Q_HEADS)

    return lax.map(one_block, (q_blocks, row_starts)).reshape(SLICE_LEN, Q_HEADS)


def setup_inputs(seed: int = 0, part: int = 0) -> dict:
    base_key = jax.random.fold_in(jax.random.key(seed), part)
    key_q, key_k, key_v, key_o, key_g = jax.random.split(base_key, 5)
    total_len = PREFIX_BASE + N_SLICES * SLICE_LEN
    row_shape = (N_SLICES, SLICE_LEN, Q_HEADS, HEAD_DIM)
    cache_shape = (total_len, KV_HEADS, HEAD_DIM)
    queries = jax.random.normal(key_q, row_shape, jnp.float32).astype(jnp.bfloat16)
    key_cache = jax.random.normal(key_k, cache_shape, jnp.float32).astype(jnp.bfloat16)
    value_cache = jax.random.normal(key_v, cache_shape, jnp.float32).astype(jnp.bfloat16)
    out_val = jax.random.normal(key_o, row_shape, jnp.float32)
    grad_out = (0.1 * out_val + jax.random.normal(key_g, row_shape, jnp.float32)).astype(jnp.bfloat16)
    attn_out = out_val.astype(jnp.bfloat16)
    queries_f = queries.astype(jnp.float32)
    keys_f = key_cache.astype(jnp.float32)
    log_sum_exp = jnp.stack([slice_lse(queries_f[slice_idx], keys_f, slice_idx) for slice_idx in range(N_SLICES)])
    return {'queries': queries, 'attn_out': attn_out, 'grad_out': grad_out, 'log_sum_exp': log_sum_exp, 'key_cache': key_cache, 'value_cache': value_cache}


def reference(queries, attn_out, grad_out, log_sum_exp, key_cache, value_cache):
    group_size = Q_HEADS // KV_HEADS
    softmax_scale = HEAD_DIM ** -0.5
    total_len = PREFIX_BASE + N_SLICES * SLICE_LEN
    n_blocks = SLICE_LEN // ROW_BLOCK
    blk_shape = (n_blocks, ROW_BLOCK, KV_HEADS, group_size)
    keys_f = key_cache.astype(jnp.float32)
    values_f = value_cache.astype(jnp.float32)
    row_delta = jnp.sum(grad_out.astype(jnp.float32) * attn_out.astype(jnp.float32), axis=-1)
    grad_key = jnp.zeros((total_len, KV_HEADS, HEAD_DIM), jnp.float32)
    grad_value = jnp.zeros((total_len, KV_HEADS, HEAD_DIM), jnp.float32)
    dq_list = []
    for slice_idx in reversed(range(N_SLICES)):
        limit_len = PREFIX_BASE + (slice_idx + 1) * SLICE_LEN
        key_part = keys_f[:limit_len]
        value_part = values_f[:limit_len]
        key_pos = jnp.arange(limit_len)
        operands = (
            queries[slice_idx].astype(jnp.float32).reshape(blk_shape + (HEAD_DIM,)),
            grad_out[slice_idx].astype(jnp.float32).reshape(blk_shape + (HEAD_DIM,)),
            log_sum_exp[slice_idx].reshape(blk_shape),
            row_delta[slice_idx].reshape(blk_shape),
            PREFIX_BASE + slice_idx * SLICE_LEN + ROW_BLOCK * jnp.arange(n_blocks),
        )

        def one_block(carry_acc, operand):
            key_acc, value_acc = carry_acc
            q_blk, g_blk, lse_blk, delta_blk, row_start = operand
            scores = jnp.einsum('rhgd,khd->rhgk', q_blk, key_part) * softmax_scale
            q_pos = row_start + jnp.arange(ROW_BLOCK)
            visible = (key_pos[None, :] <= q_pos[:, None])[:, None, None, :]
            attn_prob = jnp.where(visible, jnp.exp(scores - lse_blk[..., None]), 0.0)
            prob_bf = attn_prob.astype(jnp.bfloat16).astype(jnp.float32)
            value_acc = value_acc + jnp.einsum('rhgk,rhgd->khd', prob_bf, g_blk)
            grad_prob = jnp.einsum('rhgd,khd->rhgk', g_blk, value_part)
            grad_scores = attn_prob * (grad_prob - delta_blk[..., None])
            grad_scores = grad_scores.astype(jnp.bfloat16).astype(jnp.float32)
            dq_blk = jnp.einsum('rhgk,khd->rhgd', grad_scores, key_part) * softmax_scale
            key_acc = key_acc + softmax_scale * jnp.einsum('rhgk,rhgd->khd', grad_scores, q_blk)
            return (key_acc, value_acc), dq_blk.astype(jnp.bfloat16)

        start_acc = (grad_key[:limit_len], grad_value[:limit_len])
        (key_acc, value_acc), dq_blocks = lax.scan(one_block, start_acc, operands)
        grad_key = lax.dynamic_update_slice(grad_key, key_acc, (0, 0, 0))
        grad_value = lax.dynamic_update_slice(grad_value, value_acc, (0, 0, 0))
        dq_list.append(dq_blocks.reshape(SLICE_LEN, Q_HEADS, HEAD_DIM))
    grad_query = jnp.stack(dq_list[::-1])
    return grad_query, grad_key, grad_value
```

```python
import jax
import jax.numpy as jnp
from jax import lax
from jax.experimental import pallas as pl
from jax.experimental.pallas import tpu as pltpu
from jax.sharding import PartitionSpec as P

CP_AXES = ('cpo', 'cp')
MESH = pl.DeviceIdType.MESH
LOG2E = 1.4426950408889634

ROW = 8
RING = 4
GRP = 3
TOK = 16
KEYS = 32
DIM = 128
HALF = ROW // 2
QROWS = ROW * GRP * TOK
KROWS = ROW * KEYS
PACK = GRP * TOK
SCALE = DIM ** -0.5
NSEM = 80

NT = (((1,), (1,)), ((), ()))
NN = (((1,), (0,)), ((), ()))
TN = (((0,), (0,)), ((), ()))


def dot(a, b, dims):
    return lax.dot_general(a, b, dims, preferred_element_type=jnp.float32)


def kernel(q_in, o_in, g_in, l_in, k_in, v_in, out_q, out_kv,
           q_vm, o_vm, g_vm, l_vm, k_vm, v_vm, xs, xk, ts, tt,
           pq, pst, pkv, qd, st, kv, ld, rowc, akv, aqt, oq,
           ra_kv, rb_kv, ra_q, rb_q, fq, in_sem, ssem, rsem):
    me = lax.axis_index('cp')
    cpo = lax.axis_index('cpo')
    z, y = cpo // RING, cpo % RING

    def row_dev(j):
        return (0, cpo, j)

    def ring_devs(axis):
        if axis == 'y':
            return [(0, z * RING + (y + d) % RING, me) for d in (1, 3)]
        return [(0, ((z + d) % RING) * RING + y, me) for d in (1, 3)]

    ydev, zdev = ring_devs('y'), ring_devs('z')

    barrier = pltpu.get_barrier_semaphore()
    for j in range(1, ROW):
        pl.semaphore_signal(barrier, inc=1, device_id=row_dev((me + j) % ROW), device_id_type=MESH)
    for dev in ydev + zdev:
        pl.semaphore_signal(barrier, inc=1, device_id=dev, device_id_type=MESH)

    loads = [pltpu.make_async_copy(src, dst, in_sem.at[i]) for i, (src, dst) in enumerate(
        ((g_in, g_vm), (o_in, o_vm), (q_in, q_vm), (l_in, l_vm), (k_in, k_vm), (v_in, v_vm)))]
    for ld_copy in loads:
        ld_copy.start()

    counter = [0]

    def take(n):
        first = counter[0]
        counter[0] += n
        assert counter[0] <= NSEM
        return first

    def remote(src, dst, send_i, recv_i, dev):
        return pltpu.make_async_remote_copy(
            src_ref=src, dst_ref=dst, send_sem=ssem.at[send_i], recv_sem=rsem.at[recv_i],
            device_id=dev, device_id_type=MESH)

    sent = []

    loads[0].wait()
    loads[1].wait()
    gf = g_vm[...].reshape(TOK, ROW * GRP, DIM).astype(jnp.float32)
    xs[...] = gf
    of = o_vm[...].reshape(TOK, ROW * GRP, DIM).astype(jnp.float32)
    delta = jnp.sum(gf * of, axis=-1)
    ts[...] = jnp.zeros_like(ts)
    loads[3].wait()
    ts[pl.ds(0, TOK), pl.ds(0, ROW * GRP)] = l_vm[...].reshape(TOK, ROW * GRP)
    ts[pl.ds(TOK, TOK), pl.ds(0, ROW * GRP)] = delta
    for h in range(ROW):
        for g in range(GRP):
            pq[h, GRP + g] = xs[:, h * GRP + g, :].astype(jnp.bfloat16)
    loads[2].wait()
    xs[...] = q_vm[...].reshape(TOK, ROW * GRP, DIM).astype(jnp.float32)
    for h in range(ROW):
        for g in range(GRP):
            pq[h, g] = xs[:, h * GRP + g, :].astype(jnp.bfloat16)
    tt[...] = ts[...].T
    lane = lax.broadcasted_iota(jnp.int32, (ROW, DIM), 1)
    for which in range(2):
        packed = jnp.zeros((ROW, DIM), jnp.float32)
        for g in range(GRP):
            part = tt[pl.ds(g, ROW, stride=GRP), :]
            shift = (g * TOK - which * TOK) % DIM
            if shift:
                part = pltpu.roll(part, shift, 1)
            packed = jnp.where((lane >= g * TOK) & (lane < (g + 1) * TOK), part, packed)
        pst[:, which, :] = pltpu.roll(packed, (PACK * me) % DIM, 1)

    pl.semaphore_wait(barrier, ROW - 1 + 4)

    def row_send(src, dst, base):
        for j in (4, 5, 2, 3, 6, 7, 1):
            d = (me + j) % ROW
            remote(src.at[d], dst.at[0, me], base + d, base + me, row_dev(d)).start()

    def row_wait(buf, base, s):
        @pl.when(me != s)
        def _():
            remote(buf.at[0, s], buf.at[0, s], base + s, base + s, row_dev(s)).wait_recv()

    def row_wait_send(src, dst, base):
        for j in range(1, ROW):
            d = (me + j) % ROW
            remote(src.at[d], dst.at[0, me], base + d, base + me, row_dev(d)).wait_send()

    xq, xst, xkv = take(ROW), take(ROW), take(ROW)
    row_send(pq, qd, xq)
    row_send(pst, st, xst)
    qd[0, me] = pq[me]
    st[0, me] = pst[me]

    loads[4].wait()
    xk[...] = k_vm[...].astype(jnp.float32)
    for h in range(ROW):
        pkv[h, 0] = xk[:, h, :].astype(jnp.bfloat16)
    loads[5].wait()
    xk[...] = v_vm[...].astype(jnp.float32)
    for h in range(ROW):
        pkv[h, 1] = xk[:, h, :].astype(jnp.bfloat16)
    row_send(pkv, kv, xkv)
    kv[0, me] = pkv[me]

    r_id = lax.broadcasted_iota(jnp.int32, (1, QROWS), 1)
    rowc[...] = (((r_id >> 3) & 1) * 1024 + ((r_id * 1366) >> 16) * 8 + (r_id & 7)) + (2048 + z * 256 - y * 256)
    akv[...] = jnp.zeros_like(akv)
    aqt[...] = jnp.zeros_like(aqt)

    class Gather:
        def __init__(self, buf, devs):
            self.buf, self.devs = buf, devs
            self.near = take(4)
            self.far = take(2)

        def part(self, slot, half):
            return self.buf.at[slot, pl.ds(half * HALF, HALF)]

        def near_copy(self, slot, half):
            i = self.near + (slot - 1) * 2 + half
            return remote(self.part(0, half), self.part(slot, half), i, i, self.devs[slot - 1])

        def far_copy(self, half):
            i = self.far + half
            return remote(self.part(1 + half, half), self.part(3, half), i, i, self.devs[half])

        def send(self, half):
            for slot in (1, 2):
                self.near_copy(slot, half).start()
                sent.append((self.near_copy, slot, half))

        def wait(self, slot, half):
            self.near_copy(slot, half).wait_recv()

        def forward(self, half):
            self.wait(1 + half, half)
            self.far_copy(half).start()
            sent.append((self.far_copy, half))

        def wait_far(self):
            for half in (0, 1):
                self.far_copy(half).wait_recv()

    agq, agst, agkv = Gather(qd, ydev), Gather(st, ydev), Gather(kv, zdev)
    for half in (0, 1):
        for s in range(half * HALF, (half + 1) * HALF):
            row_wait(qd, xq, s)
            row_wait(st, xst, s)
        agq.send(half)
        agst.send(half)
    for half in (0, 1):
        for s in range(half * HALF, (half + 1) * HALF):
            row_wait(kv, xkv, s)
        agkv.send(half)

    src_id = lax.broadcasted_iota(jnp.int32, (ROW, DIM), 0)

    def assemble(slot):
        for which in range(2):
            rows = st[slot, :, which, :]
            for k in range(QROWS // DIM):
                mine = (((lane + k * DIM) * 1366) >> 16) == src_id
                line = jnp.sum(jnp.where(mine, rows, 0.0), axis=0, keepdims=True)
                ld[slot, pl.ds(which, 1), pl.ds(k * DIM, DIM)] = line * LOG2E if which == 0 else line

    class Scatter:
        def __init__(self, acc, ra, rb, devs):
            self.acc, self.ra, self.rb, self.devs = acc, ra, rb, devs
            self.first = take(2)
            self.second = take(4)

        def part(self, slot, half):
            return self.acc.at[slot, pl.ds(half * HALF, HALF)]

        def far_copy(self, half):
            i = self.first + half
            return remote(self.part(3, half), self.ra.at[half], i, i, self.devs[half])

        def near_copy(self, side, half):
            i = self.second + side * 2 + half
            return remote(self.part(2 - side, half), self.rb.at[side, pl.ds(half * HALF, HALF)], i, i, self.devs[side])

        def send_far(self):
            for half in (0, 1):
                self.far_copy(half).start()
                sent.append((self.far_copy, half))

        def send_early(self, side):
            self.near_copy(side, 1 - side).start()
            sent.append((self.near_copy, side, 1 - side))

        def send_late(self, side):
            self.far_copy(side).wait_recv()
            part = pl.ds(side * HALF, HALF)
            self.acc[2 - side, part] = self.acc[2 - side, part] + self.ra[side]
            self.near_copy(side, side).start()
            sent.append((self.near_copy, side, side))

        def total(self, half):
            for side in (0, 1):
                self.near_copy(side, half).wait_recv()
            part = pl.ds(half * HALF, HALF)
            return self.acc[0, part] + self.rb[0, part] + self.rb[1, part]

    rskv, rsq = Scatter(akv, ra_kv, rb_kv, zdev), Scatter(oq, ra_q, rb_q, ydev)

    key_row = lax.broadcasted_iota(jnp.int32, (KROWS, QROWS), 0)

    def offset(slot):
        return jnp.where(slot == 1, 3, jnp.where(slot == 2, 1, jnp.where(slot == 3, 2, 0)))

    def block(qs, ks):
        yq = (y + offset(qs)) % RING
        zk = (z + offset(ks)) % RING
        q = qd[qs, :, pl.ds(0, GRP)].reshape(QROWS, DIM)
        g = qd[qs, :, pl.ds(GRP, GRP)].reshape(QROWS, DIM)
        k = kv[ks, :, 0].reshape(KROWS, DIM)
        v = kv[ks, :, 1].reshape(KROWS, DIM)
        lse = ld[qs, pl.ds(0, 1), :]
        dlt = ld[qs, pl.ds(1, 1), :]
        thr = rowc[...] + (yq * 64 - zk * 1024)
        s_t = dot(k, q, NT)
        p_t = jnp.where(key_row <= thr, jnp.exp2(s_t * (SCALE * LOG2E) - lse), 0.0)
        dp_t = dot(v, g, NT)
        ds_t = (p_t * (dp_t - dlt)).astype(jnp.bfloat16)
        akv[ks, :, 1] = akv[ks, :, 1] + dot(p_t.astype(jnp.bfloat16), g, NN).reshape(ROW, KEYS, DIM)
        akv[ks, :, 0] = akv[ks, :, 0] + dot(ds_t, q, NN).reshape(ROW, KEYS, DIM)
        aqt[qs] = aqt[qs] + dot(k, ds_t, TN)

    def finish_q(slot):
        oq[slot] = aqt[slot].T.reshape(ROW, PACK, DIM)

    def before_0():
        assemble(0)

    def before_1():
        for half in (0, 1):
            agq.forward(half)
            agst.forward(half)
        for half in (0, 1):
            agkv.forward(half)
        agkv.wait(1, 1)

    def before_2():
        agkv.wait(2, 0)

    def before_3():
        agq.wait(1, 1)
        agst.wait(1, 1)
        assemble(1)

    def before_6():
        agq.wait(2, 0)
        agst.wait(2, 0)
        assemble(2)

    def before_9():
        agkv.wait_far()

    def before_12():
        agq.wait_far()
        agst.wait_far()
        assemble(3)

    def after_10():
        finish_q(1)
        rsq.send_early(1)

    def after_11():
        finish_q(2)
        rsq.send_early(0)

    def after_15():
        finish_q(3)
        rsq.send_far()

    before = {0: before_0, 1: before_1, 2: before_2, 3: before_3, 6: before_6, 9: before_9, 12: before_12}
    after = {9: lambda: finish_q(0), 10: after_10, 11: after_11, 12: rskv.send_far,
             13: lambda: rskv.send_early(1), 14: lambda: rskv.send_early(0), 15: after_15}

    def step(i, carry):
        for n, act in before.items():
            pl.when(i == n)(act)
        qs = jnp.where(i < 9, i // 3, jnp.where(i < 12, i - 9, 3))
        late = jnp.where(i == 12, 3, jnp.where(i == 15, 0, i - 12))
        ks = jnp.where(i < 9, i % 3, jnp.where(i < 12, 3, late))
        block(qs, ks)
        for n, act in after.items():
            pl.when(i == n)(act)
        return carry

    lax.fori_loop(0, 16, step, 0)

    rskv.send_late(1)
    rskv.send_late(0)
    rsq.send_late(1)
    rsq.send_late(0)

    fkv_i, fq_i = take(ROW), take(ROW)

    def give(src, dst, base, half):
        for s in range(half * HALF, (half + 1) * HALF):
            @pl.when(me != s)
            def _():
                remote(src(s), dst.at[me], base + s, base + me, row_dev(s)).start()

    for half in (0, 1):
        tot = rskv.total(half)
        part = pl.ds(half * HALF, HALF)
        akv[0, part, 0] = tot[:, 0] * SCALE
        akv[0, part, 1] = tot[:, 1]
        give(lambda s: akv.at[0, s], out_kv, fkv_i, half)
    out_kv[me] = akv[0, me]
    for half in (0, 1):
        fq[pl.ds(half * HALF, HALF)] = (rsq.total(half) * SCALE).astype(jnp.bfloat16)
        give(lambda s: fq.at[s], out_q, fq_i, half)
    out_q[me] = fq[me]

    row_wait_send(pq, qd, xq)
    row_wait_send(pst, st, xst)
    row_wait_send(pkv, kv, xkv)
    for make, *where in sent:
        make(*where).wait_send()
    for src, dst, base in ((akv.at[0], out_kv, fkv_i), (fq, out_q, fq_i)):
        for s in range(ROW):
            @pl.when(me != s)
            def _():
                copy = remote(src.at[s], dst.at[s], base + s, base + s, row_dev(s))
                copy.wait_send()
                copy.wait_recv()


def call(queries, attn_out, grad_out, log_sum_exp, key_cache, value_cache):
    f32, bf16 = jnp.float32, jnp.bfloat16
    vmem = pltpu.VMEM
    tok = (2, TOK // 2, ROW * GRP, DIM)
    key = (KEYS, ROW, DIM)
    scratch = [
        vmem(tok, bf16), vmem(tok, bf16), vmem(tok, bf16), vmem(tok[:3], f32), vmem(key, bf16), vmem(key, bf16),
        vmem((TOK, ROW * GRP, DIM), f32), vmem(key, f32), vmem((DIM, DIM), f32), vmem((DIM, DIM), f32),
        vmem((ROW, 2 * GRP, TOK, DIM), bf16), vmem((ROW, 2, DIM), f32), vmem((ROW, 2, KEYS, DIM), bf16),
        vmem((RING, ROW, 2 * GRP, TOK, DIM), bf16), vmem((RING, ROW, 2, DIM), f32), vmem((RING, ROW, 2, KEYS, DIM), bf16),
        vmem((RING, 8, QROWS), f32), vmem((1, QROWS), jnp.int32),
        vmem((RING, ROW, 2, KEYS, DIM), f32), vmem((RING, DIM, QROWS), f32), vmem((RING, ROW, PACK, DIM), f32),
        vmem((2, HALF, 2, KEYS, DIM), f32), vmem((2, ROW, 2, KEYS, DIM), f32),
        vmem((2, HALF, PACK, DIM), f32), vmem((2, ROW, PACK, DIM), f32),
        vmem((ROW, PACK, DIM), bf16),
        pltpu.SemaphoreType.DMA((6,)), pltpu.SemaphoreType.DMA((NSEM,)), pltpu.SemaphoreType.DMA((NSEM,)),
    ]
    return pl.pallas_call(
        kernel,
        out_shape=(jax.ShapeDtypeStruct((ROW, PACK, DIM), bf16),
                   jax.ShapeDtypeStruct((ROW, 2, KEYS, DIM), f32)),
        in_specs=[pl.BlockSpec(memory_space=pl.ANY)] * 6,
        out_specs=[pl.BlockSpec(memory_space=pltpu.VMEM)] * 2,
        scratch_shapes=scratch,
        compiler_params=pltpu.CompilerParams(collective_id=0, has_side_effects=True),
        name='attn_bwd_3d',
    )(queries, attn_out, grad_out, log_sum_exp, key_cache, value_cache)


def solution(mesh):
    row_spec = P(None, CP_AXES, 'heads', None)
    stat_spec = P(None, CP_AXES, 'heads')
    key_spec = P(CP_AXES, 'heads', None)

    def local_grads(queries, attn_out, grad_out, log_sum_exp, key_cache, value_cache):
        out_q, out_kv = call(queries, attn_out, grad_out, log_sum_exp, key_cache, value_cache)
        grad_query = out_q.reshape(ROW, GRP, 2, TOK // 2, DIM).transpose(2, 3, 0, 1, 4).reshape(queries.shape)
        grad_key = out_kv[:, 0].transpose(1, 0, 2)
        grad_value = out_kv[:, 1].transpose(1, 0, 2)
        return grad_query, grad_key, grad_value

    return jax.shard_map(local_grads, mesh=mesh, in_specs=(row_spec, row_spec, row_spec, stat_spec, key_spec, key_spec),
                         out_specs=(row_spec, key_spec, key_spec), check_vma=False)
```

```python
import jax
import jax.numpy as jnp
from jax import lax
from jax.experimental import pallas as pl
from jax.experimental.pallas import tpu as pltpu
from jax.sharding import PartitionSpec as P

CP_AXES = ('cpo', 'cp')
MESH = pl.DeviceIdType.MESH
LOG2E = 1.4426950408889634

ROW = 8
RING = 4
GRP = 3
TOK = 16
KEYS = 32
DIM = 128
HALF = ROW // 2
QROWS = ROW * GRP * TOK
KROWS = ROW * KEYS
PACK = GRP * TOK
SCALE = DIM ** -0.5
NSEM = 96
OWN, F, G, X = range(4)

NT = (((1,), (1,)), ((), ()))
NN = (((1,), (0,)), ((), ()))
TN = (((0,), (0,)), ((), ()))


def dot(a, b, dims):
    return lax.dot_general(a, b, dims, preferred_element_type=jnp.float32)


def kernel(q_in, o_in, g_in, l_in, k_in, v_in, out_q, out_kv,
           q_vm, o_vm, g_vm, l_vm, k_vm, v_vm, xs, xk, ts, tt,
           pq, pst, pkv, qd, st, kv, ld, rowc, akv, aqt, oq,
           ra_kv, rb_kv, ra_q, rb_q, fq, in_sem, ssem, rsem):
    me = lax.axis_index('cp')
    cpo = lax.axis_index('cpo')
    z, y = cpo // RING, cpo % RING

    def row_dev(j):
        return (0, cpo, j)

    def ring_devs(axis):
        if axis == 'y':
            return [(0, z * RING + (y + d) % RING, me) for d in (1, 3)]
        return [(0, ((z + d) % RING) * RING + y, me) for d in (1, 3)]

    ydev, zdev = ring_devs('y'), ring_devs('z')

    barrier = pltpu.get_barrier_semaphore()
    for j in range(1, ROW):
        pl.semaphore_signal(barrier, inc=1, device_id=row_dev((me + j) % ROW), device_id_type=MESH)
    for dev in ydev + zdev:
        pl.semaphore_signal(barrier, inc=1, device_id=dev, device_id_type=MESH)

    loads = [pltpu.make_async_copy(src, dst, in_sem.at[i]) for i, (src, dst) in enumerate(
        ((g_in, g_vm), (o_in, o_vm), (q_in, q_vm), (l_in, l_vm), (k_in, k_vm), (v_in, v_vm)))]
    for ld_copy in loads:
        ld_copy.start()

    counter = [0]

    def take(n):
        first = counter[0]
        counter[0] += n
        assert counter[0] <= NSEM
        return first

    def remote(src, dst, send_i, recv_i, dev):
        return pltpu.make_async_remote_copy(
            src_ref=src, dst_ref=dst, send_sem=ssem.at[send_i], recv_sem=rsem.at[recv_i],
            device_id=dev, device_id_type=MESH)

    sent = []

    loads[0].wait()
    loads[1].wait()
    gf = g_vm[...].reshape(TOK, ROW * GRP, DIM).astype(jnp.float32)
    xs[...] = gf
    of = o_vm[...].reshape(TOK, ROW * GRP, DIM).astype(jnp.float32)
    delta = jnp.sum(gf * of, axis=-1)
    ts[...] = jnp.zeros_like(ts)
    loads[3].wait()
    ts[pl.ds(0, TOK), pl.ds(0, ROW * GRP)] = l_vm[...].reshape(TOK, ROW * GRP)
    ts[pl.ds(TOK, TOK), pl.ds(0, ROW * GRP)] = delta
    for h in range(ROW):
        for g in range(GRP):
            pq[h, GRP + g] = xs[:, h * GRP + g, :].astype(jnp.bfloat16)
    loads[2].wait()
    xs[...] = q_vm[...].reshape(TOK, ROW * GRP, DIM).astype(jnp.float32)
    for h in range(ROW):
        for g in range(GRP):
            pq[h, g] = xs[:, h * GRP + g, :].astype(jnp.bfloat16)
    tt[...] = ts[...].T
    lane = lax.broadcasted_iota(jnp.int32, (ROW, DIM), 1)
    for which in range(2):
        packed = jnp.zeros((ROW, DIM), jnp.float32)
        for g in range(GRP):
            part = tt[pl.ds(g, ROW, stride=GRP), :]
            shift = (g * TOK - which * TOK) % DIM
            if shift:
                part = pltpu.roll(part, shift, 1)
            packed = jnp.where((lane >= g * TOK) & (lane < (g + 1) * TOK), part, packed)
        pst[:, which, :] = pltpu.roll(packed, (PACK * me) % DIM, 1)

    with jax.named_scope('barrier'):
        pl.semaphore_wait(barrier, ROW - 1 + 4)

    def row_send(src, dst, base):
        for j in (4, 5, 2, 3, 6, 7, 1):
            d = (me + j) % ROW
            remote(src.at[d], dst.at[0, me], base + d, base + me, row_dev(d)).start()

    def row_wait(buf, base, s):
        @pl.when(me != s)
        def _():
            remote(buf.at[0, s], buf.at[0, s], base + s, base + s, row_dev(s)).wait_recv()

    def row_wait_send(src, dst, base):
        for j in range(1, ROW):
            d = (me + j) % ROW
            remote(src.at[d], dst.at[0, me], base + d, base + me, row_dev(d)).wait_send()

    xq, xst, xkv = take(ROW), take(ROW), take(ROW)
    row_send(pq, qd, xq)
    row_send(pst, st, xst)
    qd[0, me] = pq[me]
    st[0, me] = pst[me]

    loads[4].wait()
    xk[...] = k_vm[...].astype(jnp.float32)
    for h in range(ROW):
        pkv[h, 0] = xk[:, h, :].astype(jnp.bfloat16)
    loads[5].wait()
    xk[...] = v_vm[...].astype(jnp.float32)
    for h in range(ROW):
        pkv[h, 1] = xk[:, h, :].astype(jnp.bfloat16)
    row_send(pkv, kv, xkv)
    kv[0, me] = pkv[me]

    akv[...] = jnp.zeros_like(akv)
    aqt[...] = jnp.zeros_like(aqt)

    def offset(group, half):
        near = (1, 3) if half else (3, 1)
        return jnp.where(group == F, near[0], jnp.where(group == G, near[1], jnp.where(group == X, 2, 0)))

    def part(ref, half):
        return ref.at[pl.ds(half * HALF, HALF)]

    r_id = lax.broadcasted_iota(jnp.int32, (1, QROWS), 1)
    token = ((r_id >> 3) & 1) * 1024 + ((r_id * 1366) >> 16) * 8 + (r_id & 7) + (2048 + z * 256)
    for group in range(RING):
        plane = jnp.where(r_id < QROWS // 2, (y + offset(group, 0)) % RING, (y + offset(group, 1)) % RING)
        rowc[group] = token + plane * 64

    class Gather:
        def __init__(self, buf, devs):
            self.buf, self.devs = buf, devs
            self.near = take(4)
            self.far = take(2)

        def near_copy(self, group, half):
            i = self.near + (group - F) * 2 + half
            dev = self.devs[half if group == F else 1 - half]
            return remote(part(self.buf.at[OWN], half), part(self.buf.at[group], half), i, i, dev)

        def far_copy(self, half):
            i = self.far + half
            return remote(part(self.buf.at[F], half), part(self.buf.at[X], half), i, i, self.devs[half])

        def send(self, group):
            for half in (0, 1):
                self.near_copy(group, half).start()
                sent.append((self.near_copy, group, half))

        def wait(self, group):
            for half in (0, 1):
                self.near_copy(group, half).wait_recv()

        def forward(self, half):
            self.near_copy(F, half).wait_recv()
            self.far_copy(half).start()
            sent.append((self.far_copy, half))

        def wait_far(self):
            for half in (0, 1):
                self.far_copy(half).wait_recv()

    agq, agst, agkv = Gather(qd, ydev), Gather(st, ydev), Gather(kv, zdev)
    with jax.named_scope('wait_row_q'):
        for s in range(ROW):
            row_wait(qd, xq, s)
            row_wait(st, xst, s)
    agq.send(F)
    agst.send(F)
    agq.send(G)
    agst.send(G)
    with jax.named_scope('wait_row_kv'):
        for s in range(ROW):
            row_wait(kv, xkv, s)
    agkv.send(F)
    agkv.send(G)

    src_id = lax.broadcasted_iota(jnp.int32, (ROW, DIM), 0)

    def assemble(group):
        for which in range(2):
            rows = st[group, :, which, :]
            for k in range(QROWS // DIM):
                mine = (((lane + k * DIM) * 1366) >> 16) == src_id
                line = jnp.sum(jnp.where(mine, rows, 0.0), axis=0, keepdims=True)
                ld[group, pl.ds(which, 1), pl.ds(k * DIM, DIM)] = line * LOG2E if which == 0 else line

    class Scatter:
        def __init__(self, acc, ra, rb, devs):
            self.acc, self.ra, self.rb, self.devs = acc, ra, rb, devs
            self.first = take(2)
            self.second = take(4)

        def far_copy(self, half):
            i = self.first + half
            return remote(part(self.acc(X), half), self.ra.at[half], i, i, self.devs[half])

        def early_copy(self, half):
            i = self.second + half
            return remote(part(self.acc(F), half), part(self.rb.at[1 - half], half), i, i, self.devs[1 - half])

        def late_copy(self, half):
            i = self.second + 2 + half
            return remote(part(self.acc(G), half), part(self.rb.at[half], half), i, i, self.devs[half])

        def start(self, make):
            for half in (0, 1):
                make(half).start()
                sent.append((make, half))

        def send_late(self):
            for half in (0, 1):
                self.far_copy(half).wait_recv()
                mine = part(self.acc(G), half)
                mine[...] = mine[...] + self.ra[half]
                self.late_copy(half).start()
                sent.append((self.late_copy, half))

        def total(self, half):
            self.early_copy(half).wait_recv()
            self.late_copy(half).wait_recv()
            return part(self.acc(OWN), half)[...] + part(self.rb.at[0], half)[...] + part(self.rb.at[1], half)[...]

    rsk = Scatter(lambda group: akv.at[group, 0], ra_kv.at[0], rb_kv.at[0], zdev)
    rsv = Scatter(lambda group: akv.at[group, 1], ra_kv.at[1], rb_kv.at[1], zdev)
    rsq = Scatter(lambda group: oq.at[group], ra_q, rb_q, ydev)

    half_rows = KROWS // 2
    key_row = lax.broadcasted_iota(jnp.int32, (half_rows, QROWS), 0)

    def block(qs, ks):
        q = qd[qs, :, pl.ds(0, GRP)].reshape(QROWS, DIM)
        g = qd[qs, :, pl.ds(GRP, GRP)].reshape(QROWS, DIM)
        k = kv[ks, :, 0].reshape(KROWS, DIM)
        v = kv[ks, :, 1].reshape(KROWS, DIM)
        lse = ld[qs, pl.ds(0, 1), :]
        dlt = ld[qs, pl.ds(1, 1), :]
        s_t = dot(k, q, NT)
        halves = []
        for half in (0, 1):
            first = ((z + offset(ks, half)) % RING) * 1024 + y * 256 + half * half_rows
            rows = s_t[half * half_rows:(half + 1) * half_rows]
            halves.append(jnp.where(key_row <= rowc[qs] - first, jnp.exp2(rows * (SCALE * LOG2E) - lse), 0.0))
        p_t = jnp.concatenate(halves, axis=0)
        dp_t = dot(v, g, NT)
        ds_t = (p_t * (dp_t - dlt)).astype(jnp.bfloat16)
        akv[ks, 1] = akv[ks, 1] + dot(p_t.astype(jnp.bfloat16), g, NN).reshape(ROW, KEYS, DIM)
        akv[ks, 0] = akv[ks, 0] + dot(ds_t, q, NN).reshape(ROW, KEYS, DIM)
        aqt[qs] = aqt[qs] + dot(k, ds_t, TN)

    def finish_q(group):
        oq[group] = aqt[group].T.reshape(ROW, PACK, DIM)

    def before_0():
        for half in (0, 1):
            agq.forward(half)
            agst.forward(half)
        for half in (0, 1):
            agkv.forward(half)
        assemble(F)

    def before_1():
        agkv.wait(G)

    def before_2():
        agq.wait(G)
        agst.wait(G)
        assemble(G)

    def before_4():
        agkv.wait_far()

    def before_5():
        agq.wait_far()
        agst.wait_far()
        assemble(X)

    def after_4():
        finish_q(OWN)
        finish_q(G)

    def after_5():
        rsv.start(rsv.far_copy)
        rsk.start(rsk.far_copy)
        finish_q(F)
        rsq.start(rsq.early_copy)

    def after_6():
        rsv.start(rsv.early_copy)

    before = {0: before_0, 1: before_1, 2: before_2, 4: before_4, 5: before_5}
    after = {4: after_4, 5: after_5, 6: after_6}
    pairs = (((OWN, F), (F, F)), ((F, OWN), (OWN, G)), ((F, G), (G, OWN)), ((G, F), (G, G)),
             ((G, X), (OWN, X)), ((F, X), (X, X)), ((X, F), (X, G)))

    def pick(i, values):
        out = values[-1]
        for n in range(len(values) - 1):
            out = jnp.where(i == n, values[n], out)
        return out

    def step(i, carry):
        for n, act in before.items():
            @pl.when(i == n)
            def _(n=n, act=act):
                with jax.named_scope(f'before_{n}'):
                    act()
        with jax.named_scope('pair'):
            for j in (0, 1):
                block(pick(i, [pair[j][0] for pair in pairs]), pick(i, [pair[j][1] for pair in pairs]))
        for n, act in after.items():
            @pl.when(i == n)
            def _(n=n, act=act):
                with jax.named_scope(f'after_{n}'):
                    act()
        return carry

    assemble(OWN)
    with jax.named_scope('first'):
        block(OWN, OWN)
    lax.fori_loop(0, len(pairs), step, 0)
    with jax.named_scope('last'):
        block(X, OWN)
    finish_q(X)
    rsq.start(rsq.far_copy)

    with jax.named_scope('late_v'):
        rsv.send_late()
    rsk.start(rsk.early_copy)
    with jax.named_scope('late_k'):
        rsk.send_late()
    with jax.named_scope('late_q'):
        rsq.send_late()

    fk_i, fv_i, fq_i = take(ROW), take(ROW), take(ROW)

    def give(src, dst, base, half):
        for s in range(half * HALF, (half + 1) * HALF):
            @pl.when(me != s)
            def _():
                remote(src.at[s], dst.at[me], base + s, base + me, row_dev(s)).start()

    own_k, own_v = akv.at[OWN, 0], akv.at[OWN, 1]
    for half in (0, 1):
        with jax.named_scope('total_v'):
            part(own_v, half)[...] = rsv.total(half)
        give(own_v, out_kv.at[1], fv_i, half)
    out_kv[1, me] = akv[OWN, 1, me]
    for half in (0, 1):
        with jax.named_scope('total_q'):
            fq[pl.ds(half * HALF, HALF)] = (rsq.total(half) * SCALE).astype(jnp.bfloat16)
        give(fq, out_q, fq_i, half)
    out_q[me] = fq[me]
    for half in (0, 1):
        with jax.named_scope('total_k'):
            part(own_k, half)[...] = rsk.total(half) * SCALE
        give(own_k, out_kv.at[0], fk_i, half)
    out_kv[0, me] = akv[OWN, 0, me]

    with jax.named_scope('drain'):
        row_wait_send(pq, qd, xq)
        row_wait_send(pst, st, xst)
        row_wait_send(pkv, kv, xkv)
        for make, *where in sent:
            make(*where).wait_send()
    for name, src, dst, base in (('v', own_v, out_kv.at[1], fv_i), ('q', fq, out_q, fq_i), ('k', own_k, out_kv.at[0], fk_i)):
        with jax.named_scope('final_' + name):
            for s in range(ROW):
                @pl.when(me != s)
                def _():
                    copy = remote(src.at[s], dst.at[s], base + s, base + s, row_dev(s))
                    copy.wait_send()
                    copy.wait_recv()


def relayout(q_ref, kv_ref, dq_ref, dk_ref, dv_ref, rows):
    for h in range(ROW):
        dk_ref[:, h, :] = kv_ref[0, h]
        dv_ref[:, h, :] = kv_ref[1, h]
        for g in range(GRP):
            rows[:, h * GRP + g, :] = q_ref[h, pl.ds(g * TOK, TOK), :].astype(jnp.float32)
    dq_ref[...] = rows[...].astype(jnp.bfloat16).reshape(dq_ref.shape)


def call(queries, attn_out, grad_out, log_sum_exp, key_cache, value_cache):
    f32, bf16 = jnp.float32, jnp.bfloat16
    vmem = pltpu.VMEM
    tok = (2, TOK // 2, ROW * GRP, DIM)
    key = (KEYS, ROW, DIM)
    scratch = [
        vmem(tok, bf16), vmem(tok, bf16), vmem(tok, bf16), vmem(tok[:3], f32), vmem(key, bf16), vmem(key, bf16),
        vmem((TOK, ROW * GRP, DIM), f32), vmem(key, f32), vmem((DIM, DIM), f32), vmem((DIM, DIM), f32),
        vmem((ROW, 2 * GRP, TOK, DIM), bf16), vmem((ROW, 2, DIM), f32), vmem((ROW, 2, KEYS, DIM), bf16),
        vmem((RING, ROW, 2 * GRP, TOK, DIM), bf16), vmem((RING, ROW, 2, DIM), f32), vmem((RING, ROW, 2, KEYS, DIM), bf16),
        vmem((RING, 8, QROWS), f32), vmem((RING, 1, QROWS), jnp.int32),
        vmem((RING, 2, ROW, KEYS, DIM), f32), vmem((RING, DIM, QROWS), f32), vmem((RING, ROW, PACK, DIM), f32),
        vmem((2, 2, HALF, KEYS, DIM), f32), vmem((2, 2, ROW, KEYS, DIM), f32),
        vmem((2, HALF, PACK, DIM), f32), vmem((2, ROW, PACK, DIM), f32),
        vmem((ROW, PACK, DIM), bf16),
        pltpu.SemaphoreType.DMA((6,)), pltpu.SemaphoreType.DMA((NSEM,)), pltpu.SemaphoreType.DMA((NSEM,)),
    ]
    out_q, out_kv = pl.pallas_call(
        kernel,
        out_shape=(jax.ShapeDtypeStruct((ROW, PACK, DIM), bf16),
                   jax.ShapeDtypeStruct((2, ROW, KEYS, DIM), f32)),
        in_specs=[pl.BlockSpec(memory_space=pl.ANY)] * 6,
        out_specs=[pl.BlockSpec(memory_space=pltpu.VMEM)] * 2,
        scratch_shapes=scratch,
        compiler_params=pltpu.CompilerParams(collective_id=0, has_side_effects=True),
        name='attn_bwd_3d',
    )(queries, attn_out, grad_out, log_sum_exp, key_cache, value_cache)
    return pl.pallas_call(
        relayout,
        out_shape=(jax.ShapeDtypeStruct(tok, bf16), jax.ShapeDtypeStruct(key, f32), jax.ShapeDtypeStruct(key, f32)),
        in_specs=[pl.BlockSpec(memory_space=pltpu.VMEM)] * 2,
        out_specs=[pl.BlockSpec(memory_space=pltpu.VMEM)] * 3,
        scratch_shapes=[vmem((TOK, ROW * GRP, DIM), f32)],
        name='relayout',
    )(out_q, out_kv)


def solution(mesh):
    row_spec = P(None, CP_AXES, 'heads', None)
    stat_spec = P(None, CP_AXES, 'heads')
    key_spec = P(CP_AXES, 'heads', None)
    return jax.shard_map(call, mesh=mesh, in_specs=(row_spec, row_spec, row_spec, stat_spec, key_spec, key_spec),
                         out_specs=(row_spec, key_spec, key_spec), check_vma=False)
```

```python
import jax
import jax.numpy as jnp
from jax import lax
from jax.experimental import pallas as pl
from jax.experimental.pallas import tpu as pltpu
from jax.sharding import PartitionSpec as P

CP_AXES = ('cpo', 'cp')
MESH = pl.DeviceIdType.MESH
LOG2E = 1.4426950408889634

ROW = 8
RING = 4
GRP = 3
TOK = 16
KEYS = 32
DIM = 128
HALF = ROW // 2
QROWS = ROW * GRP * TOK
KROWS = ROW * KEYS
PACK = GRP * TOK
SCALE = DIM ** -0.5
NSEM = 30
NSEND = 12
OWN, F, G, X = range(4)

NT = (((1,), (1,)), ((), ()))
NN = (((1,), (0,)), ((), ()))
TN = (((0,), (0,)), ((), ()))


def dot(a, b, dims):
    return lax.dot_general(a, b, dims, preferred_element_type=jnp.float32)


def kernel(q_in, o_in, g_in, l_in, k_in, v_in, out_q, out_kv,
           q_vm, o_vm, g_vm, l_vm, k_vm, v_vm, xs, xk, ts, tt,
           pq, pst, pkv, qd, st, kv, ld, rowc, akv, aqt, oq,
           ra_kv, rb_kv, ra_q, rb_q, fq, in_sem, ssem, rsem):
    me = lax.axis_index('cp')
    cpo = lax.axis_index('cpo')
    z, y = cpo // RING, cpo % RING

    def row_dev(j):
        return (0, cpo, j)

    def ring_devs(axis):
        if axis == 'y':
            return [(0, z * RING + (y + d) % RING, me) for d in (1, 3)]
        return [(0, ((z + d) % RING) * RING + y, me) for d in (1, 3)]

    ydev, zdev = ring_devs('y'), ring_devs('z')

    barrier = pltpu.get_barrier_semaphore()
    for j in range(1, ROW):
        pl.semaphore_signal(barrier, inc=1, device_id=row_dev((me + j) % ROW), device_id_type=MESH)
    for dev in ydev + zdev:
        pl.semaphore_signal(barrier, inc=1, device_id=dev, device_id_type=MESH)

    loads = [pltpu.make_async_copy(src, dst, in_sem.at[i]) for i, (src, dst) in enumerate(
        ((g_in, g_vm), (o_in, o_vm), (q_in, q_vm), (l_in, l_vm), (k_in, k_vm), (v_in, v_vm)))]
    for ld_copy in loads:
        ld_copy.start()

    counter = [0, 0]

    def take(n):
        first = counter[0]
        counter[0] += n
        assert counter[0] <= NSEM
        return first

    def take_send():
        counter[1] += 1
        assert counter[1] <= NSEND
        return counter[1] - 1

    def remote(src, dst, send_i, recv_i, dev):
        return pltpu.make_async_remote_copy(
            src_ref=src, dst_ref=dst, send_sem=ssem.at[send_i], recv_sem=rsem.at[recv_i],
            device_id=dev, device_id_type=MESH)

    def arrived(ref, recv_i):
        remote(ref, ref, 0, recv_i, row_dev(me)).wait_recv()

    sent = []

    loads[0].wait()
    loads[1].wait()
    gf = g_vm[...].reshape(TOK, ROW * GRP, DIM).astype(jnp.float32)
    xs[...] = gf
    of = o_vm[...].reshape(TOK, ROW * GRP, DIM).astype(jnp.float32)
    delta = jnp.sum(gf * of, axis=-1)
    ts[...] = jnp.zeros_like(ts)
    loads[3].wait()
    ts[pl.ds(0, TOK), pl.ds(0, ROW * GRP)] = l_vm[...].reshape(TOK, ROW * GRP)
    ts[pl.ds(TOK, TOK), pl.ds(0, ROW * GRP)] = delta
    for h in range(ROW):
        for g in range(GRP):
            pq[h, GRP + g] = xs[:, h * GRP + g, :].astype(jnp.bfloat16)
    loads[2].wait()
    xs[...] = q_vm[...].reshape(TOK, ROW * GRP, DIM).astype(jnp.float32)
    for h in range(ROW):
        for g in range(GRP):
            pq[h, g] = xs[:, h * GRP + g, :].astype(jnp.bfloat16)
    tt[...] = ts[...].T
    lane = lax.broadcasted_iota(jnp.int32, (ROW, DIM), 1)
    for which in range(2):
        packed = jnp.zeros((ROW, DIM), jnp.float32)
        for g in range(GRP):
            part = tt[pl.ds(g, ROW, stride=GRP), :]
            shift = (g * TOK - which * TOK) % DIM
            if shift:
                part = pltpu.roll(part, shift, 1)
            packed = jnp.where((lane >= g * TOK) & (lane < (g + 1) * TOK), part, packed)
        pst[:, which, :] = pltpu.roll(packed, (PACK * me) % DIM, 1)

    with jax.named_scope('barrier'):
        pl.semaphore_wait(barrier, ROW - 1 + 4)

    def row_send(src, dst):
        send_i, recv_i = take_send(), take(1)
        for j in (4, 5, 2, 3, 6, 7, 1):
            d = (me + j) % ROW
            remote(src.at[d], dst.at[me], send_i, recv_i, row_dev(d)).start()
        sent.append((send_i, src.at[pl.ds(0, ROW - 1)]))
        return lambda: arrived(dst.at[pl.ds(0, ROW - 1)], recv_i)

    row_q = row_send(pq, qd.at[OWN])
    row_st = row_send(pst, st.at[OWN])
    qd[OWN, me] = pq[me]
    st[OWN, me] = pst[me]

    loads[4].wait()
    xk[...] = k_vm[...].astype(jnp.float32)
    for h in range(ROW):
        pkv[h, 0] = xk[:, h, :].astype(jnp.bfloat16)
    loads[5].wait()
    xk[...] = v_vm[...].astype(jnp.float32)
    for h in range(ROW):
        pkv[h, 1] = xk[:, h, :].astype(jnp.bfloat16)
    row_kv = row_send(pkv, kv.at[OWN])
    kv[OWN, me] = pkv[me]

    akv[...] = jnp.zeros_like(akv)
    aqt[...] = jnp.zeros_like(aqt)

    def offset(group, half):
        near = (1, 3) if half else (3, 1)
        return jnp.where(group == F, near[0], jnp.where(group == G, near[1], jnp.where(group == X, 2, 0)))

    def part(ref, half):
        return ref.at[pl.ds(half * HALF, HALF)]

    r_id = lax.broadcasted_iota(jnp.int32, (1, QROWS), 1)
    token = ((r_id >> 3) & 1) * 1024 + ((r_id * 1366) >> 16) * 8 + (r_id & 7) + (2048 + z * 256)
    for group in range(RING):
        plane = jnp.where(r_id < QROWS // 2, (y + offset(group, 0)) % RING, (y + offset(group, 1)) % RING)
        rowc[group] = token + plane * 64

    class Gather:
        def __init__(self, buf, devs):
            self.buf, self.devs = buf, devs
            self.send_i, self.first, self.second, self.far = take_send(), take(2), take(1), take(1)
            sent.append((self.send_i, buf.at[pl.ds(0, RING - 1)]))

        def send(self, group):
            for half in (0, 1):
                dev = self.devs[half if group == F else 1 - half]
                recv_i = self.first + half if group == F else self.second
                remote(part(self.buf.at[OWN], half), part(self.buf.at[group], half), self.send_i, recv_i, dev).start()

        def forward(self, half):
            mine = part(self.buf.at[F], half)
            arrived(mine, self.first + half)
            remote(mine, part(self.buf.at[X], half), self.send_i, self.far, self.devs[half]).start()

        def wait_second(self):
            arrived(self.buf.at[G], self.second)

        def wait_far(self):
            arrived(self.buf.at[X], self.far)

    agq, agst, agkv = Gather(qd, ydev), Gather(st, ydev), Gather(kv, zdev)
    with jax.named_scope('wait_row_q'):
        row_q()
        row_st()
    agq.send(F)
    agst.send(F)
    agq.send(G)
    agst.send(G)
    with jax.named_scope('wait_row_kv'):
        row_kv()
    agkv.send(F)
    agkv.send(G)

    src_id = lax.broadcasted_iota(jnp.int32, (ROW, DIM), 0)

    def assemble(group):
        for which in range(2):
            rows = st[group, :, which, :]
            for k in range(QROWS // DIM):
                mine = (((lane + k * DIM) * 1366) >> 16) == src_id
                line = jnp.sum(jnp.where(mine, rows, 0.0), axis=0, keepdims=True)
                ld[group, pl.ds(which, 1), pl.ds(k * DIM, DIM)] = line * LOG2E if which == 0 else line

    class Scatter:
        def __init__(self, acc, ra, rb, devs):
            self.acc, self.ra, self.rb, self.devs = acc, ra, rb, devs
            self.send_i, self.first, self.near = take_send(), take(2), take(2)
            sent.append((self.send_i, acc.at[pl.ds(0, RING - 1)]))

        def send(self, group, half, dst, recv_i, dev):
            remote(part(self.acc.at[group], half), dst, self.send_i, recv_i, dev).start()

        def send_far(self):
            for half in (0, 1):
                self.send(X, half, self.ra.at[half], self.first + half, self.devs[half])

        def send_early(self):
            for half in (0, 1):
                self.send(F, half, part(self.rb.at[1 - half], half), self.near + half, self.devs[1 - half])

        def send_late(self):
            for half in (0, 1):
                arrived(self.ra.at[half], self.first + half)
                mine = part(self.acc.at[G], half)
                mine[...] = mine[...] + self.ra[half]
                self.send(G, half, part(self.rb.at[half], half), self.near + half, self.devs[half])

        def total(self, half):
            arrived(self.rb.at[0], self.near + half)
            return part(self.acc.at[OWN], half)[...] + part(self.rb.at[0], half)[...] + part(self.rb.at[1], half)[...]

    rsk = Scatter(akv.at[0], ra_kv.at[0], rb_kv.at[0], zdev)
    rsv = Scatter(akv.at[1], ra_kv.at[1], rb_kv.at[1], zdev)
    rsq = Scatter(oq, ra_q, rb_q, ydev)

    half_rows = KROWS // 2
    key_row = lax.broadcasted_iota(jnp.int32, (half_rows, QROWS), 0)

    def block(qs, ks):
        q = qd[qs, :, pl.ds(0, GRP)].reshape(QROWS, DIM)
        g = qd[qs, :, pl.ds(GRP, GRP)].reshape(QROWS, DIM)
        k = kv[ks, :, 0].reshape(KROWS, DIM)
        v = kv[ks, :, 1].reshape(KROWS, DIM)
        lse = ld[qs, pl.ds(0, 1), :]
        dlt = ld[qs, pl.ds(1, 1), :]
        s_t = dot(k, q, NT)
        halves = []
        for half in (0, 1):
            first = ((z + offset(ks, half)) % RING) * 1024 + y * 256 + half * half_rows
            rows = s_t[half * half_rows:(half + 1) * half_rows]
            halves.append(jnp.where(key_row <= rowc[qs] - first, jnp.exp2(rows * (SCALE * LOG2E) - lse), 0.0))
        p_t = jnp.concatenate(halves, axis=0)
        dp_t = dot(v, g, NT)
        ds_t = (p_t * (dp_t - dlt)).astype(jnp.bfloat16)
        akv[1, ks] = akv[1, ks] + dot(p_t.astype(jnp.bfloat16), g, NN).reshape(ROW, KEYS, DIM)
        akv[0, ks] = akv[0, ks] + dot(ds_t, q, NN).reshape(ROW, KEYS, DIM)
        aqt[qs] = aqt[qs] + dot(k, ds_t, TN)

    def finish_q(group):
        oq[group] = aqt[group].T.reshape(ROW, PACK, DIM)

    def before_0():
        for half in (0, 1):
            agq.forward(half)
            agst.forward(half)
        for half in (0, 1):
            agkv.forward(half)
        assemble(F)

    def before_1():
        agkv.wait_second()

    def before_2():
        agq.wait_second()
        agst.wait_second()
        assemble(G)

    def before_4():
        agkv.wait_far()

    def before_5():
        agq.wait_far()
        agst.wait_far()
        assemble(X)

    def after_4():
        finish_q(OWN)
        finish_q(G)

    def after_5():
        rsv.send_far()
        rsk.send_far()
        finish_q(F)
        rsq.send_early()

    def after_6():
        rsv.send_early()

    before = {0: before_0, 1: before_1, 2: before_2, 4: before_4, 5: before_5}
    after = {4: after_4, 5: after_5, 6: after_6}
    pairs = (((OWN, F), (F, F)), ((F, OWN), (OWN, G)), ((F, G), (G, OWN)), ((G, F), (G, G)),
             ((G, X), (OWN, X)), ((F, X), (X, X)), ((X, F), (X, G)))

    def pick(i, values):
        out = values[-1]
        for n in range(len(values) - 1):
            out = jnp.where(i == n, values[n], out)
        return out

    def step(i, carry):
        for n, act in before.items():
            @pl.when(i == n)
            def _(n=n, act=act):
                with jax.named_scope(f'before_{n}'):
                    act()
        with jax.named_scope('pair'):
            for j in (0, 1):
                block(pick(i, [pair[j][0] for pair in pairs]), pick(i, [pair[j][1] for pair in pairs]))
        for n, act in after.items():
            @pl.when(i == n)
            def _(n=n, act=act):
                with jax.named_scope(f'after_{n}'):
                    act()
        return carry

    assemble(OWN)
    with jax.named_scope('first'):
        block(OWN, OWN)
    lax.fori_loop(0, len(pairs), step, 0)
    with jax.named_scope('last'):
        block(X, OWN)
    finish_q(X)
    rsq.send_far()

    with jax.named_scope('late_v'):
        rsv.send_late()
    rsk.send_early()
    with jax.named_scope('late_k'):
        rsk.send_late()
    with jax.named_scope('late_q'):
        rsq.send_late()

    class Give:
        def __init__(self, src, dst):
            self.src, self.dst = src, dst
            self.send_i, self.recv_i = take_send(), take(1)
            sent.append((self.send_i, src.at[pl.ds(0, ROW - 1)]))

        def send(self, half):
            for s in range(half * HALF, (half + 1) * HALF):
                @pl.when(me != s)
                def _():
                    remote(self.src.at[s], self.dst.at[me], self.send_i, self.recv_i, row_dev(s)).start()

        def wait(self):
            arrived(self.dst.at[pl.ds(0, ROW - 1)], self.recv_i)

    own_k, own_v = akv.at[0, OWN], akv.at[1, OWN]
    give_k, give_v, give_q = Give(own_k, out_kv.at[0]), Give(own_v, out_kv.at[1]), Give(fq, out_q)
    for half in (0, 1):
        with jax.named_scope('total_v'):
            part(own_v, half)[...] = rsv.total(half)
        give_v.send(half)
    out_kv[1, me] = akv[1, OWN, me]
    for half in (0, 1):
        with jax.named_scope('total_q'):
            fq[pl.ds(half * HALF, HALF)] = (rsq.total(half) * SCALE).astype(jnp.bfloat16)
        give_q.send(half)
    out_q[me] = fq[me]
    for half in (0, 1):
        with jax.named_scope('total_k'):
            part(own_k, half)[...] = rsk.total(half) * SCALE
        give_k.send(half)
    out_kv[0, me] = akv[0, OWN, me]

    with jax.named_scope('drain'):
        for send_i, ref in sent:
            remote(ref, ref, send_i, 0, row_dev(me)).wait_send()
    with jax.named_scope('final_v'):
        give_v.wait()
    with jax.named_scope('final_q'):
        give_q.wait()
    with jax.named_scope('final_k'):
        give_k.wait()


def relayout(q_ref, kv_ref, dq_ref, dk_ref, dv_ref, rows):
    for h in range(ROW):
        dk_ref[:, h, :] = kv_ref[0, h]
        dv_ref[:, h, :] = kv_ref[1, h]
        for g in range(GRP):
            rows[:, h * GRP + g, :] = q_ref[h, pl.ds(g * TOK, TOK), :].astype(jnp.float32)
    dq_ref[...] = rows[...].astype(jnp.bfloat16).reshape(dq_ref.shape)


def call(queries, attn_out, grad_out, log_sum_exp, key_cache, value_cache):
    f32, bf16 = jnp.float32, jnp.bfloat16
    vmem = pltpu.VMEM
    tok = (2, TOK // 2, ROW * GRP, DIM)
    key = (KEYS, ROW, DIM)
    scratch = [
        vmem(tok, bf16), vmem(tok, bf16), vmem(tok, bf16), vmem(tok[:3], f32), vmem(key, bf16), vmem(key, bf16),
        vmem((TOK, ROW * GRP, DIM), f32), vmem(key, f32), vmem((DIM, DIM), f32), vmem((DIM, DIM), f32),
        vmem((ROW, 2 * GRP, TOK, DIM), bf16), vmem((ROW, 2, DIM), f32), vmem((ROW, 2, KEYS, DIM), bf16),
        vmem((RING, ROW, 2 * GRP, TOK, DIM), bf16), vmem((RING, ROW, 2, DIM), f32), vmem((RING, ROW, 2, KEYS, DIM), bf16),
        vmem((RING, 8, QROWS), f32), vmem((RING, 1, QROWS), jnp.int32),
        vmem((2, RING, ROW, KEYS, DIM), f32), vmem((RING, DIM, QROWS), f32), vmem((RING, ROW, PACK, DIM), f32),
        vmem((2, 2, HALF, KEYS, DIM), f32), vmem((2, 2, ROW, KEYS, DIM), f32),
        vmem((2, HALF, PACK, DIM), f32), vmem((2, ROW, PACK, DIM), f32),
        vmem((ROW, PACK, DIM), bf16),
        pltpu.SemaphoreType.DMA((6,)), pltpu.SemaphoreType.DMA((NSEND,)), pltpu.SemaphoreType.DMA((NSEM,)),
    ]
    out_q, out_kv = pl.pallas_call(
        kernel,
        out_shape=(vmem((ROW, PACK, DIM), bf16), vmem((2, ROW, KEYS, DIM), f32)),
        in_specs=[pl.BlockSpec(memory_space=pl.ANY)] * 6,
        out_specs=[pl.BlockSpec(memory_space=pltpu.VMEM)] * 2,
        scratch_shapes=scratch,
        compiler_params=pltpu.CompilerParams(collective_id=0, has_side_effects=True),
        name='attn_bwd_3d',
    )(queries, attn_out, grad_out, log_sum_exp, key_cache, value_cache)
    return pl.pallas_call(
        relayout,
        out_shape=(jax.ShapeDtypeStruct(tok, bf16), jax.ShapeDtypeStruct(key, f32), jax.ShapeDtypeStruct(key, f32)),
        in_specs=[pl.BlockSpec(memory_space=pltpu.VMEM)] * 2,
        out_specs=[pl.BlockSpec(memory_space=pltpu.VMEM)] * 3,
        scratch_shapes=[vmem((TOK, ROW * GRP, DIM), f32)],
        name='relayout',
    )(pltpu.with_memory_space_constraint(out_q, vmem), pltpu.with_memory_space_constraint(out_kv, vmem))


def solution(mesh):
    row_spec = P(None, CP_AXES, 'heads', None)
    stat_spec = P(None, CP_AXES, 'heads')
    key_spec = P(CP_AXES, 'heads', None)
    return jax.shard_map(call, mesh=mesh, in_specs=(row_spec, row_spec, row_spec, stat_spec, key_spec, key_spec),
                         out_specs=(row_spec, key_spec, key_spec), check_vma=False)
```

```python
import jax
import jax.numpy as jnp
from jax import lax
from jax.experimental import pallas as pl
from jax.experimental.pallas import tpu as pltpu
from jax.sharding import PartitionSpec as P

CP_AXES = ('cpo', 'cp')
MESH = pl.DeviceIdType.MESH
LOG2E = 1.4426950408889634

ROW = 8
RING = 4
GRP = 3
TOK = 16
KEYS = 32
DIM = 128
QROWS = ROW * GRP * TOK
KROWS = ROW * KEYS
PACK = GRP * TOK
SCALE = DIM ** -0.5
NSEM = 52
NSEND = 10
HOPS = RING

OWN, N1, N2, X = range(4)
GROUPS = (((0, 0), (0, 1), (0, 2), (0, 3)), ((-1, 0), (1, 0), (-1, 1), (1, 3)),
          ((-1, 3), (1, 2), (-1, 2), (1, 1)), ((2, 0), (2, 1), (2, 2), (2, 3)))
PLACE = {chunk: (group, slot) for group, chunks in enumerate(GROUPS) for slot, chunk in enumerate(chunks)}
VIA_PLUS = (2, 0)

NT = (((1,), (1,)), ((), ()))
NN = (((1,), (0,)), ((), ()))
TN = (((0,), (0,)), ((), ()))


def dot(a, b, dims):
    return lax.dot_general(a, b, dims, preferred_element_type=jnp.float32)


def kernel(q_in, o_in, g_in, l_in, k_in, v_in, out_q, out_kv,
           q_vm, o_vm, g_vm, l_vm, k_vm, v_vm, xs, xs2, xk, ts, tt,
           pq, pst, pkv, qd, st, kv, ld, rowc, akv, aqt, oq,
           ra_kv, rb_kv, ra_q, rb_q, fq, in_sem, ssem, rsem):
    me = lax.axis_index('cp')
    cpo = lax.axis_index('cpo')
    z, y = cpo // RING, cpo % RING
    x, core = me // 2, me % 2

    def row_dev(j):
        return (0, cpo, j)

    def ring_devs(axis):
        if axis == 'y':
            return [(0, z * RING + (y + d) % RING, me) for d in (1, 3)]
        return [(0, ((z + d) % RING) * RING + y, me) for d in (1, 3)]

    ydev, zdev = ring_devs('y'), ring_devs('z')

    barrier = pltpu.get_barrier_semaphore()
    for j in range(1, ROW):
        pl.semaphore_signal(barrier, inc=1, device_id=row_dev((me + j) % ROW), device_id_type=MESH)
    for dev in ydev + zdev:
        pl.semaphore_signal(barrier, inc=1, device_id=dev, device_id_type=MESH)

    loads = [pltpu.make_async_copy(src, dst, in_sem.at[i]) for i, (src, dst) in enumerate(
        ((g_in, g_vm), (o_in, o_vm), (q_in, q_vm), (l_in, l_vm), (k_in, k_vm), (v_in, v_vm)))]
    for ld_copy in loads:
        ld_copy.start()

    counter = [0, 0]

    def take(n):
        first = counter[0]
        counter[0] += n
        assert counter[0] <= NSEM
        return first

    def take_send():
        counter[1] += 1
        assert counter[1] <= NSEND
        return counter[1] - 1

    def remote(src, dst, send_i, recv_i, dev):
        return pltpu.make_async_remote_copy(
            src_ref=src, dst_ref=dst, send_sem=ssem.at[send_i], recv_sem=rsem.at[recv_i],
            device_id=dev, device_id_type=MESH)

    def arrived(ref, recv_i):
        remote(ref, ref, 0, recv_i, row_dev(me)).wait_recv()

    sent = []

    def chunk(ref, n, r):
        group, slot = PLACE[n, r]
        return ref.at[group, pl.ds(2 * slot, 2)]

    class Row:
        def __init__(self, src, dst):
            self.dst = dst
            self.recv = take(HOPS)
            send_i = take_send()
            sent.append((send_i, src.at[pl.ds(0, ROW - 1)]))
            for r in (1, 3, 2):
                for c in (0, 1):
                    self.send(src, send_i, r, c)
            self.send(src, send_i, 0, 1 - core)

        def send(self, src, send_i, r, c):
            back = (HOPS - r) % HOPS
            d = (x + r) % HOPS * 2 + c
            remote(src.at[d], self.dst.at[2 * back + core], send_i, self.recv + back, row_dev(d)).start()

        def wait(self, r):
            arrived(self.dst.at[pl.ds(0, 2 if r else 1)], self.recv + r)

    loads[0].wait()
    gf = g_vm[...].reshape(TOK, ROW * GRP, DIM).astype(jnp.float32)
    xs[...] = gf
    for h in range(ROW):
        for g in range(GRP):
            pq[h, GRP + g] = xs[:, h * GRP + g, :].astype(jnp.bfloat16)
    loads[2].wait()
    xs2[...] = q_vm[...].reshape(TOK, ROW * GRP, DIM).astype(jnp.float32)
    for h in range(ROW):
        for g in range(GRP):
            pq[h, g] = xs2[:, h * GRP + g, :].astype(jnp.bfloat16)
    with jax.named_scope('barrier'):
        pl.semaphore_wait(barrier, ROW - 1 + 4)
    row_q = Row(pq, qd.at[OWN])
    qd[OWN, core] = pq[me]

    loads[1].wait()
    delta = jnp.sum(xs[...] * o_vm[...].reshape(TOK, ROW * GRP, DIM).astype(jnp.float32), axis=-1)
    ts[...] = jnp.zeros_like(ts)
    loads[3].wait()
    ts[pl.ds(0, TOK), pl.ds(0, ROW * GRP)] = l_vm[...].reshape(TOK, ROW * GRP)
    ts[pl.ds(TOK, TOK), pl.ds(0, ROW * GRP)] = delta
    tt[...] = ts[...].T
    lane = lax.broadcasted_iota(jnp.int32, (ROW, DIM), 1)
    for which in range(2):
        packed = jnp.zeros((ROW, DIM), jnp.float32)
        for g in range(GRP):
            rows = tt[pl.ds(g, ROW, stride=GRP), :]
            shift = (g * TOK - which * TOK) % DIM
            if shift:
                rows = pltpu.roll(rows, shift, 1)
            packed = jnp.where((lane >= g * TOK) & (lane < (g + 1) * TOK), rows, packed)
        pst[:, which, :] = packed
    row_st = Row(pst, st.at[OWN])
    st[OWN, core] = pst[me]

    loads[4].wait()
    xk[...] = k_vm[...].astype(jnp.float32)
    for h in range(ROW):
        pkv[h, 0] = xk[:, h, :].astype(jnp.bfloat16)
    loads[5].wait()
    xk[...] = v_vm[...].astype(jnp.float32)
    for h in range(ROW):
        pkv[h, 1] = xk[:, h, :].astype(jnp.bfloat16)
    row_kv = Row(pkv, kv.at[OWN])
    kv[OWN, core] = pkv[me]

    class Gather:
        def __init__(self, buf, devs):
            self.buf, self.devs = buf, devs
            self.send_i, first, rest, self.far = take_send(), take(5), take(1), take(1)
            self.recv = {(-1, 0): first, (1, 0): first + 1, (-1, 1): first + 2, (1, 3): first + 3, (1, 2): first + 4}
            self.rest = rest
            sent.append((self.send_i, buf.at[pl.ds(0, RING - 1)]))

        def send(self, r, *sides):
            for side in sides:
                n = 1 if side else -1
                remote(chunk(self.buf, 0, r), chunk(self.buf, n, r), self.send_i, self.recv.get((n, r), self.rest),
                       self.devs[side]).start()

        def wait(self, n, r):
            arrived(chunk(self.buf, n, r), self.recv[n, r])

        def forward(self, n, r):
            self.wait(n, r)
            remote(chunk(self.buf, n, r), chunk(self.buf, 2, r), self.send_i, self.far, self.devs[0 if n < 0 else 1]).start()

        def wait_rest(self):
            arrived(self.buf.at[0, pl.ds(0, 6)], self.rest)

        def wait_far(self):
            arrived(self.buf.at[X], self.far)

    agst, agq, agkv = Gather(st, ydev), Gather(qd, ydev), Gather(kv, zdev)

    def pass_on(row, gather, r):
        row.wait(r)
        if row is row_q:
            pass_on(row_st, agst, r)
        if r == 0:
            gather.send(0, 0, 1)
        elif r == 1:
            gather.send(1, 0)
        elif r == 3:
            gather.send(3, 1, 0)
        else:
            gather.send(2, 1)
            gather.send(1, 1)
            gather.send(2, 0)

    with jax.named_scope('row_0'):
        pass_on(row_q, agq, 0)
        pass_on(row_kv, agkv, 0)

    r_id = lax.broadcasted_iota(jnp.int32, (1, QROWS), 1)
    packet = (r_id * 1366) >> 16
    token = ((r_id >> 3) & 1) * 1024 + (packet & 1) * 8 + (r_id & 7) + (2048 + z * 256)
    for group in range(RING):
        spot = jnp.zeros_like(token)
        for slot, (n, r) in enumerate(GROUPS[group]):
            spot = jnp.where((packet >> 1) == slot, (y + n) % RING * 64 + (x + r) % HOPS * 16, spot)
        rowc[group] = token + spot

    src_id = (3 * lax.broadcasted_iota(jnp.int32, (ROW, DIM), 0)) & 7

    def assemble(group):
        for which in range(2):
            rows = []
            for i in range(ROW):
                rows.append(st[group, pl.ds(3 * i % ROW, 1), which, :])
            rows = pltpu.roll(jnp.concatenate(rows, axis=0), 0, 1, stride=TOK, stride_axis=0)
            for k in range(QROWS // DIM):
                mine = (((lane + k * DIM) * 1366) >> 16) == src_id
                line = jnp.sum(jnp.where(mine, rows, 0.0), axis=0, keepdims=True)
                ld[group, pl.ds(which, 1), pl.ds(k * DIM, DIM)] = line * LOG2E if which == 0 else line

    class Scatter:
        def __init__(self, acc, ra, rb, devs):
            self.acc, self.ra, self.rb, self.devs = acc, ra, rb, devs
            self.send_i, self.first, self.near = take_send(), take(HOPS), take(HOPS)
            sent.append((self.send_i, acc.at[pl.ds(0, RING - 1)]))

        def send_far(self, r):
            side = 0 if r in VIA_PLUS else 1
            remote(chunk(self.acc, 2, r), self.ra.at[r], self.send_i, self.first + r, self.devs[side]).start()

        def send_near(self, side, r):
            remote(chunk(self.acc, -1 if side else 1, r), self.rb.at[side, r], self.send_i, self.near + r, self.devs[side]).start()

        def send_early(self, r):
            self.send_near(1 if r in VIA_PLUS else 0, r)

        def send_late(self, r):
            side = 0 if r in VIA_PLUS else 1
            arrived(self.ra.at[r], self.first + r)
            mine = chunk(self.acc, -1 if side else 1, r)
            mine[...] = mine[...] + self.ra[r]
            self.send_near(side, r)

        def total(self, r):
            arrived(self.rb.at[0, pl.ds(0, 2)], self.near + r)
            return chunk(self.acc, 0, r)[...] + self.rb[0, r] + self.rb[1, r]

    rskv, rsq = Scatter(akv, ra_kv, rb_kv, zdev), Scatter(oq, ra_q, rb_q, ydev)

    band_rows = KROWS // HOPS
    key_row = lax.broadcasted_iota(jnp.int32, (band_rows, QROWS), 0)
    begun = set()

    def add(ref, name, value):
        ref[...] = ref[...] + value if name in begun else value
        begun.add(name)

    def tile(qs, ks):
        with jax.named_scope('tile' + ''.join(map(str, qs)) + 'x' + ''.join(map(str, ks))):
            q = jnp.concatenate([qd[i, :, pl.ds(0, GRP)].reshape(QROWS, DIM) for i in qs], axis=0)
            g = jnp.concatenate([qd[i, :, pl.ds(GRP, GRP)].reshape(QROWS, DIM) for i in qs], axis=0)
            k = jnp.concatenate([kv[i, :, 0].reshape(KROWS, DIM) for i in ks], axis=0)
            v = jnp.concatenate([kv[i, :, 1].reshape(KROWS, DIM) for i in ks], axis=0)
            lse = jnp.concatenate([ld[i, pl.ds(0, 1), :] for i in qs], axis=1)
            dlt = jnp.concatenate([ld[i, pl.ds(1, 1), :] for i in qs], axis=1)
            expo = jnp.exp2(dot(k, q, NT) * (SCALE * LOG2E) - lse)
            bands = []
            for n, r in [at for i in ks for at in GROUPS[i]]:
                first = (z + n) % RING * 1024 + y * 256 + (x + r) % HOPS * band_rows
                seen = jnp.concatenate([key_row <= rowc[i] - first for i in qs], axis=1)
                at = len(bands) * band_rows
                bands.append(jnp.where(seen, expo[at:at + band_rows], 0.0))
            p_t = jnp.concatenate(bands, axis=0)
            dp_t = dot(v, g, NT)
            ds_t = (p_t * (dp_t - dlt)).astype(jnp.bfloat16)
            dv = dot(p_t.astype(jnp.bfloat16), g, NN)
            dk = dot(ds_t, q, NN)
            dq = dot(k, ds_t, TN)
            for n, i in enumerate(ks):
                add(akv.at[i, :, 1], ('v', i), dv[n * KROWS:(n + 1) * KROWS].reshape(ROW, KEYS, DIM))
                add(akv.at[i, :, 0], ('k', i), dk[n * KROWS:(n + 1) * KROWS].reshape(ROW, KEYS, DIM))
            for n, i in enumerate(qs):
                add(aqt.at[i], ('q', i), dq[:, n * QROWS:(n + 1) * QROWS])

    def finish_q(group):
        oq[group] = aqt[group].T.reshape(ROW, PACK, DIM)

    for r in (1, 3, 2):
        with jax.named_scope(f'row_{r}'):
            pass_on(row_q, agq, r)
    for r in (1, 3, 2):
        with jax.named_scope(f'row_kv{r}'):
            pass_on(row_kv, agkv, r)
    assemble(OWN)
    tile([OWN], [OWN])
    def forward_q(n, r):
        agst.forward(n, r)
        agq.forward(n, r)

    with jax.named_scope('fwd_0'):
        forward_q(-1, 0)
        agkv.forward(-1, 0)
    with jax.named_scope('fwd_q1'):
        forward_q(-1, 1)
        forward_q(1, 3)
        agst.wait(1, 0)
        agq.wait(1, 0)
        assemble(N1)
    tile([N1], [OWN])
    with jax.named_scope('fwd_k1'):
        agkv.forward(-1, 1)
        agkv.forward(1, 3)
    with jax.named_scope('fwd_q2'):
        forward_q(1, 2)
    with jax.named_scope('fwd_k2'):
        agkv.forward(1, 2)
        agkv.wait(1, 0)
    tile([OWN, N1], [N1])
    with jax.named_scope('rest_q'):
        agst.wait_rest()
        agq.wait_rest()
        assemble(N2)
    tile([N2], [OWN, N1])
    with jax.named_scope('rest_k'):
        agkv.wait_rest()
    tile([OWN, N1], [N2])
    tile([N2], [N2])
    with jax.named_scope('far_k'):
        agkv.wait_far()
    tile([OWN, N1], [X])
    tile([N2], [X])
    with jax.named_scope('far_q'):
        agst.wait_far()
        agq.wait_far()
        assemble(X)
    tile([X], [X])
    for r in (2, 1, 0, 3):
        rskv.send_far(r)
    tile([X], [N1, N2])
    rskv.send_early(1)
    rskv.send_early(2)
    with jax.named_scope('finish'):
        finish_q(N1)
        finish_q(N2)
    for r in (1, 2, 3, 0):
        rsq.send_early(r)
    tile([X], [OWN])
    finish_q(X)
    for r in (2, 1, 0, 3):
        rsq.send_far(r)
    finish_q(OWN)
    for name, scatter, late, early in (('kv', rskv, (2, 1), (3, 0)), ('q', rsq, (2, 1), ()), ('kv', rskv, (3, 0), ()), ('q', rsq, (3, 0), ())):
        with jax.named_scope(f'late_{name}{late[0]}'):
            for r in late:
                scatter.send_late(r)
        for r in early:
            scatter.send_early(r)

    class Give:
        def __init__(self, src, dst):
            self.src, self.dst = src, dst
            self.send_i, self.recv_i = take_send(), take(1)
            sent.append((self.send_i, src.at[pl.ds(0, ROW - 1)]))

        def send(self, r):
            for c in ((0, 1) if r else (1 - core,)):
                d = (x + r) % HOPS * 2 + c
                remote(self.src.at[2 * r + c], self.dst.at[me], self.send_i, self.recv_i, row_dev(d)).start()

        def wait(self):
            arrived(self.dst.at[pl.ds(0, ROW - 1)], self.recv_i)

    give_kv, give_q = Give(akv.at[OWN], out_kv), Give(fq, out_q)

    def total_kv(r):
        with jax.named_scope(f'total_kv{r}'):
            tot = rskv.total(r)
            akv[OWN, pl.ds(2 * r, 2), 0] = tot[:, 0] * SCALE
            akv[OWN, pl.ds(2 * r, 2), 1] = tot[:, 1]
        give_kv.send(r)

    def total_q(r):
        with jax.named_scope(f'total_q{r}'):
            fq[pl.ds(2 * r, 2)] = (rsq.total(r) * SCALE).astype(jnp.bfloat16)
        give_q.send(r)

    total_kv(2)
    total_kv(1)
    total_q(2)
    total_q(1)
    total_kv(3)
    total_q(3)
    total_q(0)
    total_kv(0)
    out_q[me] = fq[core]
    out_kv[me] = akv[OWN, core]

    with jax.named_scope('final_q'):
        give_q.wait()
    with jax.named_scope('final_kv'):
        give_kv.wait()
    with jax.named_scope('drain'):
        for send_i, ref in sent:
            remote(ref, ref, send_i, 0, row_dev(me)).wait_send()


def relayout(q_ref, kv_ref, dq_ref, dk_ref, dv_ref, rows):
    for h in range(ROW):
        dk_ref[:, h, :] = kv_ref[h, 0]
        dv_ref[:, h, :] = kv_ref[h, 1]
        for g in range(GRP):
            rows[:, h * GRP + g, :] = q_ref[h, pl.ds(g * TOK, TOK), :].astype(jnp.float32)
    dq_ref[...] = rows[...].astype(jnp.bfloat16).reshape(dq_ref.shape)


def call(queries, attn_out, grad_out, log_sum_exp, key_cache, value_cache):
    f32, bf16 = jnp.float32, jnp.bfloat16
    vmem = pltpu.VMEM
    tok = (2, TOK // 2, ROW * GRP, DIM)
    key = (KEYS, ROW, DIM)
    scratch = [
        vmem(tok, bf16), vmem(tok, bf16), vmem(tok, bf16), vmem(tok[:3], f32), vmem(key, bf16), vmem(key, bf16),
        vmem((TOK, ROW * GRP, DIM), f32), vmem((TOK, ROW * GRP, DIM), f32), vmem(key, f32), vmem((DIM, DIM), f32), vmem((DIM, DIM), f32),
        vmem((ROW, 2 * GRP, TOK, DIM), bf16), vmem((ROW, 2, DIM), f32), vmem((ROW, 2, KEYS, DIM), bf16),
        vmem((RING, ROW, 2 * GRP, TOK, DIM), bf16), vmem((RING, ROW, 2, DIM), f32), vmem((RING, ROW, 2, KEYS, DIM), bf16),
        vmem((RING, 8, QROWS), f32), vmem((RING, 1, QROWS), jnp.int32),
        vmem((RING, ROW, 2, KEYS, DIM), f32), vmem((RING, DIM, QROWS), f32), vmem((RING, ROW, PACK, DIM), f32),
        vmem((HOPS, 2, 2, KEYS, DIM), f32), vmem((2, HOPS, 2, 2, KEYS, DIM), f32),
        vmem((HOPS, 2, PACK, DIM), f32), vmem((2, HOPS, 2, PACK, DIM), f32),
        vmem((ROW, PACK, DIM), bf16),
        pltpu.SemaphoreType.DMA((6,)), pltpu.SemaphoreType.DMA((NSEND,)), pltpu.SemaphoreType.DMA((NSEM,)),
    ]
    out_q, out_kv = pl.pallas_call(
        kernel,
        out_shape=(vmem((ROW, PACK, DIM), bf16), vmem((ROW, 2, KEYS, DIM), f32)),
        in_specs=[pl.BlockSpec(memory_space=pl.ANY)] * 6,
        out_specs=[pl.BlockSpec(memory_space=pltpu.VMEM)] * 2,
        scratch_shapes=scratch,
        compiler_params=pltpu.CompilerParams(collective_id=0, has_side_effects=True),
        name='attn_bwd_3d',
    )(queries, attn_out, grad_out, log_sum_exp, key_cache, value_cache)
    return pl.pallas_call(
        relayout,
        out_shape=(jax.ShapeDtypeStruct(tok, bf16), jax.ShapeDtypeStruct(key, f32), jax.ShapeDtypeStruct(key, f32)),
        in_specs=[pl.BlockSpec(memory_space=pltpu.VMEM)] * 2,
        out_specs=[pl.BlockSpec(memory_space=pltpu.VMEM)] * 3,
        scratch_shapes=[vmem((TOK, ROW * GRP, DIM), f32)],
        name='relayout',
    )(pltpu.with_memory_space_constraint(out_q, vmem), pltpu.with_memory_space_constraint(out_kv, vmem))


def solution(mesh):
    row_spec = P(None, CP_AXES, 'heads', None)
    stat_spec = P(None, CP_AXES, 'heads')
    key_spec = P(CP_AXES, 'heads', None)
    return jax.shard_map(call, mesh=mesh, in_specs=(row_spec, row_spec, row_spec, stat_spec, key_spec, key_spec),
                         out_specs=(row_spec, key_spec, key_spec), check_vma=False)
```

```python
import jax
import jax.numpy as jnp
from jax import lax
from jax.experimental import pallas as pl
from jax.experimental.pallas import tpu as pltpu
from jax.sharding import PartitionSpec as P

CP_AXES = ('cpo', 'cp')
MESH = pl.DeviceIdType.MESH
LOG2E = 1.4426950408889634

ROW = 8
RING = 4
GRP = 3
TOK = 16
KEYS = 32
DIM = 128
QROWS = ROW * GRP * TOK
KROWS = ROW * KEYS
PACK = GRP * TOK
SCALE = DIM ** -0.5
NSEM = 60
NSEND = 12
HOPS = RING

OWN, N1, N2, X = range(4)
GROUPS = (((0, 0), (0, 1), (0, 2), (0, 3)), ((-1, 0), (1, 0), (-1, 1), (1, 3)),
          ((-1, 3), (1, 2), (-1, 2), (1, 1)), ((2, 0), (2, 1), (2, 2), (2, 3)))
PLACE = {chunk: (group, slot) for group, chunks in enumerate(GROUPS) for slot, chunk in enumerate(chunks)}
DIRECT_KV = True
VIA_PLUS = (2, 0)

NT = (((1,), (1,)), ((), ()))
NN = (((1,), (0,)), ((), ()))
TN = (((0,), (0,)), ((), ()))


def dot(a, b, dims):
    return lax.dot_general(a, b, dims, preferred_element_type=jnp.float32)


def kernel(q_in, o_in, g_in, l_in, k_in, v_in, out_q, out_kv,
           q_vm, o_vm, g_vm, l_vm, k_vm, v_vm, xs, xs2, xk, ts, tt,
           pq, pst, pkv, qd, st, kv, ld, rowc, akv, aqt, oq,
           ra_kv, rb_kv, ra_q, rb_q, fq, in_sem, ssem, rsem):
    me = lax.axis_index('cp')
    cpo = lax.axis_index('cpo')
    z, y = cpo // RING, cpo % RING
    x, core = me // 2, me % 2

    def row_dev(j):
        return (0, cpo, j)

    def ring_devs(axis):
        if axis == 'y':
            return [(0, z * RING + (y + d) % RING, me) for d in (1, 3, 2)]
        return [(0, ((z + d) % RING) * RING + y, me) for d in (1, 3, 2)]

    ydev, zdev = ring_devs('y'), ring_devs('z')

    barrier = pltpu.get_barrier_semaphore()
    for j in range(1, ROW):
        pl.semaphore_signal(barrier, inc=1, device_id=row_dev((me + j) % ROW), device_id_type=MESH)
    for dev in ydev + zdev:
        pl.semaphore_signal(barrier, inc=1, device_id=dev, device_id_type=MESH)

    loads = [pltpu.make_async_copy(src, dst, in_sem.at[i]) for i, (src, dst) in enumerate(
        ((g_in, g_vm), (o_in, o_vm), (q_in, q_vm), (l_in, l_vm), (k_in, k_vm), (v_in, v_vm)))]
    for ld_copy in loads:
        ld_copy.start()

    counter = [0, 0]

    def take(n):
        first = counter[0]
        counter[0] += n
        assert counter[0] <= NSEM
        return first

    def take_send():
        counter[1] += 1
        assert counter[1] <= NSEND
        return counter[1] - 1

    def remote(src, dst, send_i, recv_i, dev):
        return pltpu.make_async_remote_copy(
            src_ref=src, dst_ref=dst, send_sem=ssem.at[send_i], recv_sem=rsem.at[recv_i],
            device_id=dev, device_id_type=MESH)

    def arrived(ref, recv_i):
        remote(ref, ref, 0, recv_i, row_dev(me)).wait_recv()

    sent = []

    def chunk(ref, n, r):
        group, slot = PLACE[n, r]
        return ref.at[group, pl.ds(2 * slot, 2)]

    class Row:
        def __init__(self, src, dst):
            self.dst = dst
            self.recv = take(HOPS)
            send_i = take_send()
            sent.append((send_i, src.at[pl.ds(0, ROW - 1)]))
            for r in (1, 3, 2):
                for c in (0, 1):
                    self.send(src, send_i, r, c)
            self.send(src, send_i, 0, 1 - core)

        def send(self, src, send_i, r, c):
            back = (HOPS - r) % HOPS
            d = (x + r) % HOPS * 2 + c
            remote(src.at[d], self.dst.at[2 * back + core], send_i, self.recv + back, row_dev(d)).start()

        def wait(self, r):
            arrived(self.dst.at[pl.ds(0, 2 if r else 1)], self.recv + r)

    with jax.named_scope('pack_q'):
        loads[0].wait()
        gf = g_vm[...].reshape(TOK, ROW * GRP, DIM).astype(jnp.float32)
        xs[...] = gf
        for h in range(ROW):
            for g in range(GRP):
                pq[h, GRP + g] = xs[:, h * GRP + g, :].astype(jnp.bfloat16)
        loads[2].wait()
        xs2[...] = q_vm[...].reshape(TOK, ROW * GRP, DIM).astype(jnp.float32)
        for h in range(ROW):
            for g in range(GRP):
                pq[h, g] = xs2[:, h * GRP + g, :].astype(jnp.bfloat16)
    with jax.named_scope('barrier'):
        pl.semaphore_wait(barrier, ROW - 1 + 6)
    row_q = Row(pq, qd.at[OWN])
    qd[OWN, core] = pq[me]

    with jax.named_scope('stats'):
        loads[1].wait()
        delta = jnp.sum(xs[...] * o_vm[...].reshape(TOK, ROW * GRP, DIM).astype(jnp.float32), axis=-1)
        ts[...] = jnp.zeros_like(ts)
        loads[3].wait()
        ts[pl.ds(0, TOK), pl.ds(0, ROW * GRP)] = l_vm[...].reshape(TOK, ROW * GRP)
        ts[pl.ds(TOK, TOK), pl.ds(0, ROW * GRP)] = delta
        tt[...] = ts[...].T
        lane = lax.broadcasted_iota(jnp.int32, (ROW, DIM), 1)
        for which in range(2):
            packed = jnp.zeros((ROW, DIM), jnp.float32)
            for g in range(GRP):
                rows = tt[pl.ds(g, ROW, stride=GRP), :]
                shift = (g * TOK - which * TOK) % DIM
                if shift:
                    rows = pltpu.roll(rows, shift, 1)
                packed = jnp.where((lane >= g * TOK) & (lane < (g + 1) * TOK), rows, packed)
            pst[:, which, :] = packed
    row_st = Row(pst, st.at[OWN])
    st[OWN, core] = pst[me]

    with jax.named_scope('pack_kv'):
        loads[4].wait()
        xk[...] = k_vm[...].astype(jnp.float32)
        for h in range(ROW):
            pkv[h, 0] = xk[:, h, :].astype(jnp.bfloat16)
        loads[5].wait()
        xk[...] = v_vm[...].astype(jnp.float32)
        for h in range(ROW):
            pkv[h, 1] = xk[:, h, :].astype(jnp.bfloat16)
    row_kv = Row(pkv, kv.at[OWN])
    kv[OWN, core] = pkv[me]

    class Gather:
        def __init__(self, buf, devs, direct=False):
            self.buf, self.devs, self.direct = buf, devs, direct
            self.recv = {at: take(1) for at in ((-1, 0), (1, 0), (-1, 1), (1, 3)) + (() if direct else ((1, 2),))}
            self.send_i, self.rest, self.far = take_send(), take(1), take(1)
            sent.append((self.send_i, buf.at[pl.ds(0, RING - 1)]))

        def send(self, r, *sides):
            for side in sides:
                n = (-1, 1, 2)[side]
                recv_i = self.far if side == 2 else self.recv.get((n, r), self.rest)
                remote(chunk(self.buf, 0, r), chunk(self.buf, n, r), self.send_i, recv_i, self.devs[side]).start()

        def wait(self, n, r):
            arrived(chunk(self.buf, n, r), self.recv[n, r])

        def forward(self, n, r):
            self.wait(n, r)
            remote(chunk(self.buf, n, r), chunk(self.buf, 2, r), self.send_i, self.far, self.devs[0 if n < 0 else 1]).start()

        def wait_rest(self):
            arrived(self.buf.at[0, pl.ds(0, 8 if self.direct else 6)], self.rest)

        def wait_far(self):
            arrived(self.buf.at[X], self.far)

    agst, agq, agkv = Gather(st, ydev), Gather(qd, ydev), Gather(kv, zdev, DIRECT_KV)

    def pass_on(row, gather, r):
        row.wait(r)
        if row is row_q:
            pass_on(row_st, agst, r)
        if r == 0:
            gather.send(0, 0, 1)
        elif r == 1:
            gather.send(1, 0)
        elif r == 3:
            gather.send(3, 1, 0)
        elif gather.direct:
            gather.send(2, 1, 0)
            gather.send(1, 1)
            gather.send(2, 2)
        else:
            gather.send(2, 1)
            gather.send(1, 1)
            gather.send(2, 0)

    with jax.named_scope('row_0'):
        pass_on(row_q, agq, 0)
        pass_on(row_kv, agkv, 0)

    r_id = lax.broadcasted_iota(jnp.int32, (1, QROWS), 1)
    packet = (r_id * 1366) >> 16
    token = ((r_id >> 3) & 1) * 1024 + (packet & 1) * 8 + (r_id & 7) + (2048 + z * 256)
    for group in range(RING):
        spot = jnp.zeros_like(token)
        for slot, (n, r) in enumerate(GROUPS[group]):
            spot = jnp.where((packet >> 1) == slot, (y + n) % RING * 64 + (x + r) % HOPS * 16, spot)
        rowc[group] = token + spot

    src_id = (3 * lax.broadcasted_iota(jnp.int32, (ROW, DIM), 0)) & 7

    def assemble(group):
        for which in range(2):
            rows = []
            for i in range(ROW):
                rows.append(st[group, pl.ds(3 * i % ROW, 1), which, :])
            rows = pltpu.roll(jnp.concatenate(rows, axis=0), 0, 1, stride=TOK, stride_axis=0)
            for k in range(QROWS // DIM):
                mine = (((lane + k * DIM) * 1366) >> 16) == src_id
                line = jnp.sum(jnp.where(mine, rows, 0.0), axis=0, keepdims=True)
                ld[group, pl.ds(which, 1), pl.ds(k * DIM, DIM)] = line * LOG2E if which == 0 else line

    class Scatter:
        def __init__(self, acc, ra, rb, devs):
            self.acc, self.ra, self.rb, self.devs = acc, ra, rb, devs
            self.send_i, self.first, self.near = take_send(), take(HOPS), take(HOPS)
            sent.append((self.send_i, acc.at[pl.ds(0, RING - 1)]))

        def send_far(self, r):
            side = 0 if r in VIA_PLUS else 1
            remote(chunk(self.acc, 2, r), self.ra.at[r], self.send_i, self.first + r, self.devs[side]).start()

        def send_near(self, side, r):
            remote(chunk(self.acc, -1 if side else 1, r), self.rb.at[side, r], self.send_i, self.near + r, self.devs[side]).start()

        def send_early(self, r):
            self.send_near(1 if r in VIA_PLUS else 0, r)

        def send_late(self, r):
            side = 0 if r in VIA_PLUS else 1
            arrived(self.ra.at[r], self.first + r)
            mine = chunk(self.acc, -1 if side else 1, r)
            mine[...] = mine[...] + self.ra[r]
            self.send_near(side, r)

        def total(self, r):
            arrived(self.rb.at[0, pl.ds(0, 2)], self.near + r)
            return chunk(self.acc, 0, r)[...] + self.rb[0, r] + self.rb[1, r]

    rsk, rsv = (Scatter(akv.at[i], ra_kv.at[i], rb_kv.at[i], zdev) for i in (0, 1))
    rsq = Scatter(oq, ra_q, rb_q, ydev)

    band_rows = KROWS // HOPS
    key_row = lax.broadcasted_iota(jnp.int32, (band_rows, QROWS), 0)
    begun = set()

    def add(ref, name, value):
        ref[...] = ref[...] + value if name in begun else value
        begun.add(name)

    def tile(qs, ks):
        with jax.named_scope('tile' + ''.join(map(str, qs)) + 'x' + ''.join(map(str, ks))):
            q = jnp.concatenate([qd[i, :, pl.ds(0, GRP)].reshape(QROWS, DIM) for i in qs], axis=0)
            g = jnp.concatenate([qd[i, :, pl.ds(GRP, GRP)].reshape(QROWS, DIM) for i in qs], axis=0)
            k = jnp.concatenate([kv[i, :, 0].reshape(KROWS, DIM) for i in ks], axis=0)
            v = jnp.concatenate([kv[i, :, 1].reshape(KROWS, DIM) for i in ks], axis=0)
            lse = jnp.concatenate([ld[i, pl.ds(0, 1), :] for i in qs], axis=1)
            dlt = jnp.concatenate([ld[i, pl.ds(1, 1), :] for i in qs], axis=1)
            expo = jnp.exp2(dot(k, q, NT) * (SCALE * LOG2E) - lse)
            bands = []
            for n, r in [at for i in ks for at in GROUPS[i]]:
                first = (z + n) % RING * 1024 + y * 256 + (x + r) % HOPS * band_rows
                seen = jnp.concatenate([key_row <= rowc[i] - first for i in qs], axis=1)
                at = len(bands) * band_rows
                bands.append(jnp.where(seen, expo[at:at + band_rows], 0.0))
            p_t = jnp.concatenate(bands, axis=0)
            dp_t = dot(v, g, NT)
            ds_t = (p_t * (dp_t - dlt)).astype(jnp.bfloat16)
            dv = dot(p_t.astype(jnp.bfloat16), g, NN)
            dk = dot(ds_t, q, NN)
            dq = dot(k, ds_t, TN)
            for n, i in enumerate(ks):
                add(akv.at[1, i], ('v', i), dv[n * KROWS:(n + 1) * KROWS].reshape(ROW, KEYS, DIM))
                add(akv.at[0, i], ('k', i), dk[n * KROWS:(n + 1) * KROWS].reshape(ROW, KEYS, DIM))
            for n, i in enumerate(qs):
                add(aqt.at[i], ('q', i), dq[:, n * QROWS:(n + 1) * QROWS])

    def finish_q(group):
        oq[group] = aqt[group].T.reshape(ROW, PACK, DIM)

    for r in (1, 3, 2):
        with jax.named_scope(f'row_{r}'):
            pass_on(row_q, agq, r)
    for r in (1, 3, 2):
        with jax.named_scope(f'row_kv{r}'):
            pass_on(row_kv, agkv, r)
    assemble(OWN)
    tile([OWN], [OWN])
    def forward_q(n, r):
        agst.forward(n, r)
        agq.forward(n, r)

    with jax.named_scope('fwd_0'):
        forward_q(-1, 0)
        agkv.forward(-1, 0)
    with jax.named_scope('fwd_q1'):
        forward_q(-1, 1)
        forward_q(1, 3)
        agst.wait(1, 0)
        agq.wait(1, 0)
        assemble(N1)
    tile([N1], [OWN])
    with jax.named_scope('fwd_k1'):
        agkv.forward(-1, 1)
        agkv.forward(1, 3)
    with jax.named_scope('fwd_q2'):
        forward_q(1, 2)
    with jax.named_scope('fwd_k2'):
        if not DIRECT_KV:
            agkv.forward(1, 2)
        agkv.wait(1, 0)
    tile([OWN, N1], [N1])
    with jax.named_scope('rest_k'):
        agkv.wait_rest()
    tile([OWN, N1], [N2])
    with jax.named_scope('rest_q'):
        agst.wait_rest()
        agq.wait_rest()
        assemble(N2)
    tile([N2], [OWN, N1, N2])
    with jax.named_scope('far_k'):
        agkv.wait_far()
    tile([OWN, N1, N2], [X])
    with jax.named_scope('far_q'):
        agst.wait_far()
        agq.wait_far()
        assemble(X)
    tile([X], [X])
    for pair in ((2, 1), (0, 3)):
        for scatter in (rsv, rsk):
            for r in pair:
                scatter.send_far(r)
    tile([X], [N1, N2, OWN])
    finish_q(X)
    for r in (2, 1, 0, 3):
        rsq.send_far(r)
    for scatter in (rsv, rsk):
        scatter.send_early(1)
        scatter.send_early(2)
    with jax.named_scope('finish'):
        finish_q(N1)
        finish_q(N2)
    for r in (1, 2, 3, 0):
        rsq.send_early(r)
    finish_q(OWN)

    def late(name, scatter, *chunks):
        with jax.named_scope(f'late_{name}{chunks[0]}'):
            for r in chunks:
                scatter.send_late(r)

    class Give:
        def __init__(self, src, dst):
            self.src, self.dst = src, dst
            self.send_i, self.recv_i = take_send(), take(1)
            sent.append((self.send_i, src.at[pl.ds(0, ROW - 1)]))

        def send(self, r):
            for c in ((0, 1) if r else (1 - core,)):
                d = (x + r) % HOPS * 2 + c
                remote(self.src.at[2 * r + c], self.dst.at[me], self.send_i, self.recv_i, row_dev(d)).start()

        def wait(self):
            arrived(self.dst.at[pl.ds(0, ROW - 1)], self.recv_i)

    give_k, give_v, give_q = Give(akv.at[0, OWN], out_kv.at[0]), Give(akv.at[1, OWN], out_kv.at[1]), Give(fq, out_q)

    def total(name, r):
        part = pl.ds(2 * r, 2)
        with jax.named_scope(f'total_{name}{r}'):
            if name == 'v':
                akv[1, OWN, part] = rsv.total(r)
            elif name == 'k':
                akv[0, OWN, part] = rsk.total(r) * SCALE
            else:
                fq[part] = (rsq.total(r) * SCALE).astype(jnp.bfloat16)
        {'v': give_v, 'k': give_k, 'q': give_q}[name].send(r)

    late('v', rsv, 2, 1)
    late('k', rsk, 2, 1)
    rsv.send_early(3)
    rsk.send_early(3)
    late('v', rsv, 3)
    late('k', rsk, 3)
    late('v', rsv, 0)
    late('k', rsk, 0)
    rsv.send_early(0)
    rsk.send_early(0)
    late('q', rsq, 2, 1)
    total('v', 2)
    total('v', 1)
    late('q', rsq, 3, 0)
    for name, r in (('k', 2), ('k', 1), ('v', 3), ('k', 3), ('q', 2), ('q', 1), ('q', 3), ('v', 0), ('k', 0), ('q', 0)):
        total(name, r)
    out_q[me] = fq[core]
    out_kv[0, me] = akv[0, OWN, core]
    out_kv[1, me] = akv[1, OWN, core]

    with jax.named_scope('final_q'):
        give_q.wait()
    with jax.named_scope('final_kv'):
        give_v.wait()
        give_k.wait()
    with jax.named_scope('drain'):
        for send_i, ref in sent:
            remote(ref, ref, send_i, 0, row_dev(me)).wait_send()


def relayout(q_ref, kv_ref, dq_ref, dk_ref, dv_ref, rows):
    for h in range(ROW):
        dk_ref[:, h, :] = kv_ref[0, h]
        dv_ref[:, h, :] = kv_ref[1, h]
        for g in range(GRP):
            rows[:, h * GRP + g, :] = q_ref[h, pl.ds(g * TOK, TOK), :].astype(jnp.float32)
    dq_ref[...] = rows[...].astype(jnp.bfloat16).reshape(dq_ref.shape)


def call(queries, attn_out, grad_out, log_sum_exp, key_cache, value_cache):
    f32, bf16 = jnp.float32, jnp.bfloat16
    vmem = pltpu.VMEM
    tok = (2, TOK // 2, ROW * GRP, DIM)
    key = (KEYS, ROW, DIM)
    scratch = [
        vmem(tok, bf16), vmem(tok, bf16), vmem(tok, bf16), vmem(tok[:3], f32), vmem(key, bf16), vmem(key, bf16),
        vmem((TOK, ROW * GRP, DIM), f32), vmem((TOK, ROW * GRP, DIM), f32), vmem(key, f32), vmem((DIM, DIM), f32), vmem((DIM, DIM), f32),
        vmem((ROW, 2 * GRP, TOK, DIM), bf16), vmem((ROW, 2, DIM), f32), vmem((ROW, 2, KEYS, DIM), bf16),
        vmem((RING, ROW, 2 * GRP, TOK, DIM), bf16), vmem((RING, ROW, 2, DIM), f32), vmem((RING, ROW, 2, KEYS, DIM), bf16),
        vmem((RING, 8, QROWS), f32), vmem((RING, 1, QROWS), jnp.int32),
        vmem((2, RING, ROW, KEYS, DIM), f32), vmem((RING, DIM, QROWS), f32), vmem((RING, ROW, PACK, DIM), f32),
        vmem((2, HOPS, 2, KEYS, DIM), f32), vmem((2, 2, HOPS, 2, KEYS, DIM), f32),
        vmem((HOPS, 2, PACK, DIM), f32), vmem((2, HOPS, 2, PACK, DIM), f32),
        vmem((ROW, PACK, DIM), bf16),
        pltpu.SemaphoreType.DMA((6,)), pltpu.SemaphoreType.DMA((NSEND,)), pltpu.SemaphoreType.DMA((NSEM,)),
    ]
    out_q, out_kv = pl.pallas_call(
        kernel,
        out_shape=(vmem((ROW, PACK, DIM), bf16), vmem((2, ROW, KEYS, DIM), f32)),
        in_specs=[pl.BlockSpec(memory_space=pl.ANY)] * 6,
        out_specs=[pl.BlockSpec(memory_space=pltpu.VMEM)] * 2,
        scratch_shapes=scratch,
        compiler_params=pltpu.CompilerParams(collective_id=0, has_side_effects=True),
        name='attn_bwd_3d',
    )(queries, attn_out, grad_out, log_sum_exp, key_cache, value_cache)
    return pl.pallas_call(
        relayout,
        out_shape=(jax.ShapeDtypeStruct(tok, bf16), jax.ShapeDtypeStruct(key, f32), jax.ShapeDtypeStruct(key, f32)),
        in_specs=[pl.BlockSpec(memory_space=pltpu.VMEM)] * 2,
        out_specs=[pl.BlockSpec(memory_space=pltpu.VMEM)] * 3,
        scratch_shapes=[vmem((TOK, ROW * GRP, DIM), f32)],
        name='relayout',
    )(pltpu.with_memory_space_constraint(out_q, vmem), pltpu.with_memory_space_constraint(out_kv, vmem))


def solution(mesh):
    row_spec = P(None, CP_AXES, 'heads', None)
    stat_spec = P(None, CP_AXES, 'heads')
    key_spec = P(CP_AXES, 'heads', None)
    return jax.shard_map(call, mesh=mesh, in_specs=(row_spec, row_spec, row_spec, stat_spec, key_spec, key_spec),
                         out_specs=(row_spec, key_spec, key_spec), check_vma=False)
```

```python
import jax
import jax.numpy as jnp
from jax import lax
from jax.experimental import pallas as pl
from jax.experimental.pallas import tpu as pltpu
from jax.sharding import PartitionSpec as P

CP_AXES = ('cpo', 'cp')
MESH = pl.DeviceIdType.MESH
LOG2E = 1.4426950408889634

ROW = 8
RING = 4
GRP = 3
TOK = 16
KEYS = 32
DIM = 128
QROWS = ROW * GRP * TOK
KROWS = ROW * KEYS
PACK = GRP * TOK
SCALE = DIM ** -0.5
NSEM = 60
NSEND = 12
HOPS = RING

OWN, N1, N2, X = range(4)
GROUPS = (((0, 0), (0, 1), (0, 2), (0, 3)), ((-1, 0), (1, 0), (-1, 1), (1, 3)),
          ((-1, 3), (1, 2), (-1, 2), (1, 1)), ((2, 0), (2, 1), (2, 2), (2, 3)))
PLACE = {chunk: (group, slot) for group, chunks in enumerate(GROUPS) for slot, chunk in enumerate(chunks)}
DIRECT_KV = True
VIA_PLUS = (2, 0)

NT = (((1,), (1,)), ((), ()))
NN = (((1,), (0,)), ((), ()))
TN = (((0,), (0,)), ((), ()))


def dot(a, b, dims):
    return lax.dot_general(a, b, dims, preferred_element_type=jnp.float32)


def kernel(q_in, o_in, g_in, l_in, k_in, v_in, out_q, out_kv,
           q_vm, o_vm, g_vm, l_vm, k_vm, v_vm, perm_q, perm_kv, ts, tt,
           pq, pst, pkv, qd, st, kv, ld, rowc, akv, aqt, oq,
           ra_kv, rb_kv, ra_q, rb_q, fq, in_sem, ssem, rsem):
    me = lax.axis_index('cp')
    cpo = lax.axis_index('cpo')
    z, y = cpo // RING, cpo % RING
    x, core = me // 2, me % 2

    def row_dev(j):
        return (0, cpo, j)

    def along(n, queries):
        n = n % RING
        y_step = (core == 0) == queries
        return jnp.where(y_step, z, (z + n) % RING), jnp.where(y_step, (y + n) % RING, y)

    def ring_devs(queries):
        devs = []
        for n in (1, -1, 2):
            zn, yn = along(n, queries)
            devs.append((0, zn * RING + yn, me))
        return devs

    qdev, kdev = ring_devs(True), ring_devs(False)

    loads = [pltpu.make_async_copy(src, dst, in_sem.at[i]) for i, (src, dst) in enumerate(
        ((g_in, g_vm), (q_in, q_vm), (k_in, k_vm), (v_in, v_vm), (o_in, o_vm), (l_in, l_vm)))]
    for ld_copy in loads:
        ld_copy.start()

    barrier = pltpu.get_barrier_semaphore()
    for j in range(1, ROW):
        pl.semaphore_signal(barrier, inc=1, device_id=row_dev((me + j) % ROW), device_id_type=MESH)
    for dev in qdev + kdev:
        pl.semaphore_signal(barrier, inc=1, device_id=dev, device_id_type=MESH)

    counter = [0, 0]

    def take(n):
        first = counter[0]
        counter[0] += n
        assert counter[0] <= NSEM
        return first

    def take_send():
        counter[1] += 1
        assert counter[1] <= NSEND
        return counter[1] - 1

    def remote(src, dst, send_i, recv_i, dev):
        return pltpu.make_async_remote_copy(
            src_ref=src, dst_ref=dst, send_sem=ssem.at[send_i], recv_sem=rsem.at[recv_i],
            device_id=dev, device_id_type=MESH)

    def arrived(ref, recv_i):
        remote(ref, ref, 0, recv_i, row_dev(me)).wait_recv()

    sent = []

    def chunk(ref, n, r):
        group, slot = PLACE[n, r]
        return ref.at[group, pl.ds(2 * slot, 2)]

    class Row:
        def __init__(self, src, dst):
            self.dst = dst
            self.recv = take(HOPS)
            send_i = take_send()
            sent.append((send_i, src.at[pl.ds(0, ROW - 1)]))
            for r in (1, 3, 2):
                for c in (0, 1):
                    self.send(src, send_i, r, c)
            self.send(src, send_i, 0, 1 - core)

        def send(self, src, send_i, r, c):
            back = (HOPS - r) % HOPS
            d = (x + r) % HOPS * 2 + c
            remote(src.at[d], self.dst.at[2 * back + core], send_i, self.recv + back, row_dev(d)).start()

        def wait(self, r):
            arrived(self.dst.at[pl.ds(0, 2 if r else 1)], self.recv + r)

    def permutation(ref, tokens, heads):
        n = tokens * heads
        i = lax.broadcasted_iota(jnp.int32, (n, n), 0)
        source = (i & (tokens - 1)) * heads + (i >> (tokens.bit_length() - 1))
        ref[...] = (lax.broadcasted_iota(jnp.int32, (n, n), 1) == source).astype(jnp.float32).astype(jnp.bfloat16)

    permutation(perm_q, TOK, ROW * GRP)
    permutation(perm_kv, KEYS, ROW)
    ts[...] = jnp.zeros_like(ts)
    with jax.named_scope('loads'):
        for load in loads:
            load.wait()
    with jax.named_scope('pack'):
        prod = g_vm[...].astype(jnp.float32) * o_vm[...].astype(jnp.float32)
        delta = jnp.sum(prod.reshape(TOK, ROW * GRP, DIM), axis=-1)
        ts[pl.ds(0, TOK), pl.ds(0, ROW * GRP)] = l_vm[...].reshape(TOK, ROW * GRP)
        ts[pl.ds(TOK, TOK), pl.ds(0, ROW * GRP)] = delta
        tt[...] = ts[...].T
        rows = dot(perm_q[...], jnp.concatenate([q_vm[...], g_vm[...]], axis=1), NN).astype(jnp.bfloat16)
        for i in (0, 1):
            pq[:, pl.ds(i * GRP, GRP)] = rows[:, i * DIM:(i + 1) * DIM].reshape(ROW, GRP, TOK, DIM)
        rows = dot(perm_kv[...], jnp.concatenate([k_vm[...], v_vm[...]], axis=1), NN).astype(jnp.bfloat16)
        for i in (0, 1):
            pkv[:, i] = rows[:, i * DIM:(i + 1) * DIM].reshape(ROW, KEYS, DIM)
        lane = lax.broadcasted_iota(jnp.int32, (ROW, DIM), 1)
        for which in range(2):
            packed = jnp.zeros((ROW, DIM), jnp.float32)
            for g in range(GRP):
                rows = tt[pl.ds(g, ROW, stride=GRP), :]
                shift = (g * TOK - which * TOK) % DIM
                if shift:
                    rows = pltpu.roll(rows, shift, 1)
                packed = jnp.where((lane >= g * TOK) & (lane < (g + 1) * TOK), rows, packed)
            pst[:, which, :] = packed
    with jax.named_scope('barrier'):
        pl.semaphore_wait(barrier, ROW - 1 + 6)
    row_st = Row(pst, st.at[OWN])
    st[OWN, core] = pst[me]
    row_q = Row(pq, qd.at[OWN])
    qd[OWN, core] = pq[me]
    row_kv = Row(pkv, kv.at[OWN])
    kv[OWN, core] = pkv[me]

    class Gather:
        def __init__(self, buf, devs, direct=False):
            self.buf, self.devs, self.direct = buf, devs, direct
            self.recv = {at: take(1) for at in ((-1, 0), (1, 0), (-1, 1), (1, 3)) + (() if direct else ((1, 2),))}
            self.send_i, self.rest, self.far = take_send(), take(1), take(1)
            sent.append((self.send_i, buf.at[pl.ds(0, RING - 1)]))

        def send(self, r, *sides):
            for side in sides:
                n = (-1, 1, 2)[side]
                recv_i = self.far if side == 2 else self.recv.get((n, r), self.rest)
                remote(chunk(self.buf, 0, r), chunk(self.buf, n, r), self.send_i, recv_i, self.devs[side]).start()

        def wait(self, n, r):
            arrived(chunk(self.buf, n, r), self.recv[n, r])

        def forward(self, n, r):
            self.wait(n, r)
            remote(chunk(self.buf, n, r), chunk(self.buf, 2, r), self.send_i, self.far, self.devs[0 if n < 0 else 1]).start()

        def wait_rest(self):
            arrived(self.buf.at[0, pl.ds(0, 8 if self.direct else 6)], self.rest)

        def wait_far(self):
            arrived(self.buf.at[X], self.far)

    agst, agq, agkv = Gather(st, qdev), Gather(qd, qdev), Gather(kv, kdev, DIRECT_KV)

    def pass_on(row, gather, r):
        row.wait(r)
        if row is row_q:
            pass_on(row_st, agst, r)
        if r == 0:
            gather.send(0, 0, 1)
        elif r == 1:
            gather.send(1, 0)
        elif r == 3:
            gather.send(3, 1, 0)
        elif gather.direct:
            gather.send(2, 1, 0)
            gather.send(1, 1)
            gather.send(2, 2)
        else:
            gather.send(2, 1)
            gather.send(1, 1)
            gather.send(2, 0)

    with jax.named_scope('row_0'):
        pass_on(row_q, agq, 0)
        pass_on(row_kv, agkv, 0)

    r_id = lax.broadcasted_iota(jnp.int32, (1, QROWS), 1)
    packet = (r_id * 1366) >> 16
    token = ((r_id >> 3) & 1) * 1024 + (packet & 1) * 8 + (r_id & 7) + 2048
    for group in range(RING):
        spot = jnp.zeros_like(token)
        for slot, (n, r) in enumerate(GROUPS[group]):
            zq, yq = along(n, True)
            spot = jnp.where((packet >> 1) == slot, zq * 256 + yq * 64 + (x + r) % HOPS * 16, spot)
        rowc[group] = token + spot

    src_id = (3 * lax.broadcasted_iota(jnp.int32, (ROW, DIM), 0)) & 7

    def assemble(group):
        for which in range(2):
            rows = []
            for i in range(ROW):
                rows.append(st[group, pl.ds(3 * i % ROW, 1), which, :])
            rows = pltpu.roll(jnp.concatenate(rows, axis=0), 0, 1, stride=TOK, stride_axis=0)
            for k in range(QROWS // DIM):
                mine = (((lane + k * DIM) * 1366) >> 16) == src_id
                line = jnp.sum(jnp.where(mine, rows, 0.0), axis=0, keepdims=True)
                ld[group, pl.ds(which, 1), pl.ds(k * DIM, DIM)] = line * LOG2E if which == 0 else line

    class Scatter:
        def __init__(self, acc, ra, rb, devs):
            self.acc, self.ra, self.rb, self.devs = acc, ra, rb, devs
            self.send_i, self.first, self.near = take_send(), take(HOPS), take(HOPS)
            sent.append((self.send_i, acc.at[pl.ds(0, RING - 1)]))

        def send_far(self, r):
            side = 0 if r in VIA_PLUS else 1
            remote(chunk(self.acc, 2, r), self.ra.at[r], self.send_i, self.first + r, self.devs[side]).start()

        def send_near(self, side, r):
            remote(chunk(self.acc, -1 if side else 1, r), self.rb.at[side, r], self.send_i, self.near + r, self.devs[side]).start()

        def send_early(self, r):
            self.send_near(1 if r in VIA_PLUS else 0, r)

        def send_late(self, r):
            side = 0 if r in VIA_PLUS else 1
            arrived(self.ra.at[r], self.first + r)
            mine = chunk(self.acc, -1 if side else 1, r)
            mine[...] = mine[...] + self.ra[r]
            self.send_near(side, r)

        def total(self, r):
            arrived(self.rb.at[0, pl.ds(0, 2)], self.near + r)
            return chunk(self.acc, 0, r)[...] + self.rb[0, r] + self.rb[1, r]

    rsk, rsv = (Scatter(akv.at[i], ra_kv.at[i], rb_kv.at[i], kdev) for i in (0, 1))
    rsq = Scatter(oq, ra_q, rb_q, qdev)

    band_rows = KROWS // HOPS
    key_row = lax.broadcasted_iota(jnp.int32, (band_rows, QROWS), 0)
    begun = set()

    def add(ref, name, value):
        ref[...] = ref[...] + value if name in begun else value
        begun.add(name)

    def tile(qs, ks):
        with jax.named_scope('tile' + ''.join(map(str, qs)) + 'x' + ''.join(map(str, ks))):
            q = jnp.concatenate([qd[i, :, pl.ds(0, GRP)].reshape(QROWS, DIM) for i in qs], axis=0)
            g = jnp.concatenate([qd[i, :, pl.ds(GRP, GRP)].reshape(QROWS, DIM) for i in qs], axis=0)
            k = jnp.concatenate([kv[i, :, 0].reshape(KROWS, DIM) for i in ks], axis=0)
            v = jnp.concatenate([kv[i, :, 1].reshape(KROWS, DIM) for i in ks], axis=0)
            lse = jnp.concatenate([ld[i, pl.ds(0, 1), :] for i in qs], axis=1)
            dlt = jnp.concatenate([ld[i, pl.ds(1, 1), :] for i in qs], axis=1)
            expo = jnp.exp2(dot(k, q, NT) * (SCALE * LOG2E) - lse)
            bands = []
            for n, r in [at for i in ks for at in GROUPS[i]]:
                zk, yk = along(n, False)
                first = zk * 1024 + yk * 256 + (x + r) % HOPS * band_rows
                seen = jnp.concatenate([key_row <= rowc[i] - first for i in qs], axis=1)
                at = len(bands) * band_rows
                bands.append(jnp.where(seen, expo[at:at + band_rows], 0.0))
            p_t = jnp.concatenate(bands, axis=0)
            dp_t = dot(v, g, NT)
            ds_t = (p_t * (dp_t - dlt)).astype(jnp.bfloat16)
            dv = dot(p_t.astype(jnp.bfloat16), g, NN)
            dk = dot(ds_t, q, NN)
            dq = dot(k, ds_t, TN)
            for n, i in enumerate(ks):
                add(akv.at[1, i], ('v', i), dv[n * KROWS:(n + 1) * KROWS].reshape(ROW, KEYS, DIM))
                add(akv.at[0, i], ('k', i), dk[n * KROWS:(n + 1) * KROWS].reshape(ROW, KEYS, DIM))
            for n, i in enumerate(qs):
                add(aqt.at[i], ('q', i), dq[:, n * QROWS:(n + 1) * QROWS])

    def finish_q(group):
        oq[group] = aqt[group].T.reshape(ROW, PACK, DIM)

    for r in (1, 3, 2):
        with jax.named_scope(f'row_{r}'):
            pass_on(row_q, agq, r)
    for r in (1, 3, 2):
        with jax.named_scope(f'row_kv{r}'):
            pass_on(row_kv, agkv, r)
    assemble(OWN)
    tile([OWN], [OWN])
    def forward_q(n, r):
        agst.forward(n, r)
        agq.forward(n, r)

    with jax.named_scope('fwd_0'):
        forward_q(-1, 0)
        agkv.forward(-1, 0)
    with jax.named_scope('fwd_q1'):
        forward_q(-1, 1)
        forward_q(1, 3)
        agst.wait(1, 0)
        agq.wait(1, 0)
        assemble(N1)
    tile([N1], [OWN])
    with jax.named_scope('fwd_k1'):
        agkv.forward(-1, 1)
        agkv.forward(1, 3)
    with jax.named_scope('fwd_q2'):
        forward_q(1, 2)
    with jax.named_scope('fwd_k2'):
        if not DIRECT_KV:
            agkv.forward(1, 2)
        agkv.wait(1, 0)
    tile([OWN, N1], [N1])
    with jax.named_scope('rest_q'):
        agst.wait_rest()
        agq.wait_rest()
        assemble(N2)
    tile([N2], [OWN, N1])
    with jax.named_scope('rest_k'):
        agkv.wait_rest()
    tile([OWN, N1, N2], [N2])
    with jax.named_scope('far_k'):
        agkv.wait_far()
    tile([OWN, N1, N2], [X])
    with jax.named_scope('far_q'):
        agst.wait_far()
        agq.wait_far()
        assemble(X)
    tile([X], [X])
    for pair in ((2, 1), (0, 3)):
        for scatter in (rsv, rsk):
            for r in pair:
                scatter.send_far(r)
    tile([X], [N1, N2, OWN])
    finish_q(X)
    for r in (2, 1, 0, 3):
        rsq.send_far(r)
    for scatter in (rsv, rsk):
        scatter.send_early(1)
        scatter.send_early(2)
    with jax.named_scope('finish'):
        finish_q(N1)
        finish_q(N2)
    rsq.send_early(1)
    rsq.send_early(2)
    finish_q(OWN)

    def late(name, scatter, *chunks):
        with jax.named_scope(f'late_{name}{chunks[0]}'):
            for r in chunks:
                scatter.send_late(r)

    class Give:
        def __init__(self, src, dst):
            self.src, self.dst = src, dst
            self.send_i, self.recv_i = take_send(), take(1)
            sent.append((self.send_i, src.at[pl.ds(0, ROW - 1)]))

        def send(self, r):
            for c in ((0, 1) if r else (1 - core,)):
                d = (x + r) % HOPS * 2 + c
                remote(self.src.at[2 * r + c], self.dst.at[me], self.send_i, self.recv_i, row_dev(d)).start()

        def wait(self):
            arrived(self.dst.at[pl.ds(0, ROW - 1)], self.recv_i)

    give_k, give_v, give_q = Give(akv.at[0, OWN], out_kv.at[0]), Give(akv.at[1, OWN], out_kv.at[1]), Give(fq, out_q)

    def total(name, r):
        part = pl.ds(2 * r, 2)
        with jax.named_scope(f'total_{name}{r}'):
            if name == 'v':
                akv[1, OWN, part] = rsv.total(r)
            elif name == 'k':
                akv[0, OWN, part] = rsk.total(r) * SCALE
            else:
                fq[part] = (rsq.total(r) * SCALE).astype(jnp.bfloat16)
        {'v': give_v, 'k': give_k, 'q': give_q}[name].send(r)

    late('v', rsv, 2, 1)
    late('k', rsk, 2, 1)
    rsv.send_early(3)
    rsk.send_early(3)
    late('v', rsv, 3)
    late('k', rsk, 3)
    late('q', rsq, 2, 1)
    rsq.send_early(3)
    late('q', rsq, 3)
    late('v', rsv, 0)
    late('k', rsk, 0)
    rsv.send_early(0)
    rsk.send_early(0)
    late('q', rsq, 0)
    rsq.send_early(0)
    for name, r in (('v', 2), ('k', 2), ('v', 1), ('k', 1)):
        total(name, r)
    pl.when(core == 0)(lambda: total('q', 2))
    total('v', 3)
    total('k', 3)
    pl.when(core == 1)(lambda: total('q', 2))
    for name, r in (('q', 1), ('q', 3), ('v', 0), ('k', 0), ('q', 0)):
        total(name, r)
    out_q[me] = fq[core]
    out_kv[0, me] = akv[0, OWN, core]
    out_kv[1, me] = akv[1, OWN, core]

    with jax.named_scope('final_q'):
        give_q.wait()
    with jax.named_scope('final_kv'):
        give_v.wait()
        give_k.wait()
    with jax.named_scope('drain'):
        for send_i, ref in sent:
            remote(ref, ref, send_i, 0, row_dev(me)).wait_send()


def relayout(q_ref, kv_ref, dq_ref, dk_ref, dv_ref, rows):
    for h in range(ROW):
        dk_ref[:, h, :] = kv_ref[0, h]
        dv_ref[:, h, :] = kv_ref[1, h]
        for g in range(GRP):
            rows[:, h * GRP + g, :] = q_ref[h, pl.ds(g * TOK, TOK), :].astype(jnp.float32)
    dq_ref[...] = rows[...].astype(jnp.bfloat16).reshape(dq_ref.shape)


def call(queries, attn_out, grad_out, log_sum_exp, key_cache, value_cache):
    f32, bf16 = jnp.float32, jnp.bfloat16
    vmem = pltpu.VMEM
    tok = (2, TOK // 2, ROW * GRP, DIM)
    key = (KEYS, ROW, DIM)
    tok2, key2 = (QROWS, DIM), (KROWS, DIM)
    scratch = [
        vmem(tok2, bf16), vmem(tok2, bf16), vmem(tok2, bf16), vmem(tok[:3], f32), vmem(key2, bf16), vmem(key2, bf16),
        vmem((QROWS, QROWS), bf16), vmem((KROWS, KROWS), bf16), vmem((DIM, DIM), f32), vmem((DIM, DIM), f32),
        vmem((ROW, 2 * GRP, TOK, DIM), bf16), vmem((ROW, 2, DIM), f32), vmem((ROW, 2, KEYS, DIM), bf16),
        vmem((RING, ROW, 2 * GRP, TOK, DIM), bf16), vmem((RING, ROW, 2, DIM), f32), vmem((RING, ROW, 2, KEYS, DIM), bf16),
        vmem((RING, 8, QROWS), f32), vmem((RING, 1, QROWS), jnp.int32),
        vmem((2, RING, ROW, KEYS, DIM), f32), vmem((RING, DIM, QROWS), f32), vmem((RING, ROW, PACK, DIM), f32),
        vmem((2, HOPS, 2, KEYS, DIM), f32), vmem((2, 2, HOPS, 2, KEYS, DIM), f32),
        vmem((HOPS, 2, PACK, DIM), f32), vmem((2, HOPS, 2, PACK, DIM), f32),
        vmem((ROW, PACK, DIM), bf16),
        pltpu.SemaphoreType.DMA((6,)), pltpu.SemaphoreType.DMA((NSEND,)), pltpu.SemaphoreType.DMA((NSEM,)),
    ]
    out_q, out_kv = pl.pallas_call(
        kernel,
        out_shape=(vmem((ROW, PACK, DIM), bf16), vmem((2, ROW, KEYS, DIM), f32)),
        in_specs=[pl.BlockSpec(memory_space=pl.ANY)] * 6,
        out_specs=[pl.BlockSpec(memory_space=pltpu.VMEM)] * 2,
        scratch_shapes=scratch,
        compiler_params=pltpu.CompilerParams(collective_id=0, has_side_effects=True),
        name='attn_bwd_3d',
    )(queries.reshape(tok2), attn_out.reshape(tok2), grad_out.reshape(tok2), log_sum_exp,
      key_cache.reshape(key2), value_cache.reshape(key2))
    return pl.pallas_call(
        relayout,
        out_shape=(jax.ShapeDtypeStruct(tok, bf16), jax.ShapeDtypeStruct(key, f32), jax.ShapeDtypeStruct(key, f32)),
        in_specs=[pl.BlockSpec(memory_space=pltpu.VMEM)] * 2,
        out_specs=[pl.BlockSpec(memory_space=pltpu.VMEM)] * 3,
        scratch_shapes=[vmem((TOK, ROW * GRP, DIM), f32)],
        name='relayout',
    )(pltpu.with_memory_space_constraint(out_q, vmem), pltpu.with_memory_space_constraint(out_kv, vmem))


def solution(mesh):
    row_spec = P(None, CP_AXES, 'heads', None)
    stat_spec = P(None, CP_AXES, 'heads')
    key_spec = P(CP_AXES, 'heads', None)
    return jax.shard_map(call, mesh=mesh, in_specs=(row_spec, row_spec, row_spec, stat_spec, key_spec, key_spec),
                         out_specs=(row_spec, key_spec, key_spec), check_vma=False)
```

```python
import jax
import jax.numpy as jnp
from jax import lax
from jax.experimental import pallas as pl
from jax.experimental.pallas import tpu as pltpu
from jax.sharding import PartitionSpec as P

CP_AXES = ('cpo', 'cp')
MESH = pl.DeviceIdType.MESH
LOG2E = 1.4426950408889634

ROW = 8
RING = 4
GRP = 3
TOK = 16
KEYS = 32
DIM = 128
QROWS = ROW * GRP * TOK
KROWS = ROW * KEYS
PACK = GRP * TOK
SCALE = DIM ** -0.5
NSEM = 60
NSEND = 12
HOPS = RING

OWN, N1, N2, X = range(4)
GROUPS = (((0, 0), (0, 1), (0, 2), (0, 3)), ((-1, 0), (1, 0), (-1, 1), (1, 3)),
          ((-1, 3), (1, 2), (-1, 2), (1, 1)), ((2, 0), (2, 1), (2, 2), (2, 3)))
PLACE = {chunk: (group, slot) for group, chunks in enumerate(GROUPS) for slot, chunk in enumerate(chunks)}
DIRECT_KV = True
VIA_PLUS = (2, 0)

NT = (((1,), (1,)), ((), ()))
NN = (((1,), (0,)), ((), ()))
TN = (((0,), (0,)), ((), ()))


def dot(a, b, dims):
    return lax.dot_general(a, b, dims, preferred_element_type=jnp.float32)


def kernel(q_in, o_in, g_in, l_in, k_in, v_in, out_q, out_kv,
           q_vm, o_vm, g_vm, l_vm, k_vm, v_vm, perm_q, perm_kv, ts, tt,
           pq, pst, pkv, qd, st, kv, ld, rowc, akv, aqt, oq,
           ra_kv, rb_kv, ra_q, rb_q, fq, in_sem, ssem, rsem):
    me = lax.axis_index('cp')
    cpo = lax.axis_index('cpo')
    z, y = cpo // RING, cpo % RING
    x, core = me // 2, me % 2

    def row_dev(j):
        return (0, cpo, j)

    def along(n, queries):
        n = n % RING
        y_step = (core == 0) == queries
        return jnp.where(y_step, z, (z + n) % RING), jnp.where(y_step, (y + n) % RING, y)

    def ring_devs(queries):
        devs = []
        for n in (1, -1, 2):
            zn, yn = along(n, queries)
            devs.append((0, zn * RING + yn, me))
        return devs

    qdev, kdev = ring_devs(True), ring_devs(False)

    loads = [pltpu.make_async_copy(src, dst, in_sem.at[i]) for i, (src, dst) in enumerate(
        ((g_in, g_vm), (q_in, q_vm), (k_in, k_vm), (v_in, v_vm), (o_in, o_vm), (l_in, l_vm)))]
    for ld_copy in loads:
        ld_copy.start()

    barrier = pltpu.get_barrier_semaphore()
    for j in range(1, ROW):
        pl.semaphore_signal(barrier, inc=1, device_id=row_dev((me + j) % ROW), device_id_type=MESH)
    for dev in qdev + kdev:
        pl.semaphore_signal(barrier, inc=1, device_id=dev, device_id_type=MESH)

    counter = [0, 0]

    def take(n):
        first = counter[0]
        counter[0] += n
        assert counter[0] <= NSEM
        return first

    def take_send():
        counter[1] += 1
        assert counter[1] <= NSEND
        return counter[1] - 1

    def remote(src, dst, send_i, recv_i, dev):
        return pltpu.make_async_remote_copy(
            src_ref=src, dst_ref=dst, send_sem=ssem.at[send_i], recv_sem=rsem.at[recv_i],
            device_id=dev, device_id_type=MESH)

    def arrived(ref, recv_i):
        remote(ref, ref, 0, recv_i, row_dev(me)).wait_recv()

    sent = []

    def chunk(ref, n, r):
        group, slot = PLACE[n, r]
        return ref.at[group, pl.ds(2 * slot, 2)]

    class Row:
        def __init__(self, src, dst):
            self.dst = dst
            self.src, self.recv, self.send_i = src, take(HOPS), take_send()
            sent.append((self.send_i, src.at[pl.ds(0, ROW - 1)]))

        def send(self, *chips):
            for r in chips:
                back = (HOPS - r) % HOPS
                for c in ((0, 1) if r else (1 - core,)):
                    d = (x + r) % HOPS * 2 + c
                    remote(self.src.at[d], self.dst.at[2 * back + core], self.send_i, self.recv + back, row_dev(d)).start()

        def wait(self, r):
            arrived(self.dst.at[pl.ds(0, 2 if r else 1)], self.recv + r)

    def permutation(ref, tokens, heads):
        n = tokens * heads
        i = lax.broadcasted_iota(jnp.int32, (n, n), 0)
        source = (i & (tokens - 1)) * heads + (i >> (tokens.bit_length() - 1))
        ref[...] = (lax.broadcasted_iota(jnp.int32, (n, n), 1) == source).astype(jnp.float32).astype(jnp.bfloat16)

    permutation(perm_q, TOK, ROW * GRP)
    permutation(perm_kv, KEYS, ROW)
    ts[...] = jnp.zeros_like(ts)
    with jax.named_scope('loads'):
        for load in loads:
            load.wait()
    with jax.named_scope('pack'):
        prod = g_vm[...].astype(jnp.float32) * o_vm[...].astype(jnp.float32)
        delta = jnp.sum(prod.reshape(TOK, ROW * GRP, DIM), axis=-1)
        ts[pl.ds(0, TOK), pl.ds(0, ROW * GRP)] = l_vm[...].reshape(TOK, ROW * GRP)
        ts[pl.ds(TOK, TOK), pl.ds(0, ROW * GRP)] = delta
        tt[...] = ts[...].T
        rows = dot(perm_q[...], jnp.concatenate([q_vm[...], g_vm[...]], axis=1), NN).astype(jnp.bfloat16)
        for i in (0, 1):
            pq[:, pl.ds(i * GRP, GRP)] = rows[:, i * DIM:(i + 1) * DIM].reshape(ROW, GRP, TOK, DIM)
        rows = dot(perm_kv[...], jnp.concatenate([k_vm[...], v_vm[...]], axis=1), NN).astype(jnp.bfloat16)
        for i in (0, 1):
            pkv[:, i] = rows[:, i * DIM:(i + 1) * DIM].reshape(ROW, KEYS, DIM)
        lane = lax.broadcasted_iota(jnp.int32, (ROW, DIM), 1)
        for which in range(2):
            packed = jnp.zeros((ROW, DIM), jnp.float32)
            for g in range(GRP):
                rows = tt[pl.ds(g, ROW, stride=GRP), :]
                shift = (g * TOK - which * TOK) % DIM
                if shift:
                    rows = pltpu.roll(rows, shift, 1)
                packed = jnp.where((lane >= g * TOK) & (lane < (g + 1) * TOK), rows, packed)
            pst[:, which, :] = packed
    with jax.named_scope('barrier'):
        pl.semaphore_wait(barrier, ROW - 1 + 6)
    row_st, row_q, row_kv = Row(pst, st.at[OWN]), Row(pq, qd.at[OWN]), Row(pkv, kv.at[OWN])
    for row in (row_st, row_q, row_kv):
        row.send(0)
    row_st.send(1, 3, 2)
    row_q.send(1, 3)
    row_kv.send(1, 3)
    row_q.send(2)
    row_kv.send(2)
    st[OWN, core] = pst[me]
    qd[OWN, core] = pq[me]
    kv[OWN, core] = pkv[me]

    class Gather:
        def __init__(self, buf, devs, direct=False):
            self.buf, self.devs, self.direct = buf, devs, direct
            self.recv = {at: take(1) for at in ((-1, 0), (1, 0), (-1, 1), (1, 3)) + (() if direct else ((1, 2),))}
            self.send_i, self.rest, self.far = take_send(), take(1), take(1)
            sent.append((self.send_i, buf.at[pl.ds(0, RING - 1)]))

        def send(self, r, *sides):
            for side in sides:
                n = (-1, 1, 2)[side]
                recv_i = self.far if side == 2 else self.recv.get((n, r), self.rest)
                remote(chunk(self.buf, 0, r), chunk(self.buf, n, r), self.send_i, recv_i, self.devs[side]).start()

        def wait(self, n, r):
            arrived(chunk(self.buf, n, r), self.recv[n, r])

        def forward(self, n, r):
            self.wait(n, r)
            remote(chunk(self.buf, n, r), chunk(self.buf, 2, r), self.send_i, self.far, self.devs[0 if n < 0 else 1]).start()

        def wait_rest(self):
            arrived(self.buf.at[0, pl.ds(0, 8 if self.direct else 6)], self.rest)

        def wait_far(self):
            arrived(self.buf.at[X], self.far)

    agst, agq, agkv = Gather(st, qdev), Gather(qd, qdev), Gather(kv, kdev, DIRECT_KV)

    def pass_on(row, gather, r):
        row.wait(r)
        if row is row_q:
            pass_on(row_st, agst, r)
        if r == 0:
            gather.send(0, 0, 1)
        elif r == 1:
            gather.send(1, 0)
        elif r == 3:
            gather.send(3, 1, 0)
        elif gather.direct:
            gather.send(2, 1, 0)
            gather.send(1, 1)
            gather.send(2, 2)
        else:
            gather.send(2, 1)
            gather.send(1, 1)
            gather.send(2, 0)

    with jax.named_scope('row_0'):
        pass_on(row_q, agq, 0)
        pass_on(row_kv, agkv, 0)

    r_id = lax.broadcasted_iota(jnp.int32, (1, QROWS), 1)
    packet = (r_id * 1366) >> 16
    token = ((r_id >> 3) & 1) * 1024 + (packet & 1) * 8 + (r_id & 7) + 2048
    for group in range(RING):
        spot = jnp.zeros_like(token)
        for slot, (n, r) in enumerate(GROUPS[group]):
            zq, yq = along(n, True)
            spot = jnp.where((packet >> 1) == slot, zq * 256 + yq * 64 + (x + r) % HOPS * 16, spot)
        rowc[group] = token + spot

    src_id = (3 * lax.broadcasted_iota(jnp.int32, (ROW, DIM), 0)) & 7

    def assemble(group):
        for which in range(2):
            rows = []
            for i in range(ROW):
                rows.append(st[group, pl.ds(3 * i % ROW, 1), which, :])
            rows = pltpu.roll(jnp.concatenate(rows, axis=0), 0, 1, stride=TOK, stride_axis=0)
            for k in range(QROWS // DIM):
                mine = (((lane + k * DIM) * 1366) >> 16) == src_id
                line = jnp.sum(jnp.where(mine, rows, 0.0), axis=0, keepdims=True)
                ld[group, pl.ds(which, 1), pl.ds(k * DIM, DIM)] = line * LOG2E if which == 0 else line

    class Scatter:
        def __init__(self, acc, ra, rb, devs):
            self.acc, self.ra, self.rb, self.devs = acc, ra, rb, devs
            self.send_i, self.first, self.near = take_send(), take(HOPS), take(HOPS)
            sent.append((self.send_i, acc.at[pl.ds(0, RING - 1)]))

        def send_far(self, r):
            side = 0 if r in VIA_PLUS else 1
            remote(chunk(self.acc, 2, r), self.ra.at[r], self.send_i, self.first + r, self.devs[side]).start()

        def send_near(self, side, r):
            remote(chunk(self.acc, -1 if side else 1, r), self.rb.at[side, r], self.send_i, self.near + r, self.devs[side]).start()

        def send_early(self, r):
            self.send_near(1 if r in VIA_PLUS else 0, r)

        def send_late(self, r):
            side = 0 if r in VIA_PLUS else 1
            arrived(self.ra.at[r], self.first + r)
            mine = chunk(self.acc, -1 if side else 1, r)
            mine[...] = mine[...] + self.ra[r]
            self.send_near(side, r)

        def total(self, r):
            arrived(self.rb.at[0, pl.ds(0, 2)], self.near + r)
            return chunk(self.acc, 0, r)[...] + self.rb[0, r] + self.rb[1, r]

    rsk, rsv = (Scatter(akv.at[i], ra_kv.at[i], rb_kv.at[i], kdev) for i in (0, 1))
    rsq = Scatter(oq, ra_q, rb_q, qdev)

    band_rows = KROWS // HOPS
    key_row = lax.broadcasted_iota(jnp.int32, (band_rows, QROWS), 0)
    begun = set()

    def add(ref, name, value):
        ref[...] = ref[...] + value if name in begun else value
        begun.add(name)

    def tile(qs, ks):
        with jax.named_scope('tile' + ''.join(map(str, qs)) + 'x' + ''.join(map(str, ks))):
            q = jnp.concatenate([qd[i, :, pl.ds(0, GRP)].reshape(QROWS, DIM) for i in qs], axis=0)
            g = jnp.concatenate([qd[i, :, pl.ds(GRP, GRP)].reshape(QROWS, DIM) for i in qs], axis=0)
            k = jnp.concatenate([kv[i, :, 0].reshape(KROWS, DIM) for i in ks], axis=0)
            v = jnp.concatenate([kv[i, :, 1].reshape(KROWS, DIM) for i in ks], axis=0)
            lse = jnp.concatenate([ld[i, pl.ds(0, 1), :] for i in qs], axis=1)
            dlt = jnp.concatenate([ld[i, pl.ds(1, 1), :] for i in qs], axis=1)
            expo = jnp.exp2(dot(k, q, NT) * (SCALE * LOG2E) - lse)
            bands = []
            for n, r in [at for i in ks for at in GROUPS[i]]:
                zk, yk = along(n, False)
                first = zk * 1024 + yk * 256 + (x + r) % HOPS * band_rows
                seen = jnp.concatenate([key_row <= rowc[i] - first for i in qs], axis=1)
                at = len(bands) * band_rows
                bands.append(jnp.where(seen, expo[at:at + band_rows], 0.0))
            p_t = jnp.concatenate(bands, axis=0)
            dp_t = dot(v, g, NT)
            ds_t = (p_t * (dp_t - dlt)).astype(jnp.bfloat16)
            dv = dot(p_t.astype(jnp.bfloat16), g, NN)
            dk = dot(ds_t, q, NN)
            dq = dot(k, ds_t, TN)
            for n, i in enumerate(ks):
                add(akv.at[1, i], ('v', i), dv[n * KROWS:(n + 1) * KROWS].reshape(ROW, KEYS, DIM))
                add(akv.at[0, i], ('k', i), dk[n * KROWS:(n + 1) * KROWS].reshape(ROW, KEYS, DIM))
            for n, i in enumerate(qs):
                add(aqt.at[i], ('q', i), dq[:, n * QROWS:(n + 1) * QROWS])

    def finish_q(group):
        oq[group] = aqt[group].T.reshape(ROW, PACK, DIM)

    for chips in ((1, 3), (2,)):
        for name, row, gather in (('', row_q, agq), ('kv', row_kv, agkv)):
            for r in chips:
                with jax.named_scope(f'row_{name}{r}'):
                    pass_on(row, gather, r)
    assemble(OWN)
    tile([OWN], [OWN])
    def forward_q(n, r):
        agst.forward(n, r)
        agq.forward(n, r)

    with jax.named_scope('fwd_0'):
        forward_q(-1, 0)
        agkv.forward(-1, 0)
    with jax.named_scope('fwd_q1'):
        forward_q(-1, 1)
        forward_q(1, 3)
        agst.wait(1, 0)
        agq.wait(1, 0)
        assemble(N1)
    tile([N1], [OWN])
    with jax.named_scope('fwd_k1'):
        agkv.forward(-1, 1)
        agkv.forward(1, 3)
    with jax.named_scope('fwd_q2'):
        forward_q(1, 2)
    with jax.named_scope('fwd_k2'):
        if not DIRECT_KV:
            agkv.forward(1, 2)
        agkv.wait(1, 0)
    tile([OWN, N1], [N1])
    with jax.named_scope('rest_k'):
        agkv.wait_rest()
    tile([OWN, N1], [N2])
    with jax.named_scope('rest_q'):
        agst.wait_rest()
        agq.wait_rest()
        assemble(N2)
    tile([N2], [OWN, N1, N2])
    with jax.named_scope('far_k'):
        agkv.wait_far()
    tile([OWN, N1, N2], [X])
    with jax.named_scope('far_q'):
        agst.wait_far()
        agq.wait_far()
        assemble(X)
    tile([X], [X])
    for pair in ((2, 1), (0, 3)):
        for scatter in (rsv, rsk):
            for r in pair:
                scatter.send_far(r)
    tile([X], [N1, N2, OWN])
    finish_q(X)
    rsq.send_far(2)
    rsq.send_far(1)

    @pl.when(core == 0)
    def _():
        rsq.send_far(0)
        rsq.send_far(3)

    for scatter in (rsv, rsk):
        scatter.send_early(1)
        scatter.send_early(2)
    with jax.named_scope('finish'):
        finish_q(N1)
        finish_q(N2)

    @pl.when(core == 0)
    def _():
        rsq.send_early(1)
        rsq.send_early(2)

    finish_q(OWN)

    def late(name, scatter, *chunks):
        with jax.named_scope(f'late_{name}{chunks[0]}'):
            for r in chunks:
                scatter.send_late(r)

    class Give:
        def __init__(self, src, dst):
            self.src, self.dst = src, dst
            self.send_i, self.recv_i = take_send(), take(1)
            sent.append((self.send_i, src.at[pl.ds(0, ROW - 1)]))

        def send(self, r):
            for c in ((0, 1) if r else (1 - core,)):
                d = (x + r) % HOPS * 2 + c
                remote(self.src.at[2 * r + c], self.dst.at[me], self.send_i, self.recv_i, row_dev(d)).start()

        def wait(self):
            arrived(self.dst.at[pl.ds(0, ROW - 1)], self.recv_i)

    give_k, give_v, give_q = Give(akv.at[0, OWN], out_kv.at[0]), Give(akv.at[1, OWN], out_kv.at[1]), Give(fq, out_q)

    def total(name, r):
        part = pl.ds(2 * r, 2)
        with jax.named_scope(f'total_{name}{r}'):
            if name == 'v':
                akv[1, OWN, part] = rsv.total(r)
            elif name == 'k':
                akv[0, OWN, part] = rsk.total(r) * SCALE
            else:
                fq[part] = (rsq.total(r) * SCALE).astype(jnp.bfloat16)
        {'v': give_v, 'k': give_k, 'q': give_q}[name].send(r)

    def early(r):
        rsv.send_early(r)
        rsk.send_early(r)

    def totals(names, *chunks):
        for r in chunks:
            for name in names:
                total(name, r)

    late('v', rsv, 2, 1)
    late('k', rsk, 2, 1)

    @pl.when(core == 0)
    def _():
        early(3)
        late('v', rsv, 3)
        late('k', rsk, 3)
        late('q', rsq, 2, 1)
        rsq.send_early(3)
        late('q', rsq, 3)
        late('v', rsv, 0)
        late('k', rsk, 0)
        early(0)
        late('q', rsq, 0)
        rsq.send_early(0)
        totals('vk', 2, 1)
        totals('q', 2)
        totals('vk', 3)
        totals('q', 1, 3)
        totals('vkq', 0)

    @pl.when(core == 1)
    def _():
        rsq.send_far(0)
        rsq.send_far(3)
        rsq.send_early(1)
        rsq.send_early(2)
        early(3)
        late('v', rsv, 3)
        late('k', rsk, 3)
        late('q', rsq, 2, 1)
        totals('vk', 2, 1)
        rsq.send_early(3)
        late('q', rsq, 3)
        late('v', rsv, 0)
        late('k', rsk, 0)
        early(0)
        totals('vk', 3)
        late('q', rsq, 0)
        rsq.send_early(0)
        totals('q', 2, 1, 3)
        totals('vkq', 0)

    out_q[me] = fq[core]
    out_kv[0, me] = akv[0, OWN, core]
    out_kv[1, me] = akv[1, OWN, core]

    with jax.named_scope('final_q'):
        give_q.wait()
    with jax.named_scope('final_kv'):
        give_v.wait()
        give_k.wait()
    with jax.named_scope('drain'):
        for send_i, ref in sent:
            remote(ref, ref, send_i, 0, row_dev(me)).wait_send()


def relayout(q_ref, kv_ref, dq_ref, dk_ref, dv_ref, rows):
    for h in range(ROW):
        dk_ref[:, h, :] = kv_ref[0, h]
        dv_ref[:, h, :] = kv_ref[1, h]
        for g in range(GRP):
            rows[:, h * GRP + g, :] = q_ref[h, pl.ds(g * TOK, TOK), :].astype(jnp.float32)
    dq_ref[...] = rows[...].astype(jnp.bfloat16).reshape(dq_ref.shape)


def call(queries, attn_out, grad_out, log_sum_exp, key_cache, value_cache):
    f32, bf16 = jnp.float32, jnp.bfloat16
    vmem = pltpu.VMEM
    tok = (2, TOK // 2, ROW * GRP, DIM)
    key = (KEYS, ROW, DIM)
    tok2, key2 = (QROWS, DIM), (KROWS, DIM)
    scratch = [
        vmem(tok2, bf16), vmem(tok2, bf16), vmem(tok2, bf16), vmem(tok[:3], f32), vmem(key2, bf16), vmem(key2, bf16),
        vmem((QROWS, QROWS), bf16), vmem((KROWS, KROWS), bf16), vmem((DIM, DIM), f32), vmem((DIM, DIM), f32),
        vmem((ROW, 2 * GRP, TOK, DIM), bf16), vmem((ROW, 2, DIM), f32), vmem((ROW, 2, KEYS, DIM), bf16),
        vmem((RING, ROW, 2 * GRP, TOK, DIM), bf16), vmem((RING, ROW, 2, DIM), f32), vmem((RING, ROW, 2, KEYS, DIM), bf16),
        vmem((RING, 8, QROWS), f32), vmem((RING, 1, QROWS), jnp.int32),
        vmem((2, RING, ROW, KEYS, DIM), f32), vmem((RING, DIM, QROWS), f32), vmem((RING, ROW, PACK, DIM), f32),
        vmem((2, HOPS, 2, KEYS, DIM), f32), vmem((2, 2, HOPS, 2, KEYS, DIM), f32),
        vmem((HOPS, 2, PACK, DIM), f32), vmem((2, HOPS, 2, PACK, DIM), f32),
        vmem((ROW, PACK, DIM), bf16),
        pltpu.SemaphoreType.DMA((6,)), pltpu.SemaphoreType.DMA((NSEND,)), pltpu.SemaphoreType.DMA((NSEM,)),
    ]
    out_q, out_kv = pl.pallas_call(
        kernel,
        out_shape=(vmem((ROW, PACK, DIM), bf16), vmem((2, ROW, KEYS, DIM), f32)),
        in_specs=[pl.BlockSpec(memory_space=pl.ANY)] * 6,
        out_specs=[pl.BlockSpec(memory_space=pltpu.VMEM)] * 2,
        scratch_shapes=scratch,
        compiler_params=pltpu.CompilerParams(collective_id=0, has_side_effects=True),
        name='attn_bwd_3d',
    )(queries.reshape(tok2), attn_out.reshape(tok2), grad_out.reshape(tok2), log_sum_exp,
      key_cache.reshape(key2), value_cache.reshape(key2))
    return pl.pallas_call(
        relayout,
        out_shape=(jax.ShapeDtypeStruct(tok, bf16), jax.ShapeDtypeStruct(key, f32), jax.ShapeDtypeStruct(key, f32)),
        in_specs=[pl.BlockSpec(memory_space=pltpu.VMEM)] * 2,
        out_specs=[pl.BlockSpec(memory_space=pltpu.VMEM)] * 3,
        scratch_shapes=[vmem((TOK, ROW * GRP, DIM), f32)],
        name='relayout',
    )(pltpu.with_memory_space_constraint(out_q, vmem), pltpu.with_memory_space_constraint(out_kv, vmem))


def solution(mesh):
    row_spec = P(None, CP_AXES, 'heads', None)
    stat_spec = P(None, CP_AXES, 'heads')
    key_spec = P(CP_AXES, 'heads', None)
    return jax.shard_map(call, mesh=mesh, in_specs=(row_spec, row_spec, row_spec, stat_spec, key_spec, key_spec),
                         out_specs=(row_spec, key_spec, key_spec), check_vma=False)
```

```python
import jax
import jax.numpy as jnp
from jax import lax
from jax.experimental import pallas as pl
from jax.experimental.pallas import tpu as pltpu
from jax.sharding import PartitionSpec as P

CP_AXES = ('cpo', 'cp')
MESH = pl.DeviceIdType.MESH
LOG2E = 1.4426950408889634

ROW = 8
RING = 4
GRP = 3
TOK = 16
KEYS = 32
DIM = 128
QROWS = ROW * GRP * TOK
KROWS = ROW * KEYS
PACK = GRP * TOK
SCALE = DIM ** -0.5
HOPS = RING

OWN, N1, N2, X = range(4)
GROUPS = (((0, 0), (0, 1), (0, 2), (0, 3)), ((-1, 0), (1, 0), (-1, 1), (1, 3)),
          ((-1, 3), (1, 2), (-1, 2), (1, 1)), ((2, 0), (2, 1), (2, 2), (2, 3)))
PLACE = {chunk: (group, slot) for group, chunks in enumerate(GROUPS) for slot, chunk in enumerate(chunks)}
DIRECT_KV = True
VIA_PLUS = (2, 0)

NSEM = 48
LINE_Q, LINE_KV, LINE_DQ = 50, 32, 24
SENT = (ROW - 1 + (RING - 1) * ROW) * (LINE_Q + LINE_KV) + (RING - 1) * ROW * (2 * KEYS + PACK) + (ROW - 1) * (2 * KEYS + LINE_DQ)

NT = (((1,), (1,)), ((), ()))
NN = (((1,), (0,)), ((), ()))
TN = (((0,), (0,)), ((), ()))


def dot(a, b, dims):
    return lax.dot_general(a, b, dims, preferred_element_type=jnp.float32)


def kernel(q_in, o_in, g_in, l_in, k_in, v_in, out_q, out_kv,
           q_vm, o_vm, g_vm, l_vm, k_vm, v_vm, perm_q, perm_kv, ts, tt,
           pq, pst, pkv, qd, st, kv, ld, rowc, akv, aqt, oq,
           ra_kv, rb_kv, ra_q, rb_q, fq, in_sem, ssem, rsem, gauge):
    me = lax.axis_index('cp')
    cpo = lax.axis_index('cpo')
    z, y = cpo // RING, cpo % RING
    x, core = me // 2, me % 2

    def row_dev(j):
        return (0, cpo, j)

    def along(n, queries):
        n = n % RING
        y_step = (core == 0) == queries
        return jnp.where(y_step, z, (z + n) % RING), jnp.where(y_step, (y + n) % RING, y)

    def ring_devs(queries):
        devs = []
        for n in (1, -1, 2):
            zn, yn = along(n, queries)
            devs.append((0, zn * RING + yn, me))
        return devs

    qdev, kdev = ring_devs(True), ring_devs(False)

    loads = [pltpu.make_async_copy(src, dst, in_sem.at[i // 5]) for i, (src, dst) in enumerate(
        ((g_in, g_vm), (q_in, q_vm), (k_in, k_vm), (v_in, v_vm), (o_in, o_vm), (l_in, l_vm)))]
    for ld_copy in loads:
        ld_copy.start()

    barrier = pltpu.get_barrier_semaphore()
    for j in range(1, ROW):
        pl.semaphore_signal(barrier, inc=1, device_id=row_dev((me + j) % ROW), device_id_type=MESH)
    for dev in qdev + kdev:
        pl.semaphore_signal(barrier, inc=1, device_id=dev, device_id_type=MESH)

    counter = [0]

    def take(n):
        first = counter[0]
        counter[0] += n
        assert counter[0] <= NSEM
        return first

    def remote(src, dst, recv_i, dev):
        return pltpu.make_async_remote_copy(
            src_ref=src, dst_ref=dst, send_sem=ssem.at[0], recv_sem=rsem.at[recv_i],
            device_id=dev, device_id_type=MESH)

    def lines(n):
        return gauge.at[pl.ds(0, n)]

    def arrived(n, recv_i):
        remote(lines(n), lines(n), recv_i, row_dev(me)).wait_recv()

    def chunk(ref, n, r):
        group, slot = PLACE[n, r]
        return ref.at[group, pl.ds(2 * slot, 2)]

    class Row:
        def __init__(self, size, *pairs):
            self.size, self.pairs, self.recv = size, pairs, take(HOPS)

        def send(self, *chips):
            for r in chips:
                back = (HOPS - r) % HOPS
                for c in ((0, 1) if r else (1 - core,)):
                    d = (x + r) % HOPS * 2 + c
                    for src, dst in self.pairs:
                        remote(src.at[d], dst.at[2 * back + core], self.recv + back, row_dev(d)).start()

        def wait(self, r):
            arrived(self.size * (2 if r else 1), self.recv + r)

    def permutation(ref, tokens, heads):
        n = tokens * heads
        i = lax.broadcasted_iota(jnp.int32, (n, n), 0)
        source = (i & (tokens - 1)) * heads + (i >> (tokens.bit_length() - 1))
        ref[...] = (lax.broadcasted_iota(jnp.int32, (n, n), 1) == source).astype(jnp.float32).astype(jnp.bfloat16)

    permutation(perm_q, TOK, ROW * GRP)
    permutation(perm_kv, KEYS, ROW)
    ts[...] = jnp.zeros_like(ts)
    with jax.named_scope('loads'):
        whole = lines((3 * QROWS + 2 * KROWS) // 2)
        pltpu.make_async_copy(whole, whole, in_sem.at[0]).wait()
        loads[5].wait()
    with jax.named_scope('pack'):
        prod = g_vm[...].astype(jnp.float32) * o_vm[...].astype(jnp.float32)
        delta = jnp.sum(prod.reshape(TOK, ROW * GRP, DIM), axis=-1)
        ts[pl.ds(0, TOK), pl.ds(0, ROW * GRP)] = l_vm[...].reshape(TOK, ROW * GRP)
        ts[pl.ds(TOK, TOK), pl.ds(0, ROW * GRP)] = delta
        tt[...] = ts[...].T
        rows = dot(perm_q[...], jnp.concatenate([q_vm[...], g_vm[...]], axis=1), NN).astype(jnp.bfloat16)
        for i in (0, 1):
            pq[:, pl.ds(i * GRP, GRP)] = rows[:, i * DIM:(i + 1) * DIM].reshape(ROW, GRP, TOK, DIM)
        rows = dot(perm_kv[...], jnp.concatenate([k_vm[...], v_vm[...]], axis=1), NN).astype(jnp.bfloat16)
        for i in (0, 1):
            pkv[:, i] = rows[:, i * DIM:(i + 1) * DIM].reshape(ROW, KEYS, DIM)
        lane = lax.broadcasted_iota(jnp.int32, (ROW, DIM), 1)
        for which in range(2):
            packed = jnp.zeros((ROW, DIM), jnp.float32)
            for g in range(GRP):
                rows = tt[pl.ds(g, ROW, stride=GRP), :]
                shift = (g * TOK - which * TOK) % DIM
                if shift:
                    rows = pltpu.roll(rows, shift, 1)
                packed = jnp.where((lane >= g * TOK) & (lane < (g + 1) * TOK), rows, packed)
            pst[:, which, :] = packed
    with jax.named_scope('barrier'):
        pl.semaphore_wait(barrier, ROW - 1 + 6)
    row_q = Row(LINE_Q, (pst, st.at[OWN]), (pq, qd.at[OWN]))
    row_kv = Row(LINE_KV, (pkv, kv.at[OWN]))
    row_q.send(0)
    row_kv.send(0)
    row_q.send(1, 3)
    row_kv.send(1, 3)
    row_q.send(2)
    row_kv.send(2)
    st[OWN, core] = pst[me]
    qd[OWN, core] = pq[me]
    kv[OWN, core] = pkv[me]

    class Gather:
        def __init__(self, size, bufs, devs, direct=False):
            self.size, self.bufs, self.devs, self.direct = 2 * size, bufs, devs, direct
            self.recv = {at: take(1) for at in ((-1, 0), (1, 0), (-1, 1), (1, 3)) + (() if direct else ((1, 2),))}
            self.rest, self.far = take(1), take(1)

        def send(self, r, *sides):
            for side in sides:
                n = (-1, 1, 2)[side]
                recv_i = self.far if side == 2 else self.recv.get((n, r), self.rest)
                for buf in self.bufs:
                    remote(chunk(buf, 0, r), chunk(buf, n, r), recv_i, self.devs[side]).start()

        def wait(self, n, r):
            arrived(self.size, self.recv[n, r])

        def forward(self, n, r):
            self.wait(n, r)
            for buf in self.bufs:
                remote(chunk(buf, n, r), chunk(buf, 2, r), self.far, self.devs[0 if n < 0 else 1]).start()

        def wait_rest(self):
            arrived(self.size * (4 if self.direct else 3), self.rest)

        def wait_far(self):
            arrived(self.size * HOPS, self.far)

    agq, agkv = Gather(LINE_Q, (st, qd), qdev), Gather(LINE_KV, (kv,), kdev, DIRECT_KV)

    def pass_on(row, gather, r):
        row.wait(r)
        if r == 0:
            gather.send(0, 0, 1)
        elif r == 1:
            gather.send(1, 0)
        elif r == 3:
            gather.send(3, 1, 0)
        elif gather.direct:
            gather.send(2, 1, 0)
            gather.send(1, 1)
            gather.send(2, 2)
        else:
            gather.send(2, 1)
            gather.send(1, 1)
            gather.send(2, 0)

    with jax.named_scope('row_0'):
        pass_on(row_q, agq, 0)
        pass_on(row_kv, agkv, 0)

    r_id = lax.broadcasted_iota(jnp.int32, (1, QROWS), 1)
    packet = (r_id * 1366) >> 16
    token = ((r_id >> 3) & 1) * 1024 + (packet & 1) * 8 + (r_id & 7) + 2048
    for group in range(RING):
        spot = jnp.zeros_like(token)
        for slot, (n, r) in enumerate(GROUPS[group]):
            zq, yq = along(n, True)
            spot = jnp.where((packet >> 1) == slot, zq * 256 + yq * 64 + (x + r) % HOPS * 16, spot)
        rowc[group] = token + spot

    src_id = (3 * lax.broadcasted_iota(jnp.int32, (ROW, DIM), 0)) & 7

    def assemble(group):
        for which in range(2):
            rows = []
            for i in range(ROW):
                rows.append(st[group, pl.ds(3 * i % ROW, 1), which, :])
            rows = pltpu.roll(jnp.concatenate(rows, axis=0), 0, 1, stride=TOK, stride_axis=0)
            for k in range(QROWS // DIM):
                mine = (((lane + k * DIM) * 1366) >> 16) == src_id
                line = jnp.sum(jnp.where(mine, rows, 0.0), axis=0, keepdims=True)
                ld[group, pl.ds(which, 1), pl.ds(k * DIM, DIM)] = line * LOG2E if which == 0 else line

    class Scatter:
        def __init__(self, size, acc, ra, rb, devs):
            self.size, self.acc, self.ra, self.rb, self.devs = 2 * size, acc, ra, rb, devs
            self.first, self.near = take(HOPS), take(HOPS)

        def send_far(self, r):
            side = 0 if r in VIA_PLUS else 1
            remote(chunk(self.acc, 2, r), self.ra.at[r], self.first + r, self.devs[side]).start()

        def send_near(self, side, r):
            remote(chunk(self.acc, -1 if side else 1, r), self.rb.at[side, r], self.near + r, self.devs[side]).start()

        def send_early(self, r):
            self.send_near(1 if r in VIA_PLUS else 0, r)

        def send_late(self, r):
            side = 0 if r in VIA_PLUS else 1
            arrived(self.size, self.first + r)
            mine = chunk(self.acc, -1 if side else 1, r)
            mine[...] = mine[...] + self.ra[r]
            self.send_near(side, r)

        def total(self, r):
            arrived(2 * self.size, self.near + r)
            return chunk(self.acc, 0, r)[...] + self.rb[0, r] + self.rb[1, r]

    rsk, rsv = (Scatter(KEYS, akv.at[i], ra_kv.at[i], rb_kv.at[i], kdev) for i in (0, 1))
    rsq = Scatter(PACK, oq, ra_q, rb_q, qdev)

    band_rows = KROWS // HOPS
    key_row = lax.broadcasted_iota(jnp.int32, (band_rows, QROWS), 0)
    begun = set()

    def add(ref, name, value):
        ref[...] = ref[...] + value if name in begun else value
        begun.add(name)

    def tile(qs, ks):
        with jax.named_scope('tile' + ''.join(map(str, qs)) + 'x' + ''.join(map(str, ks))):
            q = jnp.concatenate([qd[i, :, pl.ds(0, GRP)].reshape(QROWS, DIM) for i in qs], axis=0)
            g = jnp.concatenate([qd[i, :, pl.ds(GRP, GRP)].reshape(QROWS, DIM) for i in qs], axis=0)
            k = jnp.concatenate([kv[i, :, 0].reshape(KROWS, DIM) for i in ks], axis=0)
            v = jnp.concatenate([kv[i, :, 1].reshape(KROWS, DIM) for i in ks], axis=0)
            lse = jnp.concatenate([ld[i, pl.ds(0, 1), :] for i in qs], axis=1)
            dlt = jnp.concatenate([ld[i, pl.ds(1, 1), :] for i in qs], axis=1)
            expo = jnp.exp2(dot(k, q, NT) * (SCALE * LOG2E) - lse)
            bands = []
            for n, r in [at for i in ks for at in GROUPS[i]]:
                zk, yk = along(n, False)
                first = zk * 1024 + yk * 256 + (x + r) % HOPS * band_rows
                seen = jnp.concatenate([key_row <= rowc[i] - first for i in qs], axis=1)
                at = len(bands) * band_rows
                bands.append(jnp.where(seen, expo[at:at + band_rows], 0.0))
            p_t = jnp.concatenate(bands, axis=0)
            dp_t = dot(v, g, NT)
            ds_t = (p_t * (dp_t - dlt)).astype(jnp.bfloat16)
            dv = dot(p_t.astype(jnp.bfloat16), g, NN)
            dk = dot(ds_t, q, NN)
            dq = dot(k, ds_t, TN)
            for n, i in enumerate(ks):
                add(akv.at[1, i], ('v', i), dv[n * KROWS:(n + 1) * KROWS].reshape(ROW, KEYS, DIM))
                add(akv.at[0, i], ('k', i), dk[n * KROWS:(n + 1) * KROWS].reshape(ROW, KEYS, DIM))
            for n, i in enumerate(qs):
                add(aqt.at[i], ('q', i), dq[:, n * QROWS:(n + 1) * QROWS])

    def finish_q(group):
        oq[group] = aqt[group].T.reshape(ROW, PACK, DIM)

    for chips in ((1, 3), (2,)):
        for name, row, gather in (('', row_q, agq), ('kv', row_kv, agkv)):
            for r in chips:
                with jax.named_scope(f'row_{name}{r}'):
                    pass_on(row, gather, r)
    assemble(OWN)
    tile([OWN], [OWN])
    with jax.named_scope('fwd_0'):
        agq.forward(-1, 0)
        agkv.forward(-1, 0)
    with jax.named_scope('fwd_q1'):
        agq.forward(-1, 1)
        agq.forward(1, 3)
        agq.wait(1, 0)
        assemble(N1)
    tile([N1], [OWN])
    with jax.named_scope('fwd_k1'):
        agkv.forward(-1, 1)
        agkv.forward(1, 3)
    with jax.named_scope('fwd_q2'):
        agq.forward(1, 2)
    with jax.named_scope('fwd_k2'):
        if not DIRECT_KV:
            agkv.forward(1, 2)
        agkv.wait(1, 0)
    tile([OWN, N1], [N1])
    with jax.named_scope('rest_k'):
        agkv.wait_rest()
    tile([OWN, N1], [N2])
    with jax.named_scope('rest_q'):
        agq.wait_rest()
        assemble(N2)
    tile([N2], [OWN, N1, N2])
    with jax.named_scope('far_k'):
        agkv.wait_far()
    tile([OWN, N1, N2], [X])
    with jax.named_scope('far_q'):
        agq.wait_far()
        assemble(X)
    tile([X], [X])
    for pair in ((2, 1), (0, 3)):
        for scatter in (rsv, rsk):
            for r in pair:
                scatter.send_far(r)
    tile([X], [N1, N2, OWN])
    finish_q(X)
    rsq.send_far(2)
    rsq.send_far(1)

    @pl.when(core == 0)
    def _():
        rsq.send_far(0)
        rsq.send_far(3)

    for scatter in (rsv, rsk):
        scatter.send_early(1)
        scatter.send_early(2)
    with jax.named_scope('finish'):
        finish_q(N1)
        finish_q(N2)

    @pl.when(core == 0)
    def _():
        rsq.send_early(1)
        rsq.send_early(2)

    finish_q(OWN)

    def late(name, scatter, *chunks):
        with jax.named_scope(f'late_{name}{chunks[0]}'):
            for r in chunks:
                scatter.send_late(r)

    class Give:
        def __init__(self, size, src, dst):
            self.size, self.src, self.dst, self.recv_i = size, src, dst, take(1)

        def send(self, r):
            for c in ((0, 1) if r else (1 - core,)):
                d = (x + r) % HOPS * 2 + c
                remote(self.src.at[2 * r + c], self.dst.at[me], self.recv_i, row_dev(d)).start()

        def wait(self):
            arrived(self.size * (ROW - 1), self.recv_i)

    give_k, give_v, give_q = Give(KEYS, akv.at[0, OWN], out_kv.at[0]), Give(KEYS, akv.at[1, OWN], out_kv.at[1]), Give(LINE_DQ, fq, out_q)

    def total(name, r):
        part = pl.ds(2 * r, 2)
        with jax.named_scope(f'total_{name}{r}'):
            if name == 'v':
                akv[1, OWN, part] = rsv.total(r)
            elif name == 'k':
                akv[0, OWN, part] = rsk.total(r) * SCALE
            else:
                fq[part] = (rsq.total(r) * SCALE).astype(jnp.bfloat16)
        {'v': give_v, 'k': give_k, 'q': give_q}[name].send(r)

    def early(r):
        rsv.send_early(r)
        rsk.send_early(r)

    def totals(names, *chunks):
        for r in chunks:
            for name in names:
                total(name, r)

    late('v', rsv, 2, 1)
    late('k', rsk, 2, 1)

    @pl.when(core == 0)
    def _():
        early(3)
        late('v', rsv, 3)
        late('k', rsk, 3)
        late('q', rsq, 2, 1)
        rsq.send_early(3)
        late('q', rsq, 3)
        late('v', rsv, 0)
        late('k', rsk, 0)
        early(0)
        late('q', rsq, 0)
        rsq.send_early(0)
        totals('vk', 2, 1)
        totals('q', 2)
        totals('vk', 3)
        totals('q', 1, 3)
        totals('vkq', 0)

    @pl.when(core == 1)
    def _():
        rsq.send_far(0)
        rsq.send_far(3)
        rsq.send_early(1)
        rsq.send_early(2)
        late('q', rsq, 2, 1)
        early(3)
        late('v', rsv, 3)
        late('k', rsk, 3)
        totals('vk', 2, 1)
        rsq.send_early(3)
        late('q', rsq, 3)
        late('v', rsv, 0)
        late('k', rsk, 0)
        early(0)
        totals('vk', 3)
        late('q', rsq, 0)
        rsq.send_early(0)
        totals('q', 2, 1, 3)
        totals('vkq', 0)

    out_q[me] = fq[core]
    out_kv[0, me] = akv[0, OWN, core]
    out_kv[1, me] = akv[1, OWN, core]

    with jax.named_scope('final_q'):
        give_q.wait()
    with jax.named_scope('final_kv'):
        give_v.wait()
        give_k.wait()
    with jax.named_scope('drain'):
        remote(lines(SENT), lines(SENT), 0, row_dev(me)).wait_send()


def relayout(q_ref, kv_ref, dq_ref, dk_ref, dv_ref, rows):
    for h in range(ROW):
        dk_ref[:, h, :] = kv_ref[0, h]
        dv_ref[:, h, :] = kv_ref[1, h]
        for g in range(GRP):
            rows[:, h * GRP + g, :] = q_ref[h, pl.ds(g * TOK, TOK), :].astype(jnp.float32)
    dq_ref[...] = rows[...].astype(jnp.bfloat16).reshape(dq_ref.shape)


def call(queries, attn_out, grad_out, log_sum_exp, key_cache, value_cache):
    f32, bf16 = jnp.float32, jnp.bfloat16
    vmem = pltpu.VMEM
    tok = (2, TOK // 2, ROW * GRP, DIM)
    key = (KEYS, ROW, DIM)
    tok2, key2 = (QROWS, DIM), (KROWS, DIM)
    scratch = [
        vmem(tok2, bf16), vmem(tok2, bf16), vmem(tok2, bf16), vmem(tok[:3], f32), vmem(key2, bf16), vmem(key2, bf16),
        vmem((QROWS, QROWS), bf16), vmem((KROWS, KROWS), bf16), vmem((DIM, DIM), f32), vmem((DIM, DIM), f32),
        vmem((ROW, 2 * GRP, TOK, DIM), bf16), vmem((ROW, 2, DIM), f32), vmem((ROW, 2, KEYS, DIM), bf16),
        vmem((RING, ROW, 2 * GRP, TOK, DIM), bf16), vmem((RING, ROW, 2, DIM), f32), vmem((RING, ROW, 2, KEYS, DIM), bf16),
        vmem((RING, 8, QROWS), f32), vmem((RING, 1, QROWS), jnp.int32),
        vmem((2, RING, ROW, KEYS, DIM), f32), vmem((RING, DIM, QROWS), f32), vmem((RING, ROW, PACK, DIM), f32),
        vmem((2, HOPS, 2, KEYS, DIM), f32), vmem((2, 2, HOPS, 2, KEYS, DIM), f32),
        vmem((HOPS, 2, PACK, DIM), f32), vmem((2, HOPS, 2, PACK, DIM), f32),
        vmem((ROW, PACK, DIM), bf16),
        pltpu.SemaphoreType.DMA((2,)), pltpu.SemaphoreType.DMA((1,)), pltpu.SemaphoreType.DMA((NSEM,)),
        vmem((SENT, DIM), f32),
    ]
    out_q, out_kv = pl.pallas_call(
        kernel,
        out_shape=(vmem((ROW, PACK, DIM), bf16), vmem((2, ROW, KEYS, DIM), f32)),
        in_specs=[pl.BlockSpec(memory_space=pl.ANY)] * 6,
        out_specs=[pl.BlockSpec(memory_space=pltpu.VMEM)] * 2,
        scratch_shapes=scratch,
        compiler_params=pltpu.CompilerParams(collective_id=0, has_side_effects=True),
        name='attn_bwd_3d',
    )(queries.reshape(tok2), attn_out.reshape(tok2), grad_out.reshape(tok2), log_sum_exp,
      key_cache.reshape(key2), value_cache.reshape(key2))
    return pl.pallas_call(
        relayout,
        out_shape=(jax.ShapeDtypeStruct(tok, bf16), jax.ShapeDtypeStruct(key, f32), jax.ShapeDtypeStruct(key, f32)),
        in_specs=[pl.BlockSpec(memory_space=pltpu.VMEM)] * 2,
        out_specs=[pl.BlockSpec(memory_space=pltpu.VMEM)] * 3,
        scratch_shapes=[vmem((TOK, ROW * GRP, DIM), f32)],
        name='relayout',
    )(pltpu.with_memory_space_constraint(out_q, vmem), pltpu.with_memory_space_constraint(out_kv, vmem))


def solution(mesh):
    row_spec = P(None, CP_AXES, 'heads', None)
    stat_spec = P(None, CP_AXES, 'heads')
    key_spec = P(CP_AXES, 'heads', None)
    return jax.shard_map(call, mesh=mesh, in_specs=(row_spec, row_spec, row_spec, stat_spec, key_spec, key_spec),
                         out_specs=(row_spec, key_spec, key_spec), check_vma=False)
```

```python
import jax
import jax.numpy as jnp
from jax import lax
from jax.experimental import pallas as pl
from jax.experimental.pallas import tpu as pltpu
from jax.sharding import PartitionSpec as P

CP_AXES = ('cpo', 'cp')
MESH = pl.DeviceIdType.MESH
LOG2E = 1.4426950408889634

ROW = 8
RING = 4
GRP = 3
TOK = 16
KEYS = 32
DIM = 128
QROWS = ROW * GRP * TOK
KROWS = ROW * KEYS
PACK = GRP * TOK
SCALE = DIM ** -0.5
HOPS = RING

OWN, N1, N2, X = range(4)
GROUPS = (((0, 0), (0, 1), (0, 2), (0, 3)), ((-1, 0), (1, 0), (-1, 1), (1, 3)),
          ((-1, 3), (1, 2), (-1, 2), (1, 1)), ((2, 0), (2, 1), (2, 2), (2, 3)))
PLACE = {chunk: (group, slot) for group, chunks in enumerate(GROUPS) for slot, chunk in enumerate(chunks)}
DIRECT_KV = True
VIA_PLUS = (2, 0)

NSEM = 48
LINE_Q, LINE_KV, LINE_DQ = 50, 32, 24
SENT = (ROW - 1 + (RING - 1) * ROW) * (LINE_Q + LINE_KV) + (RING - 1) * ROW * (2 * KEYS + PACK) + (ROW - 1) * (2 * KEYS + LINE_DQ)

NT = (((1,), (1,)), ((), ()))
NN = (((1,), (0,)), ((), ()))
TN = (((0,), (0,)), ((), ()))


def dot(a, b, dims):
    return lax.dot_general(a, b, dims, preferred_element_type=jnp.float32)


def kernel(q_in, o_in, g_in, l_in, k_in, v_in, out_q, out_kv,
           q_vm, o_vm, g_vm, l_vm, k_vm, v_vm, perm_q, perm_kv, ts, tt,
           pq, pst, pkv, qd, st, kv, ld, rowc, akv, aqt, oq,
           ra_kv, rb_kv, ra_q, rb_q, fq, in_sem, ssem, rsem, gauge):
    me = lax.axis_index('cp')
    cpo = lax.axis_index('cpo')
    z, y = cpo // RING, cpo % RING
    x, core = me // 2, me % 2

    def row_dev(j):
        return (0, cpo, j)

    def along(n, queries):
        n = n % RING
        y_step = (core == 0) == queries
        return jnp.where(y_step, z, (z + n) % RING), jnp.where(y_step, (y + n) % RING, y)

    def ring_devs(queries):
        devs = []
        for n in (1, -1, 2):
            zn, yn = along(n, queries)
            devs.append((0, zn * RING + yn, me))
        return devs

    qdev, kdev = ring_devs(True), ring_devs(False)

    loads = [pltpu.make_async_copy(src, dst, in_sem.at[i // 5]) for i, (src, dst) in enumerate(
        ((g_in, g_vm), (q_in, q_vm), (k_in, k_vm), (v_in, v_vm), (o_in, o_vm), (l_in, l_vm)))]
    for ld_copy in loads:
        ld_copy.start()

    barrier = pltpu.get_barrier_semaphore()
    for j in range(1, ROW):
        pl.semaphore_signal(barrier, inc=1, device_id=row_dev((me + j) % ROW), device_id_type=MESH)
    for dev in qdev + kdev:
        pl.semaphore_signal(barrier, inc=1, device_id=dev, device_id_type=MESH)

    counter = [0]

    def take(n):
        first = counter[0]
        counter[0] += n
        assert counter[0] <= NSEM
        return first

    def remote(src, dst, recv_i, dev):
        return pltpu.make_async_remote_copy(
            src_ref=src, dst_ref=dst, send_sem=ssem.at[0], recv_sem=rsem.at[recv_i],
            device_id=dev, device_id_type=MESH)

    def lines(n):
        return gauge.at[pl.ds(0, n)]

    def arrived(n, recv_i):
        remote(lines(n), lines(n), recv_i, row_dev(me)).wait_recv()

    def chunk(ref, n, r):
        group, slot = PLACE[n, r]
        return ref.at[group, pl.ds(2 * slot, 2)]

    class Row:
        def __init__(self, size, *pairs):
            self.size, self.pairs, self.recv = size, pairs, take(HOPS)

        def send(self, *chips):
            for r in chips:
                back = (HOPS - r) % HOPS
                for c in ((0, 1) if r else (1 - core,)):
                    d = (x + r) % HOPS * 2 + c
                    for src, dst in self.pairs:
                        remote(src.at[d], dst.at[2 * back + core], self.recv + back, row_dev(d)).start()

        def wait(self, r):
            arrived(self.size * (2 if r else 1), self.recv + r)

    def permutation(ref, tokens, heads):
        n = tokens * heads
        i = lax.broadcasted_iota(jnp.int32, (n, n), 0)
        source = (i & (tokens - 1)) * heads + (i >> (tokens.bit_length() - 1))
        ref[...] = (lax.broadcasted_iota(jnp.int32, (n, n), 1) == source).astype(jnp.float32).astype(jnp.bfloat16)

    permutation(perm_q, TOK, ROW * GRP)
    permutation(perm_kv, KEYS, ROW)
    ts[...] = jnp.zeros_like(ts)
    with jax.named_scope('loads'):
        whole = lines((3 * QROWS + 2 * KROWS) // 2)
        pltpu.make_async_copy(whole, whole, in_sem.at[0]).wait()
        loads[5].wait()
    with jax.named_scope('pack'):
        prod = g_vm[...].astype(jnp.float32) * o_vm[...].astype(jnp.float32)
        delta = jnp.sum(prod.reshape(TOK, ROW * GRP, DIM), axis=-1)
        ts[pl.ds(0, TOK), pl.ds(0, ROW * GRP)] = l_vm[...].reshape(TOK, ROW * GRP)
        ts[pl.ds(TOK, TOK), pl.ds(0, ROW * GRP)] = delta
        tt[...] = ts[...].T
        rows = dot(perm_q[...], jnp.concatenate([q_vm[...], g_vm[...]], axis=1), NN).astype(jnp.bfloat16)
        for i in (0, 1):
            pq[:, pl.ds(i * GRP, GRP)] = rows[:, i * DIM:(i + 1) * DIM].reshape(ROW, GRP, TOK, DIM)
        rows = dot(perm_kv[...], jnp.concatenate([k_vm[...], v_vm[...]], axis=1), NN).astype(jnp.bfloat16)
        for i in (0, 1):
            pkv[:, i] = rows[:, i * DIM:(i + 1) * DIM].reshape(ROW, KEYS, DIM)
        lane = lax.broadcasted_iota(jnp.int32, (ROW, DIM), 1)
        for which in range(2):
            packed = jnp.zeros((ROW, DIM), jnp.float32)
            for g in range(GRP):
                rows = tt[pl.ds(g, ROW, stride=GRP), :]
                shift = (g * TOK - which * TOK) % DIM
                if shift:
                    rows = pltpu.roll(rows, shift, 1)
                packed = jnp.where((lane >= g * TOK) & (lane < (g + 1) * TOK), rows, packed)
            pst[:, which, :] = packed
    with jax.named_scope('barrier'):
        pl.semaphore_wait(barrier, ROW - 1 + 6)
    row_q = Row(LINE_Q, (pst, st.at[OWN]), (pq, qd.at[OWN]))
    row_kv = Row(LINE_KV, (pkv, kv.at[OWN]))
    row_q.send(0)
    row_kv.send(0)
    row_q.send(1)
    row_kv.send(1)
    row_q.send(3)
    row_kv.send(3)
    row_q.send(2)
    row_kv.send(2)
    st[OWN, core] = pst[me]
    qd[OWN, core] = pq[me]
    kv[OWN, core] = pkv[me]

    class Gather:
        def __init__(self, size, bufs, devs, direct=False):
            self.size, self.bufs, self.devs, self.direct = 2 * size, bufs, devs, direct
            self.recv = {at: take(1) for at in ((-1, 0), (1, 0), (-1, 1), (1, 3)) + (() if direct else ((1, 2),))}
            self.rest, self.far = take(1), take(1)

        def send(self, r, *sides):
            for side in sides:
                n = (-1, 1, 2)[side]
                recv_i = self.far if side == 2 else self.recv.get((n, r), self.rest)
                for buf in self.bufs:
                    remote(chunk(buf, 0, r), chunk(buf, n, r), recv_i, self.devs[side]).start()

        def wait(self, n, r):
            arrived(self.size, self.recv[n, r])

        def forward(self, n, r):
            self.wait(n, r)
            for buf in self.bufs:
                remote(chunk(buf, n, r), chunk(buf, 2, r), self.far, self.devs[0 if n < 0 else 1]).start()

        def wait_rest(self):
            arrived(self.size * (4 if self.direct else 3), self.rest)

        def wait_far(self):
            arrived(self.size * HOPS, self.far)

    agq, agkv = Gather(LINE_Q, (st, qd), qdev), Gather(LINE_KV, (kv,), kdev, DIRECT_KV)

    def pass_on(row, gather, r):
        row.wait(r)
        if r == 0:
            gather.send(0, 0, 1)
        elif r == 1:
            gather.send(1, 0)
        elif r == 3:
            gather.send(3, 1, 0)
        elif gather.direct:
            gather.send(2, 1, 0)
            gather.send(1, 1)
            gather.send(2, 2)
        else:
            gather.send(2, 1)
            gather.send(1, 1)
            gather.send(2, 0)

    with jax.named_scope('row_0'):
        pass_on(row_q, agq, 0)
        pass_on(row_kv, agkv, 0)

    r_id = lax.broadcasted_iota(jnp.int32, (1, QROWS), 1)
    packet = (r_id * 1366) >> 16
    token = ((r_id >> 3) & 1) * 1024 + (packet & 1) * 8 + (r_id & 7) + 2048
    for group in range(RING):
        spot = jnp.zeros_like(token)
        for slot, (n, r) in enumerate(GROUPS[group]):
            zq, yq = along(n, True)
            spot = jnp.where((packet >> 1) == slot, zq * 256 + yq * 64 + (x + r) % HOPS * 16, spot)
        rowc[group] = token + spot

    src_id = (3 * lax.broadcasted_iota(jnp.int32, (ROW, DIM), 0)) & 7

    def assemble(group):
        for which in range(2):
            rows = []
            for i in range(ROW):
                rows.append(st[group, pl.ds(3 * i % ROW, 1), which, :])
            rows = pltpu.roll(jnp.concatenate(rows, axis=0), 0, 1, stride=TOK, stride_axis=0)
            for k in range(QROWS // DIM):
                mine = (((lane + k * DIM) * 1366) >> 16) == src_id
                line = jnp.sum(jnp.where(mine, rows, 0.0), axis=0, keepdims=True)
                ld[group, pl.ds(which, 1), pl.ds(k * DIM, DIM)] = line * LOG2E if which == 0 else line

    class Scatter:
        def __init__(self, size, acc, ra, rb, devs):
            self.size, self.acc, self.ra, self.rb, self.devs = 2 * size, acc, ra, rb, devs
            self.first, self.near = take(HOPS), take(HOPS)

        def send_far(self, r):
            side = 0 if r in VIA_PLUS else 1
            remote(chunk(self.acc, 2, r), self.ra.at[r], self.first + r, self.devs[side]).start()

        def send_near(self, side, r):
            remote(chunk(self.acc, -1 if side else 1, r), self.rb.at[side, r], self.near + r, self.devs[side]).start()

        def send_early(self, r):
            self.send_near(1 if r in VIA_PLUS else 0, r)

        def send_late(self, r):
            side = 0 if r in VIA_PLUS else 1
            arrived(self.size, self.first + r)
            mine = chunk(self.acc, -1 if side else 1, r)
            mine[...] = mine[...] + self.ra[r]
            self.send_near(side, r)

        def total(self, r):
            arrived(2 * self.size, self.near + r)
            return chunk(self.acc, 0, r)[...] + self.rb[0, r] + self.rb[1, r]

    rsk, rsv = (Scatter(KEYS, akv.at[i], ra_kv.at[i], rb_kv.at[i], kdev) for i in (0, 1))
    rsq = Scatter(PACK, oq, ra_q, rb_q, qdev)

    band_rows = KROWS // HOPS
    key_row = lax.broadcasted_iota(jnp.int32, (band_rows, QROWS), 0)
    begun = set()

    def add(ref, name, value):
        ref[...] = ref[...] + value if name in begun else value
        begun.add(name)

    def tile(qs, ks):
        with jax.named_scope('tile' + ''.join(map(str, qs)) + 'x' + ''.join(map(str, ks))):
            q = jnp.concatenate([qd[i, :, pl.ds(0, GRP)].reshape(QROWS, DIM) for i in qs], axis=0)
            g = jnp.concatenate([qd[i, :, pl.ds(GRP, GRP)].reshape(QROWS, DIM) for i in qs], axis=0)
            k = jnp.concatenate([kv[i, :, 0].reshape(KROWS, DIM) for i in ks], axis=0)
            v = jnp.concatenate([kv[i, :, 1].reshape(KROWS, DIM) for i in ks], axis=0)
            lse = jnp.concatenate([ld[i, pl.ds(0, 1), :] for i in qs], axis=1)
            dlt = jnp.concatenate([ld[i, pl.ds(1, 1), :] for i in qs], axis=1)
            expo = jnp.exp2(dot(k, q, NT) * (SCALE * LOG2E) - lse)
            bands = []
            for n, r in [at for i in ks for at in GROUPS[i]]:
                zk, yk = along(n, False)
                first = zk * 1024 + yk * 256 + (x + r) % HOPS * band_rows
                seen = jnp.concatenate([key_row <= rowc[i] - first for i in qs], axis=1)
                at = len(bands) * band_rows
                bands.append(jnp.where(seen, expo[at:at + band_rows], 0.0))
            p_t = jnp.concatenate(bands, axis=0)
            dp_t = dot(v, g, NT)
            ds_t = (p_t * (dp_t - dlt)).astype(jnp.bfloat16)
            dv = dot(p_t.astype(jnp.bfloat16), g, NN)
            dk = dot(ds_t, q, NN)
            dq = dot(k, ds_t, TN)
            for n, i in enumerate(ks):
                add(akv.at[1, i], ('v', i), dv[n * KROWS:(n + 1) * KROWS].reshape(ROW, KEYS, DIM))
                add(akv.at[0, i], ('k', i), dk[n * KROWS:(n + 1) * KROWS].reshape(ROW, KEYS, DIM))
            for n, i in enumerate(qs):
                add(aqt.at[i], ('q', i), dq[:, n * QROWS:(n + 1) * QROWS])

    def finish_q(group):
        oq[group] = aqt[group].T.reshape(ROW, PACK, DIM)

    for r in (1, 3, 2):
        for name, row, gather in (('', row_q, agq), ('kv', row_kv, agkv)):
            with jax.named_scope(f'row_{name}{r}'):
                pass_on(row, gather, r)
    assemble(OWN)
    tile([OWN], [OWN])
    with jax.named_scope('fwd_0'):
        agq.forward(-1, 0)
        agkv.forward(-1, 0)
    with jax.named_scope('fwd_q1'):
        agq.forward(-1, 1)
        agq.forward(1, 3)
        agq.wait(1, 0)
        assemble(N1)
    tile([N1], [OWN])
    with jax.named_scope('fwd_k1'):
        agkv.forward(-1, 1)
        agkv.forward(1, 3)
    with jax.named_scope('fwd_q2'):
        agq.forward(1, 2)
    with jax.named_scope('fwd_k2'):
        if not DIRECT_KV:
            agkv.forward(1, 2)
        agkv.wait(1, 0)
    tile([OWN, N1], [N1])
    with jax.named_scope('rest_k'):
        agkv.wait_rest()
    tile([OWN, N1], [N2])
    with jax.named_scope('rest_q'):
        agq.wait_rest()
        assemble(N2)
    tile([N2], [OWN, N1, N2])
    with jax.named_scope('far_k'):
        agkv.wait_far()
    tile([OWN, N1, N2], [X])
    with jax.named_scope('far_q'):
        agq.wait_far()
        assemble(X)
    tile([X], [X])
    for pair in ((2, 1), (0, 3)):
        for scatter in (rsv, rsk):
            for r in pair:
                scatter.send_far(r)
    tile([X], [N1, N2, OWN])
    finish_q(X)
    rsq.send_far(2)
    rsq.send_far(1)

    @pl.when(core == 0)
    def _():
        rsq.send_far(0)
        rsq.send_far(3)

    for scatter in (rsv, rsk):
        scatter.send_early(1)
        scatter.send_early(2)
    with jax.named_scope('finish'):
        finish_q(N1)
        finish_q(N2)

    @pl.when(core == 0)
    def _():
        rsq.send_early(1)
        rsq.send_early(2)

    finish_q(OWN)

    def late(name, scatter, *chunks):
        with jax.named_scope(f'late_{name}{chunks[0]}'):
            for r in chunks:
                scatter.send_late(r)

    class Give:
        def __init__(self, size, src, dst):
            self.size, self.src, self.dst, self.recv_i = size, src, dst, take(1)

        def send(self, r):
            for c in ((0, 1) if r else (1 - core,)):
                d = (x + r) % HOPS * 2 + c
                remote(self.src.at[2 * r + c], self.dst.at[me], self.recv_i, row_dev(d)).start()

        def wait(self):
            arrived(self.size * (ROW - 1), self.recv_i)

    give_k, give_v, give_q = Give(KEYS, akv.at[0, OWN], out_kv.at[0]), Give(KEYS, akv.at[1, OWN], out_kv.at[1]), Give(LINE_DQ, fq, out_q)

    def total(name, r):
        part = pl.ds(2 * r, 2)
        with jax.named_scope(f'total_{name}{r}'):
            if name == 'v':
                akv[1, OWN, part] = rsv.total(r)
            elif name == 'k':
                akv[0, OWN, part] = rsk.total(r) * SCALE
            else:
                fq[part] = (rsq.total(r) * SCALE).astype(jnp.bfloat16)
        {'v': give_v, 'k': give_k, 'q': give_q}[name].send(r)

    def early(r):
        rsv.send_early(r)
        rsk.send_early(r)

    def totals(names, *chunks):
        for r in chunks:
            for name in names:
                total(name, r)

    late('v', rsv, 2, 1)
    late('k', rsk, 2, 1)

    @pl.when(core == 0)
    def _():
        early(3)
        late('v', rsv, 3)
        late('k', rsk, 3)
        late('q', rsq, 2, 1)
        rsq.send_early(3)
        late('q', rsq, 3)
        late('v', rsv, 0)
        late('k', rsk, 0)
        early(0)
        late('q', rsq, 0)
        rsq.send_early(0)
        totals('vk', 2, 1, 3)
        totals('q', 2, 1, 3)
        totals('vkq', 0)

    @pl.when(core == 1)
    def _():
        rsq.send_far(0)
        rsq.send_far(3)
        rsq.send_early(1)
        rsq.send_early(2)
        early(3)
        late('v', rsv, 3)
        late('k', rsk, 3)
        late('q', rsq, 2, 1)
        rsq.send_early(3)
        totals('vk', 2, 1)
        late('q', rsq, 3)
        totals('vk', 3)
        late('v', rsv, 0)
        late('k', rsk, 0)
        early(0)
        late('q', rsq, 0)
        rsq.send_early(0)
        totals('q', 2, 1, 3)
        totals('vkq', 0)

    out_q[me] = fq[core]
    out_kv[0, me] = akv[0, OWN, core]
    out_kv[1, me] = akv[1, OWN, core]

    with jax.named_scope('final_q'):
        give_q.wait()
    with jax.named_scope('final_kv'):
        give_v.wait()
        give_k.wait()
    with jax.named_scope('drain'):
        remote(lines(SENT), lines(SENT), 0, row_dev(me)).wait_send()


def relayout(q_ref, kv_ref, dq_ref, dk_ref, dv_ref, rows):
    for h in range(ROW):
        dk_ref[:, h, :] = kv_ref[0, h]
        dv_ref[:, h, :] = kv_ref[1, h]
        for g in range(GRP):
            rows[:, h * GRP + g, :] = q_ref[h, pl.ds(g * TOK, TOK), :].astype(jnp.float32)
    dq_ref[...] = rows[...].astype(jnp.bfloat16).reshape(dq_ref.shape)


def call(queries, attn_out, grad_out, log_sum_exp, key_cache, value_cache):
    f32, bf16 = jnp.float32, jnp.bfloat16
    vmem = pltpu.VMEM
    tok = (2, TOK // 2, ROW * GRP, DIM)
    key = (KEYS, ROW, DIM)
    tok2, key2 = (QROWS, DIM), (KROWS, DIM)
    scratch = [
        vmem(tok2, bf16), vmem(tok2, bf16), vmem(tok2, bf16), vmem(tok[:3], f32), vmem(key2, bf16), vmem(key2, bf16),
        vmem((QROWS, QROWS), bf16), vmem((KROWS, KROWS), bf16), vmem((DIM, DIM), f32), vmem((DIM, DIM), f32),
        vmem((ROW, 2 * GRP, TOK, DIM), bf16), vmem((ROW, 2, DIM), f32), vmem((ROW, 2, KEYS, DIM), bf16),
        vmem((RING, ROW, 2 * GRP, TOK, DIM), bf16), vmem((RING, ROW, 2, DIM), f32), vmem((RING, ROW, 2, KEYS, DIM), bf16),
        vmem((RING, 8, QROWS), f32), vmem((RING, 1, QROWS), jnp.int32),
        vmem((2, RING, ROW, KEYS, DIM), f32), vmem((RING, DIM, QROWS), f32), vmem((RING, ROW, PACK, DIM), f32),
        vmem((2, HOPS, 2, KEYS, DIM), f32), vmem((2, 2, HOPS, 2, KEYS, DIM), f32),
        vmem((HOPS, 2, PACK, DIM), f32), vmem((2, HOPS, 2, PACK, DIM), f32),
        vmem((ROW, PACK, DIM), bf16),
        pltpu.SemaphoreType.DMA((2,)), pltpu.SemaphoreType.DMA((1,)), pltpu.SemaphoreType.DMA((NSEM,)),
        vmem((SENT, DIM), f32),
    ]
    out_q, out_kv = pl.pallas_call(
        kernel,
        out_shape=(vmem((ROW, PACK, DIM), bf16), vmem((2, ROW, KEYS, DIM), f32)),
        in_specs=[pl.BlockSpec(memory_space=pl.ANY)] * 6,
        out_specs=[pl.BlockSpec(memory_space=pltpu.VMEM)] * 2,
        scratch_shapes=scratch,
        compiler_params=pltpu.CompilerParams(collective_id=0, has_side_effects=True),
        name='attn_bwd_3d',
    )(queries.reshape(tok2), attn_out.reshape(tok2), grad_out.reshape(tok2), log_sum_exp,
      key_cache.reshape(key2), value_cache.reshape(key2))
    return pl.pallas_call(
        relayout,
        out_shape=(jax.ShapeDtypeStruct(tok, bf16), jax.ShapeDtypeStruct(key, f32), jax.ShapeDtypeStruct(key, f32)),
        in_specs=[pl.BlockSpec(memory_space=pltpu.VMEM)] * 2,
        out_specs=[pl.BlockSpec(memory_space=pltpu.VMEM)] * 3,
        scratch_shapes=[vmem((TOK, ROW * GRP, DIM), f32)],
        name='relayout',
    )(pltpu.with_memory_space_constraint(out_q, vmem), pltpu.with_memory_space_constraint(out_kv, vmem))


def solution(mesh):
    row_spec = P(None, CP_AXES, 'heads', None)
    stat_spec = P(None, CP_AXES, 'heads')
    key_spec = P(CP_AXES, 'heads', None)
    return jax.shard_map(call, mesh=mesh, in_specs=(row_spec, row_spec, row_spec, stat_spec, key_spec, key_spec),
                         out_specs=(row_spec, key_spec, key_spec), check_vma=False)
```

```python
import jax
import jax.numpy as jnp
from jax import lax
from jax.experimental import pallas as pl
from jax.experimental.pallas import tpu as pltpu
from jax.sharding import PartitionSpec as P

CP_AXES = ('cpo', 'cp')
MESH = pl.DeviceIdType.MESH
LOG2E = 1.4426950408889634

ROW = 8
RING = 4
GRP = 3
TOK = 16
KEYS = 32
DIM = 128
QROWS = ROW * GRP * TOK
KROWS = ROW * KEYS
PACK = GRP * TOK
SCALE = DIM ** -0.5
HOPS = RING

OWN, N1, N2, X = range(4)
GROUPS = (((0, 0), (0, 1), (0, 2), (0, 3)), ((-1, 0), (1, 0), (-1, 1), (1, 3)),
          ((-1, 3), (1, 2), (-1, 2), (1, 1)), ((2, 0), (2, 1), (2, 2), (2, 3)))
PLACE = {chunk: (group, slot) for group, chunks in enumerate(GROUPS) for slot, chunk in enumerate(chunks)}
DIRECT_KV = True
VIA_PLUS = (2, 0)

NSEM = 48
LINE_Q, LINE_KV, LINE_DQ = 50, 32, 24
SENT = (ROW - 1 + (RING - 1) * ROW) * (LINE_Q + LINE_KV) + (RING - 1) * ROW * (2 * KEYS + PACK) + (ROW - 1) * (2 * KEYS + LINE_DQ)

NT = (((1,), (1,)), ((), ()))
NN = (((1,), (0,)), ((), ()))
TN = (((0,), (0,)), ((), ()))


def dot(a, b, dims):
    return lax.dot_general(a, b, dims, preferred_element_type=jnp.float32)


def kernel(q_in, o_in, g_in, l_in, k_in, v_in, out_q, out_kv,
           q_vm, o_vm, g_vm, l_vm, k_vm, v_vm, perm_q, perm_kv, ts, tt,
           pq, pst, pkv, qd, st, kv, ld, rowc, akv, aqt, oq,
           ra_kv, rb_kv, ra_q, rb_q, fq, in_sem, ssem, rsem, gauge):
    me = lax.axis_index('cp')
    cpo = lax.axis_index('cpo')
    z, y = cpo // RING, cpo % RING
    x, core = me // 2, me % 2

    def row_dev(j):
        return (0, cpo, j)

    def along(n, queries):
        n = n % RING
        y_step = (core == 0) == queries
        return jnp.where(y_step, z, (z + n) % RING), jnp.where(y_step, (y + n) % RING, y)

    def ring_devs(queries):
        devs = []
        for n in (1, -1, 2):
            zn, yn = along(n, queries)
            devs.append((0, zn * RING + yn, me))
        return devs

    qdev, kdev = ring_devs(True), ring_devs(False)

    loads = [pltpu.make_async_copy(src, dst, in_sem.at[i // 5]) for i, (src, dst) in enumerate(
        ((g_in, g_vm), (q_in, q_vm), (k_in, k_vm), (v_in, v_vm), (o_in, o_vm), (l_in, l_vm)))]
    for ld_copy in loads:
        ld_copy.start()

    barrier = pltpu.get_barrier_semaphore()
    for j in range(1, ROW):
        pl.semaphore_signal(barrier, inc=1, device_id=row_dev((me + j) % ROW), device_id_type=MESH)
    for dev in qdev + kdev:
        pl.semaphore_signal(barrier, inc=1, device_id=dev, device_id_type=MESH)

    counter = [0]

    def take(n):
        first = counter[0]
        counter[0] += n
        assert counter[0] <= NSEM
        return first

    def remote(src, dst, recv_i, dev):
        return pltpu.make_async_remote_copy(
            src_ref=src, dst_ref=dst, send_sem=ssem.at[0], recv_sem=rsem.at[recv_i],
            device_id=dev, device_id_type=MESH)

    def lines(n):
        return gauge.at[pl.ds(0, n)]

    def arrived(n, recv_i):
        remote(lines(n), lines(n), recv_i, row_dev(me)).wait_recv()

    def chunk(ref, n, r):
        group, slot = PLACE[n, r]
        return ref.at[group, pl.ds(2 * slot, 2)]

    class Row:
        def __init__(self, size, *pairs):
            self.size, self.pairs, self.recv = size, pairs, take(HOPS)

        def send(self, *chips):
            for r in chips:
                back = (HOPS - r) % HOPS
                for c in ((0, 1) if r else (1 - core,)):
                    d = (x + r) % HOPS * 2 + c
                    for src, dst in self.pairs:
                        remote(src.at[d], dst.at[2 * back + core], self.recv + back, row_dev(d)).start()

        def wait(self, r):
            arrived(self.size * (2 if r else 1), self.recv + r)

    def permutation(ref, tokens, heads):
        n = tokens * heads
        i = lax.broadcasted_iota(jnp.int32, (n, n), 0)
        source = (i & (tokens - 1)) * heads + (i >> (tokens.bit_length() - 1))
        ref[...] = (lax.broadcasted_iota(jnp.int32, (n, n), 1) == source).astype(jnp.float32).astype(jnp.bfloat16)

    permutation(perm_q, TOK, ROW * GRP)
    permutation(perm_kv, KEYS, ROW)
    ts[...] = jnp.zeros_like(ts)
    with jax.named_scope('loads'):
        whole = lines((3 * QROWS + 2 * KROWS) // 2)
        pltpu.make_async_copy(whole, whole, in_sem.at[0]).wait()
        loads[5].wait()
    with jax.named_scope('pack'):
        prod = g_vm[...].astype(jnp.float32) * o_vm[...].astype(jnp.float32)
        delta = jnp.sum(prod.reshape(TOK, ROW * GRP, DIM), axis=-1)
        ts[pl.ds(0, TOK), pl.ds(0, ROW * GRP)] = l_vm[...].reshape(TOK, ROW * GRP)
        ts[pl.ds(TOK, TOK), pl.ds(0, ROW * GRP)] = delta
        tt[...] = ts[...].T
        rows = dot(perm_q[...], jnp.concatenate([q_vm[...], g_vm[...]], axis=1), NN).astype(jnp.bfloat16)
        for i in (0, 1):
            pq[:, pl.ds(i * GRP, GRP)] = rows[:, i * DIM:(i + 1) * DIM].reshape(ROW, GRP, TOK, DIM)
        rows = dot(perm_kv[...], jnp.concatenate([k_vm[...], v_vm[...]], axis=1), NN).astype(jnp.bfloat16)
        for i in (0, 1):
            pkv[:, i] = rows[:, i * DIM:(i + 1) * DIM].reshape(ROW, KEYS, DIM)
        lane = lax.broadcasted_iota(jnp.int32, (ROW, DIM), 1)
        for which in range(2):
            packed = jnp.zeros((ROW, DIM), jnp.float32)
            for g in range(GRP):
                rows = tt[pl.ds(g, ROW, stride=GRP), :]
                shift = (g * TOK - which * TOK) % DIM
                if shift:
                    rows = pltpu.roll(rows, shift, 1)
                packed = jnp.where((lane >= g * TOK) & (lane < (g + 1) * TOK), rows, packed)
            pst[:, which, :] = packed
    with jax.named_scope('barrier'):
        pl.semaphore_wait(barrier, ROW - 1 + 6)
    row_q = Row(LINE_Q, (pst, st.at[OWN]), (pq, qd.at[OWN]))
    row_kv = Row(LINE_KV, (pkv, kv.at[OWN]))
    row_q.send(0)
    row_kv.send(0)
    row_q.send(3)
    row_kv.send(3)
    row_q.send(1)
    row_kv.send(1)
    row_q.send(2)
    row_kv.send(2)
    st[OWN, core] = pst[me]
    qd[OWN, core] = pq[me]
    kv[OWN, core] = pkv[me]

    class Gather:
        def __init__(self, size, bufs, devs, direct=False):
            self.size, self.bufs, self.devs, self.direct = 2 * size, bufs, devs, direct
            self.recv = {at: take(1) for at in ((-1, 0), (1, 0), (-1, 1), (1, 3)) + (() if direct else ((1, 2),))}
            self.rest, self.far = take(1), take(1)

        def send(self, r, *sides):
            for side in sides:
                n = (-1, 1, 2)[side]
                recv_i = self.far if side == 2 else self.recv.get((n, r), self.rest)
                for buf in self.bufs:
                    remote(chunk(buf, 0, r), chunk(buf, n, r), recv_i, self.devs[side]).start()

        def wait(self, n, r):
            arrived(self.size, self.recv[n, r])

        def forward(self, n, r):
            self.wait(n, r)
            for buf in self.bufs:
                remote(chunk(buf, n, r), chunk(buf, 2, r), self.far, self.devs[0 if n < 0 else 1]).start()

        def wait_rest(self):
            arrived(self.size * (4 if self.direct else 3), self.rest)

        def wait_far(self):
            arrived(self.size * HOPS, self.far)

    agq, agkv = Gather(LINE_Q, (st, qd), qdev), Gather(LINE_KV, (kv,), kdev, DIRECT_KV)

    def pass_on(row, gather, r):
        row.wait(r)
        if r == 0:
            gather.send(0, 0, 1)
        elif r == 1:
            gather.send(1, 0)
        elif r == 3:
            gather.send(3, 1, 0)
        elif gather.direct:
            gather.send(2, 1, 0)
            gather.send(1, 1)
            gather.send(2, 2)
        else:
            gather.send(2, 1)
            gather.send(1, 1)
            gather.send(2, 0)

    with jax.named_scope('row_0'):
        pass_on(row_q, agq, 0)
        pass_on(row_kv, agkv, 0)

    r_id = lax.broadcasted_iota(jnp.int32, (1, QROWS), 1)
    packet = (r_id * 1366) >> 16
    token = ((r_id >> 3) & 1) * 1024 + (packet & 1) * 8 + (r_id & 7) + 2048
    for group in range(RING):
        spot = jnp.zeros_like(token)
        for slot, (n, r) in enumerate(GROUPS[group]):
            zq, yq = along(n, True)
            spot = jnp.where((packet >> 1) == slot, zq * 256 + yq * 64 + (x + r) % HOPS * 16, spot)
        rowc[group] = token + spot

    src_id = (3 * lax.broadcasted_iota(jnp.int32, (ROW, DIM), 0)) & 7

    def assemble(group):
        for which in range(2):
            rows = []
            for i in range(ROW):
                rows.append(st[group, pl.ds(3 * i % ROW, 1), which, :])
            rows = pltpu.roll(jnp.concatenate(rows, axis=0), 0, 1, stride=TOK, stride_axis=0)
            for k in range(QROWS // DIM):
                mine = (((lane + k * DIM) * 1366) >> 16) == src_id
                line = jnp.sum(jnp.where(mine, rows, 0.0), axis=0, keepdims=True)
                ld[group, pl.ds(which, 1), pl.ds(k * DIM, DIM)] = line * LOG2E if which == 0 else line

    class Scatter:
        def __init__(self, size, acc, ra, rb, devs):
            self.size, self.acc, self.ra, self.rb, self.devs = 2 * size, acc, ra, rb, devs
            self.first, self.near = take(HOPS), take(HOPS)

        def send_far(self, r):
            side = 0 if r in VIA_PLUS else 1
            remote(chunk(self.acc, 2, r), self.ra.at[r], self.first + r, self.devs[side]).start()

        def send_near(self, side, r):
            remote(chunk(self.acc, -1 if side else 1, r), self.rb.at[side, r], self.near + r, self.devs[side]).start()

        def send_early(self, r):
            self.send_near(1 if r in VIA_PLUS else 0, r)

        def send_late(self, r):
            side = 0 if r in VIA_PLUS else 1
            arrived(self.size, self.first + r)
            mine = chunk(self.acc, -1 if side else 1, r)
            mine[...] = mine[...] + self.ra[r]
            self.send_near(side, r)

        def total(self, r):
            arrived(2 * self.size, self.near + r)
            return chunk(self.acc, 0, r)[...] + self.rb[0, r] + self.rb[1, r]

    rsk, rsv = (Scatter(KEYS, akv.at[i], ra_kv.at[i], rb_kv.at[i], kdev) for i in (0, 1))
    rsq = Scatter(PACK, oq, ra_q, rb_q, qdev)

    band_rows = KROWS // HOPS
    key_row = lax.broadcasted_iota(jnp.int32, (band_rows, QROWS), 0)
    begun = set()

    def add(ref, name, value):
        ref[...] = ref[...] + value if name in begun else value
        begun.add(name)

    def tile(qs, ks):
        with jax.named_scope('tile' + ''.join(map(str, qs)) + 'x' + ''.join(map(str, ks))):
            q = jnp.concatenate([qd[i, :, pl.ds(0, GRP)].reshape(QROWS, DIM) for i in qs], axis=0)
            g = jnp.concatenate([qd[i, :, pl.ds(GRP, GRP)].reshape(QROWS, DIM) for i in qs], axis=0)
            k = jnp.concatenate([kv[i, :, 0].reshape(KROWS, DIM) for i in ks], axis=0)
            v = jnp.concatenate([kv[i, :, 1].reshape(KROWS, DIM) for i in ks], axis=0)
            lse = jnp.concatenate([ld[i, pl.ds(0, 1), :] for i in qs], axis=1)
            dlt = jnp.concatenate([ld[i, pl.ds(1, 1), :] for i in qs], axis=1)
            expo = jnp.exp2(dot(k, q, NT) * (SCALE * LOG2E) - lse)
            bands = []
            for n, r in [at for i in ks for at in GROUPS[i]]:
                zk, yk = along(n, False)
                first = zk * 1024 + yk * 256 + (x + r) % HOPS * band_rows
                seen = jnp.concatenate([key_row <= rowc[i] - first for i in qs], axis=1)
                at = len(bands) * band_rows
                bands.append(jnp.where(seen, expo[at:at + band_rows], 0.0))
            p_t = jnp.concatenate(bands, axis=0)
            dp_t = dot(v, g, NT)
            ds_t = (p_t * (dp_t - dlt)).astype(jnp.bfloat16)
            dv = dot(p_t.astype(jnp.bfloat16), g, NN)
            dk = dot(ds_t, q, NN)
            dq = dot(k, ds_t, TN)
            for n, i in enumerate(ks):
                add(akv.at[1, i], ('v', i), dv[n * KROWS:(n + 1) * KROWS].reshape(ROW, KEYS, DIM))
                add(akv.at[0, i], ('k', i), dk[n * KROWS:(n + 1) * KROWS].reshape(ROW, KEYS, DIM))
            for n, i in enumerate(qs):
                add(aqt.at[i], ('q', i), dq[:, n * QROWS:(n + 1) * QROWS])

    def finish_q(group):
        oq[group] = aqt[group].T.reshape(ROW, PACK, DIM)

    for r in (1, 3, 2):
        for name, row, gather in (('', row_q, agq), ('kv', row_kv, agkv)):
            with jax.named_scope(f'row_{name}{r}'):
                pass_on(row, gather, r)
    assemble(OWN)
    tile([OWN], [OWN])
    with jax.named_scope('fwd_0'):
        agq.forward(-1, 0)
        agkv.forward(-1, 0)
    with jax.named_scope('fwd_q1'):
        agq.forward(-1, 1)
        agq.forward(1, 3)
        agq.wait(1, 0)
        assemble(N1)
    tile([N1], [OWN])
    with jax.named_scope('fwd_k1'):
        agkv.forward(-1, 1)
        agkv.forward(1, 3)
    with jax.named_scope('fwd_q2'):
        agq.forward(1, 2)
    with jax.named_scope('fwd_k2'):
        if not DIRECT_KV:
            agkv.forward(1, 2)
        agkv.wait(1, 0)
    tile([OWN, N1], [N1])
    with jax.named_scope('rest_k'):
        agkv.wait_rest()
    tile([OWN, N1], [N2])
    with jax.named_scope('rest_q'):
        agq.wait_rest()
        assemble(N2)
    tile([N2], [OWN, N1, N2])
    with jax.named_scope('far_k'):
        agkv.wait_far()
    tile([OWN, N1, N2], [X])
    with jax.named_scope('far_q'):
        agq.wait_far()
        assemble(X)
    tile([X], [X])
    for pair in ((2, 1), (0, 3)):
        for scatter in (rsv, rsk):
            for r in pair:
                scatter.send_far(r)
    tile([X], [N1, N2, OWN])
    finish_q(X)
    rsq.send_far(2)
    rsq.send_far(1)

    @pl.when(core == 0)
    def _():
        rsq.send_far(0)
        rsq.send_far(3)

    for scatter in (rsv, rsk):
        scatter.send_early(1)
        scatter.send_early(2)
    with jax.named_scope('finish'):
        finish_q(N1)
        finish_q(N2)

    @pl.when(core == 0)
    def _():
        rsq.send_early(1)
        rsq.send_early(2)

    finish_q(OWN)

    def late(name, scatter, *chunks):
        with jax.named_scope(f'late_{name}{chunks[0]}'):
            for r in chunks:
                scatter.send_late(r)

    class Give:
        def __init__(self, size, src, dst):
            self.size, self.src, self.dst, self.recv_i = size, src, dst, take(1)

        def send(self, r):
            for c in ((0, 1) if r else (1 - core,)):
                d = (x + r) % HOPS * 2 + c
                remote(self.src.at[2 * r + c], self.dst.at[me], self.recv_i, row_dev(d)).start()

        def wait(self):
            arrived(self.size * (ROW - 1), self.recv_i)

    give_k, give_v, give_q = Give(KEYS, akv.at[0, OWN], out_kv.at[0]), Give(KEYS, akv.at[1, OWN], out_kv.at[1]), Give(LINE_DQ, fq, out_q)

    def total(name, r):
        part = pl.ds(2 * r, 2)
        with jax.named_scope(f'total_{name}{r}'):
            if name == 'v':
                akv[1, OWN, part] = rsv.total(r)
            elif name == 'k':
                akv[0, OWN, part] = rsk.total(r) * SCALE
            else:
                fq[part] = (rsq.total(r) * SCALE).astype(jnp.bfloat16)
        {'v': give_v, 'k': give_k, 'q': give_q}[name].send(r)

    def early(r):
        rsv.send_early(r)
        rsk.send_early(r)

    def totals(names, *chunks):
        for r in chunks:
            for name in names:
                total(name, r)

    late('v', rsv, 2, 1)
    late('k', rsk, 2, 1)

    @pl.when(core == 0)
    def _():
        early(3)
        late('v', rsv, 3)
        late('k', rsk, 3)
        late('q', rsq, 2, 1)
        rsq.send_early(3)
        late('q', rsq, 3)
        late('v', rsv, 0)
        late('k', rsk, 0)
        early(0)
        late('q', rsq, 0)
        rsq.send_early(0)
        totals('vk', 2, 1, 3)
        totals('q', 2, 1, 3)
        totals('vkq', 0)

    @pl.when(core == 1)
    def _():
        rsq.send_far(0)
        rsq.send_far(3)
        rsq.send_early(1)
        rsq.send_early(2)
        early(3)
        late('v', rsv, 3)
        late('k', rsk, 3)
        late('q', rsq, 2, 1)
        rsq.send_early(3)
        totals('vk', 2, 1)
        late('q', rsq, 3)
        totals('vk', 3)
        late('v', rsv, 0)
        late('k', rsk, 0)
        early(0)
        late('q', rsq, 0)
        rsq.send_early(0)
        totals('q', 2, 1, 3)
        totals('vkq', 0)

    out_q[me] = fq[core]
    out_kv[0, me] = akv[0, OWN, core]
    out_kv[1, me] = akv[1, OWN, core]

    with jax.named_scope('final_q'):
        give_q.wait()
    with jax.named_scope('final_kv'):
        give_v.wait()
        give_k.wait()
    with jax.named_scope('drain'):
        remote(lines(SENT), lines(SENT), 0, row_dev(me)).wait_send()


def relayout(q_ref, kv_ref, dq_ref, dk_ref, dv_ref, rows):
    for h in range(ROW):
        dk_ref[:, h, :] = kv_ref[0, h]
        dv_ref[:, h, :] = kv_ref[1, h]
        for g in range(GRP):
            rows[:, h * GRP + g, :] = q_ref[h, pl.ds(g * TOK, TOK), :].astype(jnp.float32)
    dq_ref[...] = rows[...].astype(jnp.bfloat16).reshape(dq_ref.shape)


def call(queries, attn_out, grad_out, log_sum_exp, key_cache, value_cache):
    f32, bf16 = jnp.float32, jnp.bfloat16
    vmem = pltpu.VMEM
    tok = (2, TOK // 2, ROW * GRP, DIM)
    key = (KEYS, ROW, DIM)
    tok2, key2 = (QROWS, DIM), (KROWS, DIM)
    scratch = [
        vmem(tok2, bf16), vmem(tok2, bf16), vmem(tok2, bf16), vmem(tok[:3], f32), vmem(key2, bf16), vmem(key2, bf16),
        vmem((QROWS, QROWS), bf16), vmem((KROWS, KROWS), bf16), vmem((DIM, DIM), f32), vmem((DIM, DIM), f32),
        vmem((ROW, 2 * GRP, TOK, DIM), bf16), vmem((ROW, 2, DIM), f32), vmem((ROW, 2, KEYS, DIM), bf16),
        vmem((RING, ROW, 2 * GRP, TOK, DIM), bf16), vmem((RING, ROW, 2, DIM), f32), vmem((RING, ROW, 2, KEYS, DIM), bf16),
        vmem((RING, 8, QROWS), f32), vmem((RING, 1, QROWS), jnp.int32),
        vmem((2, RING, ROW, KEYS, DIM), f32), vmem((RING, DIM, QROWS), f32), vmem((RING, ROW, PACK, DIM), f32),
        vmem((2, HOPS, 2, KEYS, DIM), f32), vmem((2, 2, HOPS, 2, KEYS, DIM), f32),
        vmem((HOPS, 2, PACK, DIM), f32), vmem((2, HOPS, 2, PACK, DIM), f32),
        vmem((ROW, PACK, DIM), bf16),
        pltpu.SemaphoreType.DMA((2,)), pltpu.SemaphoreType.DMA((1,)), pltpu.SemaphoreType.DMA((NSEM,)),
        vmem((SENT, DIM), f32),
    ]
    out_q, out_kv = pl.pallas_call(
        kernel,
        out_shape=(vmem((ROW, PACK, DIM), bf16), vmem((2, ROW, KEYS, DIM), f32)),
        in_specs=[pl.BlockSpec(memory_space=pl.ANY)] * 6,
        out_specs=[pl.BlockSpec(memory_space=pltpu.VMEM)] * 2,
        scratch_shapes=scratch,
        compiler_params=pltpu.CompilerParams(collective_id=0, has_side_effects=True),
        name='attn_bwd_3d',
    )(queries.reshape(tok2), attn_out.reshape(tok2), grad_out.reshape(tok2), log_sum_exp,
      key_cache.reshape(key2), value_cache.reshape(key2))
    return pl.pallas_call(
        relayout,
        out_shape=(jax.ShapeDtypeStruct(tok, bf16), jax.ShapeDtypeStruct(key, f32), jax.ShapeDtypeStruct(key, f32)),
        in_specs=[pl.BlockSpec(memory_space=pltpu.VMEM)] * 2,
        out_specs=[pl.BlockSpec(memory_space=pltpu.VMEM)] * 3,
        scratch_shapes=[vmem((TOK, ROW * GRP, DIM), f32)],
        name='relayout',
    )(pltpu.with_memory_space_constraint(out_q, vmem), pltpu.with_memory_space_constraint(out_kv, vmem))


def solution(mesh):
    row_spec = P(None, CP_AXES, 'heads', None)
    stat_spec = P(None, CP_AXES, 'heads')
    key_spec = P(CP_AXES, 'heads', None)
    return jax.shard_map(call, mesh=mesh, in_specs=(row_spec, row_spec, row_spec, stat_spec, key_spec, key_spec),
                         out_specs=(row_spec, key_spec, key_spec), check_vma=False)
```

```python
import jax
import jax.numpy as jnp
from jax import lax
from jax.experimental import pallas as pl
from jax.experimental.pallas import tpu as pltpu
from jax.sharding import PartitionSpec as P

CP_AXES = ('cpo', 'cp')
MESH = pl.DeviceIdType.MESH
LOG2E = 1.4426950408889634

ROW = 8
RING = 4
GRP = 3
TOK = 16
KEYS = 32
DIM = 128
QROWS = ROW * GRP * TOK
KROWS = ROW * KEYS
PACK = GRP * TOK
SCALE = DIM ** -0.5
HOPS = RING

OWN, N1, N2, X = range(4)
GROUPS = (((0, 0), (0, 1), (0, 2), (0, 3)), ((-1, 0), (1, 0), (-1, 1), (1, 3)),
          ((-1, 3), (1, 2), (-1, 2), (1, 1)), ((2, 0), (2, 1), (2, 2), (2, 3)))
PLACE = {chunk: (group, slot) for group, chunks in enumerate(GROUPS) for slot, chunk in enumerate(chunks)}
DIRECT_KV = True
VIA_PLUS = (2, 0)

NSEM = 48
LINE_Q, LINE_KV, LINE_DQ = 50, 32, 24
SENT = (ROW - 1 + (RING - 1) * ROW) * (LINE_Q + LINE_KV) + (RING - 1) * ROW * (2 * KEYS + PACK) + (ROW - 1) * (2 * KEYS + LINE_DQ)

NT = (((1,), (1,)), ((), ()))
NN = (((1,), (0,)), ((), ()))
TN = (((0,), (0,)), ((), ()))


def dot(a, b, dims):
    return lax.dot_general(a, b, dims, preferred_element_type=jnp.float32)


def kernel(q_in, o_in, g_in, l_in, k_in, v_in, out_q, out_kv,
           q_vm, o_vm, g_vm, l_vm, k_vm, v_vm, perm_q, perm_kv, ts, tt,
           pq, pst, pkv, qd, st, kv, ld, rowc, akv, aqt, oq,
           ra_kv, rb_kv, ra_q, rb_q, fq, in_sem, ssem, rsem, gauge):
    me = lax.axis_index('cp')
    cpo = lax.axis_index('cpo')
    z, y = cpo // RING, cpo % RING
    x, core = me // 2, me % 2

    def row_dev(j):
        return (0, cpo, j)

    def along(n, queries):
        n = n % RING
        y_step = (core == 0) == queries
        return jnp.where(y_step, z, (z + n) % RING), jnp.where(y_step, (y + n) % RING, y)

    def ring_devs(queries):
        devs = []
        for n in (1, -1, 2):
            zn, yn = along(n, queries)
            devs.append((0, zn * RING + yn, me))
        return devs

    qdev, kdev = ring_devs(True), ring_devs(False)

    loads = [pltpu.make_async_copy(src, dst, in_sem.at[i // 5]) for i, (src, dst) in enumerate(
        ((g_in, g_vm), (q_in, q_vm), (k_in, k_vm), (v_in, v_vm), (o_in, o_vm), (l_in, l_vm)))]
    for ld_copy in loads:
        ld_copy.start()

    barrier = pltpu.get_barrier_semaphore()
    for j in range(1, ROW):
        pl.semaphore_signal(barrier, inc=1, device_id=row_dev((me + j) % ROW), device_id_type=MESH)
    for dev in qdev + kdev:
        pl.semaphore_signal(barrier, inc=1, device_id=dev, device_id_type=MESH)

    counter = [0]

    def take(n):
        first = counter[0]
        counter[0] += n
        assert counter[0] <= NSEM
        return first

    def remote(src, dst, recv_i, dev):
        return pltpu.make_async_remote_copy(
            src_ref=src, dst_ref=dst, send_sem=ssem.at[0], recv_sem=rsem.at[recv_i],
            device_id=dev, device_id_type=MESH)

    def lines(n):
        return gauge.at[pl.ds(0, n)]

    def arrived(n, recv_i):
        remote(lines(n), lines(n), recv_i, row_dev(me)).wait_recv()

    def chunk(ref, n, r):
        group, slot = PLACE[n, r]
        return ref.at[group, pl.ds(2 * slot, 2)]

    class Row:
        def __init__(self, size, *pairs):
            self.size, self.pairs, self.recv = size, pairs, take(HOPS)

        def send(self, *chips):
            for r in chips:
                back = (HOPS - r) % HOPS
                for c in ((0, 1) if r else (1 - core,)):
                    d = (x + r) % HOPS * 2 + c
                    for src, dst in self.pairs:
                        remote(src.at[d], dst.at[2 * back + core], self.recv + back, row_dev(d)).start()

        def wait(self, r):
            arrived(self.size * (2 if r else 1), self.recv + r)

    def permutation(ref, tokens, heads):
        n = tokens * heads
        i = lax.broadcasted_iota(jnp.int32, (n, n), 0)
        source = (i & (tokens - 1)) * heads + (i >> (tokens.bit_length() - 1))
        ref[...] = (lax.broadcasted_iota(jnp.int32, (n, n), 1) == source).astype(jnp.float32).astype(jnp.bfloat16)

    permutation(perm_q, TOK, ROW * GRP)
    permutation(perm_kv, KEYS, ROW)
    ts[...] = jnp.zeros_like(ts)
    with jax.named_scope('loads'):
        whole = lines((3 * QROWS + 2 * KROWS) // 2)
        pltpu.make_async_copy(whole, whole, in_sem.at[0]).wait()
        loads[5].wait()
    with jax.named_scope('pack'):
        prod = g_vm[...].astype(jnp.float32) * o_vm[...].astype(jnp.float32)
        delta = jnp.sum(prod.reshape(TOK, ROW * GRP, DIM), axis=-1)
        ts[pl.ds(0, TOK), pl.ds(0, ROW * GRP)] = l_vm[...].reshape(TOK, ROW * GRP)
        ts[pl.ds(TOK, TOK), pl.ds(0, ROW * GRP)] = delta
        tt[...] = ts[...].T
        rows = dot(perm_q[...], jnp.concatenate([q_vm[...], g_vm[...]], axis=1), NN).astype(jnp.bfloat16)
        for i in (0, 1):
            pq[:, pl.ds(i * GRP, GRP)] = rows[:, i * DIM:(i + 1) * DIM].reshape(ROW, GRP, TOK, DIM)
        rows = dot(perm_kv[...], jnp.concatenate([k_vm[...], v_vm[...]], axis=1), NN).astype(jnp.bfloat16)
        for i in (0, 1):
            pkv[:, i] = rows[:, i * DIM:(i + 1) * DIM].reshape(ROW, KEYS, DIM)
        lane = lax.broadcasted_iota(jnp.int32, (ROW, DIM), 1)
        for which in range(2):
            packed = jnp.zeros((ROW, DIM), jnp.float32)
            for g in range(GRP):
                rows = tt[pl.ds(g, ROW, stride=GRP), :]
                shift = (g * TOK - which * TOK) % DIM
                if shift:
                    rows = pltpu.roll(rows, shift, 1)
                packed = jnp.where((lane >= g * TOK) & (lane < (g + 1) * TOK), rows, packed)
            pst[:, which, :] = packed
    with jax.named_scope('barrier'):
        pl.semaphore_wait(barrier, ROW - 1 + 6)
    row_q = Row(LINE_Q, (pst, st.at[OWN]), (pq, qd.at[OWN]))
    row_kv = Row(LINE_KV, (pkv, kv.at[OWN]))
    row_q.send(0)
    row_kv.send(0)
    row_q.send(1)
    row_kv.send(1)
    row_q.send(3)
    row_kv.send(3)
    row_q.send(2)
    row_kv.send(2)
    st[OWN, core] = pst[me]
    qd[OWN, core] = pq[me]
    kv[OWN, core] = pkv[me]

    class Gather:
        def __init__(self, size, bufs, devs, direct=False):
            self.size, self.bufs, self.devs, self.direct = 2 * size, bufs, devs, direct
            self.recv = {at: take(1) for at in ((-1, 0), (1, 0), (-1, 1), (1, 3)) + (() if direct else ((1, 2),))}
            self.rest, self.far = take(1), take(1)

        def send(self, r, *sides):
            for side in sides:
                n = (-1, 1, 2)[side]
                recv_i = self.far if side == 2 else self.recv.get((n, r), self.rest)
                for buf in self.bufs:
                    remote(chunk(buf, 0, r), chunk(buf, n, r), recv_i, self.devs[side]).start()

        def wait(self, n, r):
            arrived(self.size, self.recv[n, r])

        def forward(self, n, r):
            self.wait(n, r)
            for buf in self.bufs:
                remote(chunk(buf, n, r), chunk(buf, 2, r), self.far, self.devs[0 if n < 0 else 1]).start()

        def wait_rest(self):
            arrived(self.size * (4 if self.direct else 3), self.rest)

        def wait_far(self):
            arrived(self.size * HOPS, self.far)

    agq, agkv = Gather(LINE_Q, (st, qd), qdev), Gather(LINE_KV, (kv,), kdev, DIRECT_KV)

    def pass_on(row, gather, r):
        row.wait(r)
        if r == 0:
            gather.send(0, 0, 1)
        elif r == 1:
            gather.send(1, 0)
        elif r == 3:
            gather.send(3, 1, 0)
        elif gather.direct:
            gather.send(2, 1, 0)
            gather.send(1, 1)
            gather.send(2, 2)
        else:
            gather.send(2, 1)
            gather.send(1, 1)
            gather.send(2, 0)

    with jax.named_scope('row_0'):
        pass_on(row_q, agq, 0)
        pass_on(row_kv, agkv, 0)

    r_id = lax.broadcasted_iota(jnp.int32, (1, QROWS), 1)
    packet = (r_id * 1366) >> 16
    token = ((r_id >> 3) & 1) * 1024 + (packet & 1) * 8 + (r_id & 7) + 2048
    for group in range(RING):
        spot = jnp.zeros_like(token)
        for slot, (n, r) in enumerate(GROUPS[group]):
            zq, yq = along(n, True)
            spot = jnp.where((packet >> 1) == slot, zq * 256 + yq * 64 + (x + r) % HOPS * 16, spot)
        rowc[group] = token + spot

    src_id = (3 * lax.broadcasted_iota(jnp.int32, (ROW, DIM), 0)) & 7

    def assemble(group):
        for which in range(2):
            rows = []
            for i in range(ROW):
                rows.append(st[group, pl.ds(3 * i % ROW, 1), which, :])
            rows = pltpu.roll(jnp.concatenate(rows, axis=0), 0, 1, stride=TOK, stride_axis=0)
            for k in range(QROWS // DIM):
                mine = (((lane + k * DIM) * 1366) >> 16) == src_id
                line = jnp.sum(jnp.where(mine, rows, 0.0), axis=0, keepdims=True)
                ld[group, pl.ds(which, 1), pl.ds(k * DIM, DIM)] = line * LOG2E if which == 0 else line

    class Scatter:
        def __init__(self, size, acc, ra, rb, devs):
            self.size, self.acc, self.ra, self.rb, self.devs = 2 * size, acc, ra, rb, devs
            self.first, self.near = take(HOPS), take(HOPS)

        def send_far(self, r):
            side = 0 if r in VIA_PLUS else 1
            remote(chunk(self.acc, 2, r), self.ra.at[r], self.first + r, self.devs[side]).start()

        def send_near(self, side, r):
            remote(chunk(self.acc, -1 if side else 1, r), self.rb.at[side, r], self.near + r, self.devs[side]).start()

        def send_early(self, r):
            self.send_near(1 if r in VIA_PLUS else 0, r)

        def send_late(self, r):
            side = 0 if r in VIA_PLUS else 1
            arrived(self.size, self.first + r)
            mine = chunk(self.acc, -1 if side else 1, r)
            mine[...] = mine[...] + self.ra[r]
            self.send_near(side, r)

        def total(self, r):
            arrived(2 * self.size, self.near + r)
            return chunk(self.acc, 0, r)[...] + self.rb[0, r] + self.rb[1, r]

    rsk, rsv = (Scatter(KEYS, akv.at[i], ra_kv.at[i], rb_kv.at[i], kdev) for i in (0, 1))
    rsq = Scatter(PACK, oq, ra_q, rb_q, qdev)

    band_rows = KROWS // HOPS
    key_row = lax.broadcasted_iota(jnp.int32, (band_rows, QROWS), 0)
    begun = set()

    def add(ref, name, value):
        ref[...] = ref[...] + value if name in begun else value
        begun.add(name)

    def tile(qs, ks):
        with jax.named_scope('tile' + ''.join(map(str, qs)) + 'x' + ''.join(map(str, ks))):
            q = jnp.concatenate([qd[i, :, pl.ds(0, GRP)].reshape(QROWS, DIM) for i in qs], axis=0)
            g = jnp.concatenate([qd[i, :, pl.ds(GRP, GRP)].reshape(QROWS, DIM) for i in qs], axis=0)
            k = jnp.concatenate([kv[i, :, 0].reshape(KROWS, DIM) for i in ks], axis=0)
            v = jnp.concatenate([kv[i, :, 1].reshape(KROWS, DIM) for i in ks], axis=0)
            lse = jnp.concatenate([ld[i, pl.ds(0, 1), :] for i in qs], axis=1)
            dlt = jnp.concatenate([ld[i, pl.ds(1, 1), :] for i in qs], axis=1)
            expo = jnp.exp2(dot(k, q, NT) * (SCALE * LOG2E) - lse)
            bands = []
            for n, r in [at for i in ks for at in GROUPS[i]]:
                zk, yk = along(n, False)
                first = zk * 1024 + yk * 256 + (x + r) % HOPS * band_rows
                seen = jnp.concatenate([key_row <= rowc[i] - first for i in qs], axis=1)
                at = len(bands) * band_rows
                bands.append(jnp.where(seen, expo[at:at + band_rows], 0.0))
            p_t = jnp.concatenate(bands, axis=0)
            dp_t = dot(v, g, NT)
            ds_t = (p_t * (dp_t - dlt)).astype(jnp.bfloat16)
            dv = dot(p_t.astype(jnp.bfloat16), g, NN)
            dk = dot(ds_t, q, NN)
            dq = dot(k, ds_t, TN)
            for n, i in enumerate(ks):
                add(akv.at[1, i], ('v', i), dv[n * KROWS:(n + 1) * KROWS].reshape(ROW, KEYS, DIM))
                add(akv.at[0, i], ('k', i), dk[n * KROWS:(n + 1) * KROWS].reshape(ROW, KEYS, DIM))
            for n, i in enumerate(qs):
                add(aqt.at[i], ('q', i), dq[:, n * QROWS:(n + 1) * QROWS])

    def finish_q(group):
        oq[group] = aqt[group].T.reshape(ROW, PACK, DIM)

    for r in (1, 3, 2):
        for name, row, gather in (('', row_q, agq), ('kv', row_kv, agkv)):
            with jax.named_scope(f'row_{name}{r}'):
                pass_on(row, gather, r)
    assemble(OWN)
    tile([OWN], [OWN])
    with jax.named_scope('fwd_0'):
        agq.forward(-1, 0)
        agkv.forward(-1, 0)
    with jax.named_scope('fwd_q1'):
        agq.forward(-1, 1)
        agq.forward(1, 3)
        agq.wait(1, 0)
        assemble(N1)
    tile([N1], [OWN])
    with jax.named_scope('fwd_k1'):
        agkv.forward(-1, 1)
        agkv.forward(1, 3)
    with jax.named_scope('fwd_q2'):
        agq.forward(1, 2)
    with jax.named_scope('fwd_k2'):
        if not DIRECT_KV:
            agkv.forward(1, 2)
        agkv.wait(1, 0)
    tile([OWN, N1], [N1])
    with jax.named_scope('rest_k'):
        agkv.wait_rest()
    tile([OWN, N1], [N2])
    with jax.named_scope('rest_q'):
        agq.wait_rest()
        assemble(N2)
    tile([N2], [OWN, N1, N2])
    with jax.named_scope('far_k'):
        agkv.wait_far()
    tile([OWN, N1, N2], [X])
    with jax.named_scope('far_q'):
        agq.wait_far()
        assemble(X)
    tile([X], [X])
    for pair in ((2, 1), (0, 3)):
        for scatter in (rsv, rsk):
            for r in pair:
                scatter.send_far(r)
    tile([X], [N1, N2, OWN])
    finish_q(X)
    rsq.send_far(2)
    rsq.send_far(1)

    @pl.when(core == 0)
    def _():
        rsq.send_far(0)
        rsq.send_far(3)

    for scatter in (rsv, rsk):
        scatter.send_early(1)
        scatter.send_early(2)
    with jax.named_scope('finish'):
        finish_q(N1)
        finish_q(N2)

    @pl.when(core == 0)
    def _():
        rsq.send_early(1)
        rsq.send_early(2)

    finish_q(OWN)

    def late(name, scatter, *chunks):
        with jax.named_scope(f'late_{name}{chunks[0]}'):
            for r in chunks:
                scatter.send_late(r)

    class Give:
        def __init__(self, size, src, dst):
            self.size, self.src, self.dst, self.recv_i = size, src, dst, take(1)

        def send(self, r):
            for c in ((0, 1) if r else (1 - core,)):
                d = (x + r) % HOPS * 2 + c
                remote(self.src.at[2 * r + c], self.dst.at[me], self.recv_i, row_dev(d)).start()

        def wait(self):
            arrived(self.size * (ROW - 1), self.recv_i)

    give_k, give_v, give_q = Give(KEYS, akv.at[0, OWN], out_kv.at[0]), Give(KEYS, akv.at[1, OWN], out_kv.at[1]), Give(LINE_DQ, fq, out_q)

    def total(name, r):
        part = pl.ds(2 * r, 2)
        with jax.named_scope(f'total_{name}{r}'):
            if name == 'v':
                akv[1, OWN, part] = rsv.total(r)
            elif name == 'k':
                akv[0, OWN, part] = rsk.total(r) * SCALE
            else:
                fq[part] = (rsq.total(r) * SCALE).astype(jnp.bfloat16)
        {'v': give_v, 'k': give_k, 'q': give_q}[name].send(r)

    def early(r):
        rsv.send_early(r)
        rsk.send_early(r)

    def totals(names, *chunks):
        for r in chunks:
            for name in names:
                total(name, r)

    late('v', rsv, 2, 1)
    late('k', rsk, 2, 1)

    @pl.when(core == 0)
    def _():
        early(3)
        late('v', rsv, 3)
        late('k', rsk, 3)
        late('q', rsq, 2, 1)
        rsq.send_early(3)
        late('q', rsq, 3)
        late('q', rsq, 0)
        rsq.send_early(0)
        totals('vk', 2)
        late('v', rsv, 0)
        late('k', rsk, 0)
        early(0)
        totals('vk', 1, 3)
        totals('q', 2, 1, 3)
        totals('vkq', 0)

    @pl.when(core == 1)
    def _():
        rsq.send_far(0)
        rsq.send_far(3)
        rsq.send_early(1)
        rsq.send_early(2)
        early(3)
        late('v', rsv, 3)
        late('k', rsk, 3)
        late('q', rsq, 2, 1)
        rsq.send_early(3)
        totals('vk', 2, 1)
        late('q', rsq, 3)
        totals('vk', 3)
        late('v', rsv, 0)
        late('k', rsk, 0)
        early(0)
        late('q', rsq, 0)
        rsq.send_early(0)
        totals('q', 2, 1, 3)
        totals('vkq', 0)

    out_q[me] = fq[core]
    out_kv[0, me] = akv[0, OWN, core]
    out_kv[1, me] = akv[1, OWN, core]

    with jax.named_scope('final_q'):
        give_q.wait()
    with jax.named_scope('final_kv'):
        give_v.wait()
        give_k.wait()
    with jax.named_scope('drain'):
        remote(lines(SENT), lines(SENT), 0, row_dev(me)).wait_send()


def relayout(q_ref, kv_ref, dq_ref, dk_ref, dv_ref, rows):
    for h in range(ROW):
        dk_ref[:, h, :] = kv_ref[0, h]
        dv_ref[:, h, :] = kv_ref[1, h]
        for g in range(GRP):
            rows[:, h * GRP + g, :] = q_ref[h, pl.ds(g * TOK, TOK), :].astype(jnp.float32)
    dq_ref[...] = rows[...].astype(jnp.bfloat16).reshape(dq_ref.shape)


def call(queries, attn_out, grad_out, log_sum_exp, key_cache, value_cache):
    f32, bf16 = jnp.float32, jnp.bfloat16
    vmem = pltpu.VMEM
    tok = (2, TOK // 2, ROW * GRP, DIM)
    key = (KEYS, ROW, DIM)
    tok2, key2 = (QROWS, DIM), (KROWS, DIM)
    scratch = [
        vmem(tok2, bf16), vmem(tok2, bf16), vmem(tok2, bf16), vmem(tok[:3], f32), vmem(key2, bf16), vmem(key2, bf16),
        vmem((QROWS, QROWS), bf16), vmem((KROWS, KROWS), bf16), vmem((DIM, DIM), f32), vmem((DIM, DIM), f32),
        vmem((ROW, 2 * GRP, TOK, DIM), bf16), vmem((ROW, 2, DIM), f32), vmem((ROW, 2, KEYS, DIM), bf16),
        vmem((RING, ROW, 2 * GRP, TOK, DIM), bf16), vmem((RING, ROW, 2, DIM), f32), vmem((RING, ROW, 2, KEYS, DIM), bf16),
        vmem((RING, 8, QROWS), f32), vmem((RING, 1, QROWS), jnp.int32),
        vmem((2, RING, ROW, KEYS, DIM), f32), vmem((RING, DIM, QROWS), f32), vmem((RING, ROW, PACK, DIM), f32),
        vmem((2, HOPS, 2, KEYS, DIM), f32), vmem((2, 2, HOPS, 2, KEYS, DIM), f32),
        vmem((HOPS, 2, PACK, DIM), f32), vmem((2, HOPS, 2, PACK, DIM), f32),
        vmem((ROW, PACK, DIM), bf16),
        pltpu.SemaphoreType.DMA((2,)), pltpu.SemaphoreType.DMA((1,)), pltpu.SemaphoreType.DMA((NSEM,)),
        vmem((SENT, DIM), f32),
    ]
    out_q, out_kv = pl.pallas_call(
        kernel,
        out_shape=(vmem((ROW, PACK, DIM), bf16), vmem((2, ROW, KEYS, DIM), f32)),
        in_specs=[pl.BlockSpec(memory_space=pl.ANY)] * 6,
        out_specs=[pl.BlockSpec(memory_space=pltpu.VMEM)] * 2,
        scratch_shapes=scratch,
        compiler_params=pltpu.CompilerParams(collective_id=0, has_side_effects=True),
        name='attn_bwd_3d',
    )(queries.reshape(tok2), attn_out.reshape(tok2), grad_out.reshape(tok2), log_sum_exp,
      key_cache.reshape(key2), value_cache.reshape(key2))
    return pl.pallas_call(
        relayout,
        out_shape=(jax.ShapeDtypeStruct(tok, bf16), jax.ShapeDtypeStruct(key, f32), jax.ShapeDtypeStruct(key, f32)),
        in_specs=[pl.BlockSpec(memory_space=pltpu.VMEM)] * 2,
        out_specs=[pl.BlockSpec(memory_space=pltpu.VMEM)] * 3,
        scratch_shapes=[vmem((TOK, ROW * GRP, DIM), f32)],
        name='relayout',
    )(pltpu.with_memory_space_constraint(out_q, vmem), pltpu.with_memory_space_constraint(out_kv, vmem))


def solution(mesh):
    row_spec = P(None, CP_AXES, 'heads', None)
    stat_spec = P(None, CP_AXES, 'heads')
    key_spec = P(CP_AXES, 'heads', None)
    return jax.shard_map(call, mesh=mesh, in_specs=(row_spec, row_spec, row_spec, stat_spec, key_spec, key_spec),
                         out_specs=(row_spec, key_spec, key_spec), check_vma=False)
```
